512 devices in a mesh: front: 8 (over y), row: 8 (over z), col: 8 (over x, core).
Axes of the slice: x: 4, y: 8, z: 8, core: 2. Of those that a mesh axis runs over, the one named last changes fastest.
Arguments:
- pivot: float32 [8, 512, 512], P('front', ('row', 'col')), may hold values from -1 to 8
- col_ut: bfloat16 [8, 8, 96, 512], P('front', 'row', None, 'col'), may hold values from -6 to 6
- col_vt: bfloat16 [8, 8, 96, 512], P('front', 'row', None, 'col'), may hold values from -0.25 to 0.25
- col_rank: int32 [8, 8], P('front', 'row'), may hold values from 32 to 96
- row_ut: bfloat16 [8, 8, 96, 512], P('front', 'col', None, 'row'), may hold values from -6 to 6
- row_vt: bfloat16 [8, 8, 96, 512], P('front', 'col', None, 'row'), may hold values from -0.625 to 0.625
- row_rank: int32 [8, 8], P('front', 'col'), may hold values from 32 to 96
- cb_ut: bfloat16 [8, 8, 8, 96, 512], P('front', 'row', 'col'), may hold values from -6 to 6
- cb_vt: bfloat16 [8, 8, 8, 96, 512], P('front', 'row', 'col'), may hold values from -0.625 to 0.625
- cb_rank: int32 [8, 8, 8], P('front', 'row', 'col'), may hold values from 32 to 96
- parent_map: int32 [8, 8], P('front'), may hold values from 0 to 15, as said below
Outputs:
- parent_tiles: bfloat16 [8, 16, 8, 512, 512], P('front', 'row', 'col')
The draws below stay inside these ranges and needn't reach their ends.
Inputs may be any that keep to these rules, and one draw needn't show every extreme that they name: `parent_map`: for every front the entries are distinct; entry 0 is 8, and 0 and 15 both appear.
All inputs are finite; a program needn't handle non-finite values.
Results may differ from the reference program's by a relative error of at most 0.0062.
Values may be sent and summed in bfloat16 or wider, within the bound.
No kernel may reach another device: no remote copies, remote signals or barrier semaphores. Data moves between devices by JAX's collectives and lax.ppermute only.
A program may use at most 64 MiB of HBM per device.

```python
import math
import jax
import jax.numpy as jnp
from jax import lax

TILE = 512
RANK = 96
NS_ITERS = 2
TD = 1
NC = 8
NP = 16
FRONTS = 8
PARENTS = 4
N_COL = 8


def draw_pivot(key, part):
    key_off, key_diag = jax.random.split(key, 2)
    spread = 1.2 * TILE ** (-0.5)
    offdiag = jax.random.normal(key_off, (FRONTS, TILE, TILE), jnp.float32) * spread
    levels = jax.random.uniform(key_diag, (FRONTS, TILE), jnp.float32, math.log(4.0), math.log(8.0))
    diagonal = jnp.exp(levels)
    eye = jnp.eye(TILE, dtype=jnp.float32)
    return offdiag * (1.0 - eye)[None] + diagonal[:, :, None] * eye[None]


def pick_targets(single):
    key_pick, key_order = jax.random.split(single, 2)
    values = jnp.arange(NP, dtype=jnp.int32)
    scores = jax.random.permutation(key_pick, NP).astype(jnp.int32)
    at_ends = ((values == 0) | (values == NP - 1)).astype(jnp.int32)
    reserved = (values == NC).astype(jnp.int32)
    scores = scores + 2 * NP * at_ends - 4 * NP * reserved
    ranking = jnp.argsort(-scores, stable=True).astype(jnp.int32)
    chosen = jax.random.permutation(key_order, ranking[:NC - 1]).astype(jnp.int32)
    return jnp.concatenate([jnp.full((1,), NC, jnp.int32), chosen]).astype(jnp.int32)


def draw_parent_map(key, part):
    front_keys = jax.random.split(jax.random.fold_in(key, 7), FRONTS)
    return jax.vmap(pick_targets)(front_keys).astype(jnp.int32)


def set_ends(entries, stream_key, smallest, high):
    shape = entries.shape
    place = [jax.random.randint(jax.random.fold_in(stream_key, axis), (), 0, shape[axis]) for axis in range(len(shape))]
    entries = entries.at[tuple(place)].set(smallest)
    longest = shape.index(max(shape))
    place[longest] = (place[longest] + 1) % shape[longest]
    return entries.at[tuple(place)].set(high)


def level_of(key, dims, shards, least, largest):
    loudness, own = 1.0, jax.random.fold_in(key, 6)
    for axis_at, blocks in shards:
        heights = jnp.exp(jax.random.uniform(jax.random.fold_in(own, axis_at), (blocks,), jnp.float32, least / len(shards), largest / len(shards)))
        loudness = loudness * jnp.repeat(heights, dims[axis_at] // blocks).reshape([-1 if axis == axis_at else 1 for axis in range(len(dims))])
    return loudness


def centred(key, shape, scale, reach, shards=(), held_as=jnp.bfloat16):
    drawn = jax.random.normal(key, shape, jnp.float32) * scale
    if len(shards) > 0:
        drawn = level_of(key, shape, shards, -0.22, 0.18) * drawn
    return jnp.clip(drawn, min=-reach, max=reach).astype(held_as)


def setup_inputs(seed: int = 0) -> dict:
    streams_of = jax.random.split(jax.random.key(seed), 12)
    pivot = draw_pivot(jax.random.fold_in(streams_of[11], 71), 0)
    col_ut = centred(streams_of[1], (FRONTS, NC, RANK, TILE), 1.0, 6.0, ((0, 8), (1, 8), (3, 8)))
    col_vt = centred(streams_of[2], (FRONTS, NC, RANK, TILE), TILE ** -0.5, 0.25, ((0, 8), (1, 8), (3, 8)))
    col_rank = set_ends(jax.random.randint(streams_of[3], (FRONTS, NC), RANK // 3, RANK + 1), jax.random.fold_in(streams_of[3], 1), RANK // 3, RANK).astype(jnp.int32)
    row_ut = centred(streams_of[4], (FRONTS, NC, RANK, TILE), 1.0, 6.0, ((0, 8), (1, 8), (3, 8)))
    row_vt = centred(streams_of[5], (FRONTS, NC, RANK, TILE), RANK ** -0.5, 0.625, ((0, 8), (1, 8), (3, 8)))
    row_rank = set_ends(jax.random.randint(streams_of[6], (FRONTS, NC), RANK // 3, RANK + 1), jax.random.fold_in(streams_of[6], 1), RANK // 3, RANK).astype(jnp.int32)
    cb_ut = centred(streams_of[7], (FRONTS, NC, NC, RANK, TILE), 1.0, 6.0, ((0, 8), (1, 8), (2, 8)))
    cb_vt = centred(streams_of[8], (FRONTS, NC, NC, RANK, TILE), RANK ** -0.5, 0.625, ((0, 8), (1, 8), (2, 8)))
    cb_rank = set_ends(jax.random.randint(streams_of[9], (FRONTS, NC, NC), RANK // 3, RANK + 1), jax.random.fold_in(streams_of[9], 1), RANK // 3, RANK).astype(jnp.int32)
    parent_map = draw_parent_map(jax.random.fold_in(streams_of[11], 71), 0)
    return {"pivot": pivot, "col_ut": col_ut, "col_vt": col_vt, "col_rank": col_rank, "row_ut": row_ut, "row_vt": row_vt, "row_rank": row_rank, "cb_ut": cb_ut, "cb_vt": cb_vt, "cb_rank": cb_rank, "parent_map": parent_map}


HIGH = lax.Precision.HIGHEST


def invert(matrix):
    eye = jnp.eye(matrix.shape[0], dtype=jnp.float32)
    approx = eye / jnp.diagonal(matrix)[None, :]
    for step in range(NS_ITERS):
        approx = jnp.dot(approx, 2.0 * eye - jnp.dot(matrix, approx, precision=HIGH), precision=HIGH)
    return approx


def ranked(factor, rank):
    levels = jnp.arange(factor.shape[-2], dtype=jnp.int32)[:, None]
    keep = levels < rank[..., None, None]
    return jnp.where(keep, factor, jnp.zeros_like(factor)).astype(jnp.bfloat16)


def child(pivot, col_ut, col_vt, col_rank, row_ut, row_vt, row_rank, cb_ut, cb_vt, cb_rank, parent_map):
    inverse = invert(pivot)
    left_col = ranked(col_ut, col_rank)
    right_col = ranked(col_vt, col_rank)
    lower = jnp.einsum('atx,xy->aty', right_col.astype(jnp.float32), inverse, precision=HIGH).astype(jnp.bfloat16)
    upper_left = ranked(row_ut, row_rank)
    upper_right = ranked(row_vt, row_rank)
    core = jnp.einsum('iax,jbx->ijab', lower.astype(jnp.float32), upper_left.astype(jnp.float32)).astype(jnp.bfloat16)
    update = jnp.einsum('ijab,iax->ijbx', core.astype(jnp.float32), left_col.astype(jnp.float32)).astype(jnp.bfloat16)
    block_left = ranked(cb_ut, cb_rank)
    block_right = ranked(cb_vt, cb_rank)

    def one_row(pieces):
        left_part, right_part, update_part = pieces
        left = jnp.concatenate([left_part, -update_part], axis=1).astype(jnp.float32)
        right = jnp.concatenate([right_part, upper_right], axis=1).astype(jnp.float32)
        return jnp.einsum('jkx,jky->jxy', left, right).astype(jnp.bfloat16)

    schur = lax.map(one_row, (block_left, block_right, update))
    count = parent_map.shape[0]
    places = jnp.arange(count, dtype=jnp.int32)
    targets = jnp.arange(NP, dtype=jnp.int32)
    onehot = (parent_map[None, :] == targets[:, None]).astype(jnp.int32)
    source = jnp.sum(onehot * places[None, :], axis=1).astype(jnp.int32)
    present = jnp.sum(onehot, axis=1) > 0
    placed = schur[source][:, source]
    keep = present[:, None] & present[None, :]
    return jnp.where(keep[:, :, None, None], placed, jnp.zeros_like(placed))


def reference(pivot, col_ut, col_vt, col_rank, row_ut, row_vt, row_rank, cb_ut, cb_vt, cb_rank, parent_map):
    arrays = (pivot, col_ut, col_vt, col_rank, row_ut, row_vt, row_rank, cb_ut, cb_vt, cb_rank, parent_map)
    paired = tuple(item.reshape((PARENTS, 2) + item.shape[1:]) for item in arrays)

    def one_parent(group):
        first = child(*[item[0] for item in group])
        second = child(*[item[1] for item in group])
        return (first.astype(jnp.float32) + second.astype(jnp.float32)).astype(jnp.bfloat16)

    parents = lax.map(one_parent, paired)
    laid = parents.reshape(PARENTS, NP, N_COL, 2, TD, TILE, TILE)
    laid = jnp.transpose(laid, (0, 3, 1, 2, 4, 5, 6))
    return laid.reshape(PARENTS * 2, NP, N_COL * TD, TILE, TILE)
```

```python
import jax
import jax.numpy as jnp
from jax import lax
from jax.experimental import pallas as pl
from jax.experimental.pallas import tpu as pltpu
from jax.sharding import Mesh, PartitionSpec as P

F32 = jnp.float32
BF16 = jnp.bfloat16
RANK = 96
TILE = 512
N = 8
SMEM = pltpu.SMEM
VMEM = pltpu.VMEM


def iota(shape, dim):
    return lax.broadcasted_iota(jnp.int32, shape, dim)


def dot(a, b, contract, precision=None):
    return lax.dot_general(
        a, b, ((contract[:1], contract[1:]), ((), ())), precision=precision, preferred_element_type=F32
    )


def call(body, outs, args, specs, scratch=(), name=None):
    return pl.pallas_call(
        body,
        out_shape=outs,
        in_specs=[pl.BlockSpec(memory_space=s) for s in specs],
        out_specs=[pl.BlockSpec(memory_space=VMEM) for _ in outs],
        scratch_shapes=scratch,
        name=name,
    )(*args)


def fill_inverse(mapping, inverse):
    for k in range(2 * N):
        inverse[k] = N
    for k in range(N):
        inverse[mapping[0, k]] = k


def onehot(first, step, offset):
    row = iota((64, RANK), 0)
    level = iota((64, RANK), 1)
    t = row % 8
    keep = (t >= first) & (t < first + 6)
    return (keep & (level == step * (row // 8) + offset + t - first)).astype(BF16)


def pack(
    piv, cu, cv, ru, rv, cbu, cbv, rank_c, rank_r, rank_b, send, first, row_v
):
    level = iota((RANK, 64), 0)
    even = onehot(0, 12, 0)
    odd = onehot(0, 12, 6)

    def panel(ref, rank):
        x = jnp.where(level < rank, ref[...].astype(F32), 0.0).astype(BF16)
        return jnp.concatenate([dot(even, x, (1, 0)), dot(odd, x, (1, 0))], axis=1)

    col_u = panel(cu, rank_c[0, 0])
    col_v = panel(cv, rank_c[0, 0])
    row_u = panel(ru, rank_r[0, 0])
    row_v[...] = panel(rv, rank_r[0, 0])
    pieces = [piv[:, 128 * m : 128 * m + 128] for m in range(4)]
    both = jnp.concatenate(pieces + [col_u], axis=0)
    for k in range(N):
        first[k] = both
    wide = iota((RANK, TILE), 0)
    row = iota((64, RANK), 0)
    lev = iota((64, RANK), 1)
    t = row % 8
    extra = [
        ((t >= 6) & (lev == 64 + 4 * (row // 8) + 2 * e + t - 6)).astype(BF16) for e in range(2)
    ]
    for side, ref in enumerate((cbu, cbv)):
        x = jnp.where(wide < rank_b[0, 0], ref[...].astype(F32), 0.0)
        low = x.astype(BF16)
        x1 = dot(extra[0], low, (1, 0))
        x2 = dot(extra[1], low, (1, 0))
        for g in range(N):
            rows = slice(8 * g, 8 * g + 8)
            for m in range(4):
                lanes = slice(128 * m, 128 * m + 128)
                c = 2 * m + side
                send[g * N + c] = jnp.concatenate(
                    [
                        x[rows, lanes],
                        col_v[rows] + x1[rows, lanes],
                        row_u[8 * c : 8 * c + 8] + x2[rows, lanes],
                    ],
                    axis=0,
                ).astype(BF16)


def second(got, row_v, mapping, send_p, send_u, inverse):
    fill_inverse(mapping, inverse)
    for g in range(N):
        block = got[g, 0:32, :]
        for k in range(N):
            send_p[k, 32 * g : 32 * g + 32, :] = block
    tail = row_v[...]
    for k in range(N):
        send_p[k, 256:320, :] = tail
    here = lax.axis_index("row")
    for s in range(2):
        at = inverse[2 * here + s]
        x = got[jnp.minimum(at, N - 1), 32:96, :]
        x = jnp.where(at < N, x, jnp.zeros_like(x)).astype(BF16)
        for k in range(2 * N):
            send_u[k, 64 * s : 64 * s + 64, :] = x


def select(got, mapping, send, inverse, t0, g0, g1):
    fill_inverse(mapping, inverse)
    row = iota((8, 128), 0)
    zero = jnp.zeros((8, 128), F32)
    t0[64] = zero
    g0[64] = zero
    g1[64] = zero
    for k in range(64):
        x = got[k].astype(F32)
        a, b = x[8:16], x[16:24]
        t0[k] = x[0:8]
        g0[k] = jnp.where(row >= 6, a, jnp.where(row >= 4, pltpu.roll(b, 6, 0), 0.0))
        g1[k] = jnp.where(
            row >= 4, 0.0, jnp.where(row >= 2, pltpu.roll(a, 4, 0), pltpu.roll(b, 2, 0))
        )

    def place(r, _):
        i0 = inverse[2 * r]
        i1 = inverse[2 * r + 1]
        for h in range(2):
            for c in range(N):
                j = inverse[2 * c + h]
                at0 = jnp.where((i0 < N) & (j < N), i0 * N + j, 64)
                at1 = jnp.where((i1 < N) & (j < N), i1 * N + j, 64)
                send[(h * N + r) * N + c] = jnp.concatenate(
                    [t0[at0], t0[at1], g0[at0] + g1[at1]], axis=0
                ).astype(BF16)
        return 0

    lax.fori_loop(0, N, place, 0)


def spread(tiles):
    lane = iota(tiles[0].shape, 1)
    halves = ([], [])
    for m in range(N // 2):
        x, y = tiles[2 * m], tiles[2 * m + 1]
        halves[0].append(jnp.where(lane < 64, x, pltpu.roll(y, 64, 1)))
        halves[1].append(jnp.where(lane < 64, pltpu.roll(x, 64, 1), y))
    return [jnp.concatenate(h, axis=1) for h in halves]


def cores(got, pieces, mapping, send_c, send_v, inverse, pivot, lower_ref, right_ref):
    fill_inverse(mapping, inverse)
    for c in range(N):
        for g in range(N):
            for m in range(4):
                at = 32 * g + 8 * m
                pivot[64 * g + 8 * c : 64 * g + 8 * c + 8, 128 * m : 128 * m + 128] = pieces[
                    c, at : at + 8, :
                ]
    here = lax.axis_index("col")
    for h in range(2):
        at = inverse[2 * here + h]
        x = pieces[jnp.minimum(at, N - 1), 256:320, :]
        x = jnp.where(at < N, x, jnp.zeros_like(x)).astype(BF16)
        for r in range(N):
            send_v[h * N + r] = x
    full = pivot[...]
    eye = iota((TILE, TILE), 0) == iota((TILE, TILE), 1)
    inv = 1.0 / jnp.sum(jnp.where(eye, full, 0.0), axis=0, keepdims=True)
    valid = iota((8, 128), 0) < 6

    def tile(i, j, at):
        return jnp.where(valid, got[i * N + j, at : at + 8, :].astype(F32), 0.0)

    left = [[], []]
    for i in range(N):
        parts = spread([tile(i, j, 8) for j in range(N)])
        left[0].append(parts[0])
        left[1].append(parts[1])
    v = jnp.concatenate(left[0] + left[1], axis=0)
    high = lax.Precision.HIGHEST
    v0 = v * inv
    y = 2.0 * v0 - dot(v0, full, (1, 0), high) * inv
    z = dot(y, full, (1, 0), high) * inv
    lower = 2.0 * y - (2.0 * z - dot(z, full, (1, 0), high) * inv)
    for k in range(2 * N):
        lower_ref[k] = lower[8 * k : 8 * k + 8]
    lower_ref[2 * N] = jnp.zeros((8, TILE), F32)
    right_ref[2 * N] = jnp.zeros((8, TILE), F32)
    for j in range(N):
        parts = spread([tile(i, j, 16) for i in range(N)])
        right_ref[2 * j] = parts[0]
        right_ref[2 * j + 1] = parts[1]
    rows = []
    for half in range(2):
        for s in range(2):
            for r in range(N):
                i = inverse[2 * r + s]
                rows.append(lower_ref[jnp.where(i < N, half * N + i, 2 * N)])
    cols = []
    for k in range(2 * N):
        j = inverse[k]
        for half in range(2):
            cols.append(right_ref[jnp.where(j < N, 2 * j + half, 2 * N)])
    core = dot(
        jnp.concatenate(rows, axis=0).astype(BF16), jnp.concatenate(cols, axis=0).astype(BF16), (1, 1)
    )
    core = core.astype(BF16).astype(F32)
    lane = iota((64, 128), 1) // 16
    for k in range(2 * N):
        c, h = k // 2, k % 2
        total = jnp.zeros((64, 128), F32)
        for combo in range(4):
            x = core[64 * combo : 64 * combo + 64, 128 * (k // 8) : 128 * (k // 8) + 128]
            shift = (16 * combo - 16 * (k % 8)) % 128
            total = jnp.where(lane == combo, pltpu.roll(x, shift, 1) if shift else x, total)
        for r in range(N):
            send_c[(h * N + r) * N + c] = total[8 * r : 8 * r + 8].astype(BF16)


def finish(blocks, core_in, col_in, row_in, out):
    lefts, rights = [], []
    for f in range(2):
        for side, into in ((0, lefts), (1, rights)):
            lanes = []
            for m in range(4):
                c = 2 * m + side
                lanes.append(
                    jnp.concatenate(
                        [blocks[f * 64 + g * N + c].astype(F32) for g in range(N)], axis=0
                    )
                )
            into.append(jnp.concatenate(lanes, axis=1))
    left = jnp.concatenate(lefts, axis=0)
    row = iota(left.shape, 0) % 24
    slots = (
        (row < 8) | (row >= 20),
        (row >= 8) & (row < 20),
    )
    lane = iota((64, 128), 1) // 16
    updates = [[], []]
    for f in range(2):
        parts = [
            jnp.concatenate(
                [core_in[f * 64 + g * N + c].astype(F32) for g in range(N)], axis=0
            )
            for c in range(N)
        ]
        for s in range(2):
            halves = []
            for half in range(2):
                total = jnp.zeros((64, 128), F32)
                combo = 2 * half + s
                for c in range(N):
                    shift = (16 * c - 16 * combo) % 128
                    x = pltpu.roll(parts[c], shift, 1) if shift else parts[c]
                    total = jnp.where(lane == c, x, total)
                halves.append(total)
            core = jnp.concatenate(halves, axis=0).astype(BF16)
            col_u = spread(
                [col_in[f * N + c, 64 * s : 64 * s + 64, :].astype(F32) for c in range(N)]
            )
            col_u = jnp.concatenate(col_u, axis=0).astype(BF16)
            updates[s].append(-dot(core, col_u, (0, 0)))
        v0, v1 = spread([row_in[f * N + r].astype(F32) for r in range(N)])
        mixed = []
        for g in range(N):
            mixed += [v0[8 * g : 8 * g + 8], v1[8 * g : 8 * g + 8]]
        rights.append(jnp.concatenate(mixed, axis=0))
    right = jnp.concatenate(rights, axis=0).astype(BF16)
    for s in range(2):
        both = jnp.concatenate([jnp.where(slots[s], left, 0.0)] + updates[s], axis=0).astype(BF16)
        out[s] = dot(both, right, (0, 0)).astype(BF16)


def exchange(x, axes):
    return lax.all_to_all(x, axes, split_axis=0, concat_axis=0, tiled=True)


def shards(
    pivot, col_ut, col_vt, col_rank, row_ut, row_vt, row_rank, cb_ut, cb_vt, cb_rank, parent_map
):
    sds = jax.ShapeDtypeStruct
    send, first, row_v = call(
        pack,
        (sds((64, 24, 128), BF16), sds((N, 96, 128), F32), sds((64, 128), F32)),
        (
            pivot[0],
            col_ut[0, 0],
            col_vt[0, 0],
            row_ut[0, 0],
            row_vt[0, 0],
            cb_ut[0, 0, 0],
            cb_vt[0, 0, 0],
            col_rank,
            row_rank,
            cb_rank[0],
        ),
        (VMEM,) * 7 + (SMEM,) * 3,
        name="pack",
    )
    got_first = exchange(first, "row")
    got = exchange(send, ("row", "col"))
    send_p, send_u = call(
        second,
        (sds((N, 320, 128), F32), sds((2 * N, 128, 128), BF16)),
        (got_first, row_v, parent_map),
        (VMEM, VMEM, SMEM),
        (pltpu.SMEM((2 * N,), jnp.int32),),
        name="second",
    )
    pieces = exchange(send_p, "col")
    col_in = exchange(send_u, ("side", "col"))
    (send_b,) = call(
        select,
        (sds((128, 24, 128), BF16),),
        (got, parent_map),
        (VMEM, SMEM),
        (pltpu.SMEM((2 * N,), jnp.int32),) + (VMEM((65, 8, 128), F32),) * 3,
        name="select",
    )
    blocks = exchange(send_b, ("side", "row", "col"))
    send_c, send_v = call(
        cores,
        (sds((128, 8, 128), BF16), sds((2 * N, 64, 128), BF16)),
        (got, pieces, parent_map),
        (VMEM, VMEM, SMEM),
        (
            pltpu.SMEM((2 * N,), jnp.int32),
            VMEM((TILE, TILE), F32),
            VMEM((2 * N + 1, 8, TILE), F32),
            VMEM((2 * N + 1, 8, TILE), F32),
        ),
        name="cores",
    )
    core_in = exchange(send_c, ("side", "row", "col"))
    row_in = exchange(send_v, ("side", "row"))
    (out,) = call(
        finish,
        (sds((2, TILE, TILE), BF16),),
        (blocks, core_in, col_in, row_in),
        (VMEM,) * 4,
        name="finish",
    )
    return out[None, :, None]


def solution(mesh):
    front = ("pair", "side")
    split = Mesh(mesh.devices.reshape(4, 2, N, N), ("pair", "side", "row", "col"))
    placed = (
        P(front, ("row", "col"), None),
        P(front, "row", None, "col"),
        P(front, "row", None, "col"),
        P(front, "row"),
        P(front, "col", None, "row"),
        P(front, "col", None, "row"),
        P(front, "col"),
        P(front, "row", "col", None, None),
        P(front, "row", "col", None, None),
        P(front, "row", "col"),
        P(front, None),
    )
    return jax.shard_map(
        shards,
        mesh=split,
        in_specs=placed,
        out_specs=P(front, "row", "col", None, None),
        check_vma=False,
    )
```

```python
import jax
import jax.numpy as jnp
from jax import lax
from jax.experimental import pallas as pl
from jax.experimental.pallas import tpu as pltpu
from jax.sharding import Mesh, PartitionSpec as P


F32 = jnp.float32
BF16 = jnp.bfloat16
RANK = 96
TILE = 512
N = 8
SMEM = pltpu.SMEM
VMEM = pltpu.VMEM


def iota(shape, dim):
    return lax.broadcasted_iota(jnp.int32, shape, dim)


def dot(a, b, contract):
    return lax.dot_general(
        a, b, ((contract[:1], contract[1:]), ((), ())), preferred_element_type=F32
    )


def call(body, outs, args, specs, scratch=()):
    return pl.pallas_call(
        body,
        out_shape=outs,
        in_specs=[pl.BlockSpec(memory_space=s) for s in specs],
        out_specs=[pl.BlockSpec(memory_space=VMEM) for _ in outs],
        scratch_shapes=scratch,
    )(*args)


def fill_inverse(mapping, inverse):
    for k in range(2 * N):
        inverse[k] = N
    for k in range(N):
        inverse[mapping[0, k]] = k


def onehot(offset):
    row = iota((64, RANK), 0)
    level = iota((64, RANK), 1)
    t = row % 8
    return ((t < 6) & (level == 12 * (row // 8) + offset + t)).astype(BF16)


def pack(piv, cu, cv, ru, rv, cbu, cbv, rank_c, rank_r, rank_b, send, col_u):
    level = iota((64, RANK), 1)
    even = onehot(0)
    odd = onehot(6)

    def panel(ref, rank):
        x = jnp.where(level < rank, ref[...].astype(F32), 0.0).astype(BF16)
        return jnp.concatenate([dot(even, x, (1, 1)), dot(odd, x, (1, 1))], axis=1)

    col_u[...] = panel(cu, rank_c[...]).astype(BF16)
    col_v = panel(cv, rank_c[...])
    row_u = panel(ru, rank_r[...])
    row_v = panel(rv, rank_r[...]).astype(BF16)
    r = lax.axis_index("row")
    q = r * N + lax.axis_index("col")
    full = piv[...]
    on_diag = iota((8, TILE), 1) == 8 * q + iota((8, TILE), 0)
    diag = jnp.sum(jnp.where(on_diag, full, 0.0), axis=1, keepdims=True)
    off = jnp.where(on_diag, 0.0, full)
    lane = iota((8, 128), 1)
    sub = iota((8, 128), 0)
    here = 8 * lax.axis_index("col") + sub
    high = diag.astype(BF16).astype(F32)
    rest = diag - high
    mid = rest.astype(BF16).astype(F32)
    low = rest - mid
    zero = jnp.zeros((8, 128), F32)
    first = jnp.where(lane == here, high, jnp.where(lane == 64 + here, mid, zero))
    first = jnp.sum(first, axis=0, keepdims=True)
    last = jnp.sum(jnp.where(lane == here, low, zero), axis=0, keepdims=True)
    parts = jnp.where(sub == 6, first, jnp.where(sub == 7, last, zero))
    pivot = [off[:, 128 * m : 128 * m + 128] for m in range(4)]
    wide = iota((RANK, TILE), 0)
    row = iota((64, RANK), 0)
    lev = iota((64, RANK), 1)
    t = row % 8
    extra = [
        ((t >= 6) & (lev == 64 + 4 * (row // 8) + 2 * e + t - 6)).astype(BF16) for e in range(2)
    ]
    from_lane = iota((128, 128), 0)
    to_lane = iota((128, 128), 1)
    same = (from_lane // 64 == to_lane // 64) & ((to_lane // 8) % 8 == r)
    thin = []
    for g in range(N):
        move = same & (from_lane % 64 == 8 * g + to_lane % 8)
        thin.append(dot(row_v, move.astype(BF16), (1, 0)))
    for side, ref in enumerate((cbu, cbv)):
        x = jnp.where(wide < rank_b[0], ref[...].astype(F32), 0.0)
        narrow = x.astype(BF16)
        x1 = dot(extra[0], narrow, (1, 0))
        x2 = dot(extra[1], narrow, (1, 0))
        for g in range(N):
            rows = slice(8 * g, 8 * g + 8)
            for m in range(4):
                lanes = slice(128 * m, 128 * m + 128)
                c = 2 * m + side
                send[g * N + c] = jnp.concatenate(
                    [
                        x[rows, lanes],
                        col_v[rows] + x1[rows, lanes],
                        row_u[8 * c : 8 * c + 8] + x2[rows, lanes],
                    ]
                    + pivot
                    + [thin[g][8 * c : 8 * c + 8] + parts],
                    axis=0,
                ).astype(BF16)


def slots(got, mapping, send, inverse):
    fill_inverse(mapping, inverse)
    here = lax.axis_index("row")
    for s in range(2):
        at = inverse[2 * here + s]
        x = got[jnp.minimum(at, N - 1)].astype(F32)
        x = jnp.where(at < N, x, jnp.zeros_like(x)).astype(BF16)
        send[64 * s : 64 * s + 64, :] = x


def spread(tiles):
    lane = iota(tiles[0].shape, 1)
    halves = ([], [])
    for m in range(N // 2):
        x, y = tiles[2 * m], tiles[2 * m + 1]
        halves[0].append(jnp.where(lane < 64, x, pltpu.roll(y, 64, 1)))
        halves[1].append(jnp.where(lane < 64, pltpu.roll(x, 64, 1), y))
    return [jnp.concatenate(h, axis=1) for h in halves]


def route(got, mapping, send, inverse, t0, g0, g1, lower_ref, right_ref, tail_ref):
    fill_inverse(mapping, inverse)
    sub = iota((8, 128), 0)
    valid = sub < 6
    zero = jnp.zeros((8, 128), F32)
    t0[64] = zero
    g0[64] = zero
    g1[64] = zero
    left = [[], []]
    diag = []
    right = [[] for _ in range(N)]
    thin = [zero] * N
    for i in range(N):
        row_tiles = []
        total = zero
        for j in range(N):
            k = i * N + j
            x = got[k, 0:24, :].astype(F32)
            a, b = x[8:16], x[16:24]
            t0[k] = x[0:8]
            g0[k] = jnp.where(sub >= 6, a, jnp.where(sub >= 4, pltpu.roll(b, 6, 0), 0.0))
            g1[k] = jnp.where(
                sub >= 4, 0.0, jnp.where(sub >= 2, pltpu.roll(a, 4, 0), pltpu.roll(b, 2, 0))
            )
            row_tiles.append(jnp.where(valid, a, 0.0))
            right[j].append(jnp.where(valid, b, 0.0))
            tail = got[k, 56:64, :].astype(F32)
            thin[j] = thin[j] + jnp.where(valid, tail, 0.0)
            total = total + tail
        parts = spread(row_tiles)
        left[0].append(parts[0])
        left[1].append(parts[1])
        top = total[6:7]
        diag.append(top + pltpu.roll(top, 64, 1) + total[7:8])
    lane = iota((1, 128), 1)
    inv = jnp.concatenate(
        [
            jnp.where(lane < 64, diag[2 * m], pltpu.roll(diag[2 * m + 1], 64, 1))
            for m in range(4)
        ],
        axis=1,
    )
    inv = 1.0 / inv
    off = jnp.concatenate(
        [
            got[:, 24 + 8 * m : 32 + 8 * m, :].astype(F32).reshape(TILE, 128).astype(BF16)
            for m in range(4)
        ],
        axis=1,
    )

    def times(x):
        high = x.astype(BF16)
        low = (x - high.astype(F32)).astype(BF16)
        both = dot(jnp.concatenate([high, low], axis=0), off, (1, 0))
        return (both[:128] + both[128:]) * inv

    v = jnp.concatenate(left[0] + left[1], axis=0) * inv
    y = v - times(v)
    z = y + times(y)
    lower = 2.0 * y - z + times(z)
    for k in range(2 * N):
        lower_ref[k] = lower[8 * k : 8 * k + 8]
    lower_ref[2 * N] = jnp.zeros((8, TILE), F32)
    right_ref[2 * N] = jnp.zeros((8, TILE), F32)
    for j in range(N):
        parts = spread(right[j])
        right_ref[2 * j] = parts[0]
        right_ref[2 * j + 1] = parts[1]
        tail_ref[j] = thin[j]
    tail_ref[N] = zero
    rows = []
    for half in range(2):
        for s in range(2):
            for r in range(N):
                i = inverse[2 * r + s]
                rows.append(lower_ref[jnp.where(i < N, half * N + i, 2 * N)])
    cols = []
    for k in range(2 * N):
        j = inverse[k]
        for half in range(2):
            cols.append(right_ref[jnp.where(j < N, 2 * j + half, 2 * N)])
    core = dot(
        jnp.concatenate(rows, axis=0).astype(BF16), jnp.concatenate(cols, axis=0).astype(BF16), (1, 1)
    )
    core = core.astype(BF16).astype(F32)
    group = iota((64, 128), 1) // 16
    for k in range(2 * N):
        c, h = k // 2, k % 2
        total = jnp.zeros((64, 128), F32)
        for combo in range(4):
            x = core[64 * combo : 64 * combo + 64, 128 * (k // 8) : 128 * (k // 8) + 128]
            shift = (16 * combo - 16 * (k % 8)) % 128
            total = jnp.where(group == combo, pltpu.roll(x, shift, 1) if shift else x, total)
        j = inverse[k]
        tail = tail_ref[j]
        for r in range(N):
            i0 = inverse[2 * r]
            i1 = inverse[2 * r + 1]
            at0 = jnp.where((i0 < N) & (j < N), i0 * N + j, 64)
            at1 = jnp.where((i1 < N) & (j < N), i1 * N + j, 64)
            send[(h * N + r) * N + c] = jnp.concatenate(
                [t0[at0], t0[at1], g0[at0] + g1[at1], tail, total[8 * r : 8 * r + 8]], axis=0
            ).astype(BF16)


def finish(blocks, col_in, out):
    lefts, rights = [], []
    for f in range(2):
        for side, into in ((0, lefts), (1, rights)):
            lanes = []
            for m in range(4):
                c = 2 * m + side
                lanes.append(
                    jnp.concatenate(
                        [blocks[f * 64 + g * N + c, 0:24, :].astype(F32) for g in range(N)], axis=0
                    )
                )
            into.append(jnp.concatenate(lanes, axis=1))
    left = jnp.concatenate(lefts, axis=0)
    row = iota(left.shape, 0) % 24
    of_slot = (
        (row < 8) | (row >= 20),
        (row >= 8) & (row < 20),
    )
    group = iota((64, 128), 1) // 16
    updates = [[], []]
    mixed = []
    for f in range(2):
        parts = [
            jnp.concatenate(
                [blocks[f * 64 + g * N + c, 32:40, :].astype(F32) for g in range(N)], axis=0
            )
            for c in range(N)
        ]
        for s in range(2):
            halves = []
            for half in range(2):
                total = jnp.zeros((64, 128), F32)
                combo = 2 * half + s
                for c in range(N):
                    shift = (16 * c - 16 * combo) % 128
                    x = pltpu.roll(parts[c], shift, 1) if shift else parts[c]
                    total = jnp.where(group == c, x, total)
                halves.append(total)
            core = jnp.concatenate(halves, axis=0).astype(BF16)
            col_u = spread(
                [
                    col_in[(f * N + c) * 128 + 64 * s : (f * N + c) * 128 + 64 * s + 64, :].astype(F32)
                    for c in range(N)
                ]
            )
            col_u = jnp.concatenate(col_u, axis=0).astype(BF16)
            updates[s].append(-dot(core, col_u, (0, 0)))
        for c in range(N):
            mixed += spread([blocks[f * 64 + g * N + c, 24:32, :].astype(F32) for g in range(N)])
    k = iota((TILE, TILE), 0)
    target = 64 * ((k // 8) % 8) + 8 * (k // 64) + k % 8
    order = (target == iota((TILE, TILE), 1)).astype(BF16)
    row_v = dot(jnp.concatenate(mixed, axis=0).astype(BF16), order, (1, 0))
    right = jnp.concatenate(rights + [row_v], axis=0).astype(BF16)
    for s in range(2):
        both = jnp.concatenate([jnp.where(of_slot[s], left, 0.0)] + updates[s], axis=0).astype(BF16)
        out[s] = dot(both, right, (0, 0)).astype(BF16)


def exchange(x, axes):
    return lax.all_to_all(x, axes, split_axis=0, concat_axis=0, tiled=True)


def collect(x, axes):
    return lax.all_gather(x, axes, axis=0, tiled=True)


def shards(
    pivot, col_ut, col_vt, col_rank, row_ut, row_vt, row_rank, cb_ut, cb_vt, cb_rank, parent_map
):
    sds = jax.ShapeDtypeStruct
    send, col_u = call(
        pack,
        (sds((64, 64, 128), BF16), sds((64, 128), BF16)),
        (
            pivot[0],
            col_ut[0, 0].T,
            col_vt[0, 0].T,
            row_ut[0, 0].T,
            row_vt[0, 0].T,
            cb_ut[0, 0, 0],
            cb_vt[0, 0, 0],
            col_rank,
            row_rank,
            cb_rank,
        ),
        (VMEM,) * 10,
    )
    got = exchange(send, ("row", "col"))
    col_rows = collect(col_u, "row")
    (col_slots,) = call(
        slots,
        (sds((128, 128), BF16),),
        (col_rows.reshape(N, 64, 128), parent_map),
        (VMEM, SMEM),
        (SMEM((2 * N,), jnp.int32),),
    )
    (send_f,) = call(
        route,
        (sds((128, 40, 128), BF16),),
        (got, parent_map),
        (VMEM, SMEM),
        (SMEM((2 * N,), jnp.int32),)
        + (VMEM((65, 8, 128), F32),) * 3
        + (VMEM((2 * N + 1, 8, TILE), F32),) * 2
        + (VMEM((N + 1, 8, 128), F32),),
    )
    blocks = exchange(send_f, ("side", "row", "col"))
    col_in = collect(col_slots, ("side", "col"))
    (out,) = call(finish, (sds((2, TILE, TILE), BF16),), (blocks, col_in), (VMEM,) * 2)
    return out[None, :, None]


def solution(mesh):
    front = ("pair", "side")
    split = Mesh(mesh.devices.reshape(4, 2, N, N), ("pair", "side", "row", "col"))
    placed = (
        P(front, ("row", "col"), None),
        P(front, "row", None, "col"),
        P(front, "row", None, "col"),
        P(front, "row"),
        P(front, "col", None, "row"),
        P(front, "col", None, "row"),
        P(front, "col"),
        P(front, "row", "col", None, None),
        P(front, "row", "col", None, None),
        P(front, "row", "col"),
        P(front, None),
    )

    return jax.shard_map(
        shards,
        mesh=split,
        in_specs=placed,
        out_specs=P(front, "row", "col", None, None),
        check_vma=False,
    )
```

```python
import jax
import jax.numpy as jnp
from jax import lax
from jax.experimental import pallas as pl
from jax.experimental.pallas import tpu as pltpu
from jax.sharding import Mesh, PartitionSpec as P

F32 = jnp.float32
BF16 = jnp.bfloat16
RANK = 96
TILE = 512
N = 8
SMEM = pltpu.SMEM
VMEM = pltpu.VMEM


def iota(shape, dim):
    return lax.broadcasted_iota(jnp.int32, shape, dim)


def dot(a, b, contract):
    return lax.dot_general(
        a, b, ((contract[:1], contract[1:]), ((), ())), preferred_element_type=F32
    )


def call(body, outs, args, specs, scratch=(), name=None):
    kernel = pl.pallas_call(
        body,
        out_shape=outs,
        in_specs=[pl.BlockSpec(memory_space=s) for s in specs],
        out_specs=[pl.BlockSpec(memory_space=VMEM) for _ in outs],
        scratch_shapes=scratch,
        name=name,
    )
    with jax.named_scope("do_" + name):
        return kernel(*args)


def fill_inverse(mapping, inverse):
    for k in range(2 * N):
        inverse[k] = N
    for k in range(N):
        inverse[mapping[0, k]] = k


def onehot(offset):
    row = iota((64, RANK), 0)
    level = iota((64, RANK), 1)
    t = row % 8
    return ((t < 6) & (level == 12 * (row // 8) + offset + t)).astype(BF16)


def pack(piv, cu, cv, ru, rv, cbu, cbv, rank_c, rank_r, rank_b, send):
    level = iota((64, RANK), 1)
    even = onehot(0)
    odd = onehot(6)

    def panel(ref, rank):
        x = jnp.where(level < rank, ref[...].astype(F32), 0.0).astype(BF16)
        return jnp.concatenate([dot(even, x, (1, 1)), dot(odd, x, (1, 1))], axis=1)

    col_u = panel(cu, rank_c[0, 0]).astype(BF16)
    col_v = panel(cv, rank_c[0, 0])
    row_u = panel(ru, rank_r[0, 0])
    row_v = panel(rv, rank_r[0, 0]).astype(BF16)
    r = lax.axis_index("row")
    c0 = lax.axis_index("col")
    q = r * N + c0
    full = piv[...]
    on_diag = iota((8, TILE), 1) == 8 * q + iota((8, TILE), 0)
    diag = jnp.sum(jnp.where(on_diag, full, 0.0), axis=1, keepdims=True)
    off = jnp.where(on_diag, 0.0, full)
    lane = iota((8, 128), 1)
    sub = iota((8, 128), 0)
    here = 8 * c0 + sub
    high = diag.astype(BF16).astype(F32)
    rest = diag - high
    mid = rest.astype(BF16).astype(F32)
    low = rest - mid
    zero = jnp.zeros((8, 128), F32)
    first = jnp.where(lane == here, high, jnp.where(lane == 64 + here, mid, zero))
    first = jnp.sum(first, axis=0, keepdims=True)
    last = jnp.sum(jnp.where(lane == here, low, zero), axis=0, keepdims=True)
    parts = jnp.where(sub == 6, first, jnp.where(sub == 7, last, zero))
    pivot = [off[:, 128 * m : 128 * m + 128] for m in range(4)]
    wide = iota((RANK, TILE), 0)
    row = iota((64, RANK), 0)
    lev = iota((64, RANK), 1)
    t = row % 8
    extra = [
        ((t >= 6) & (lev == 64 + 4 * (row // 8) + 2 * e + t - 6)).astype(BF16) for e in range(2)
    ]
    from_lane = iota((128, 128), 0)
    to_lane = iota((128, 128), 1)
    col_group = (c0 + jnp.where(c0 == r, 1, 0)) % N
    same = from_lane // 64 == to_lane // 64
    to_group = (to_lane // 8) % 8
    thin = []
    for g in range(N):
        move = same & (from_lane % 64 == 8 * g + to_lane % 8)
        thin.append(
            (
                dot(row_v, (move & (to_group == r)).astype(BF16), (1, 0)),
                dot(col_u, (move & (to_group == col_group)).astype(BF16), (1, 0)),
            )
        )
    for side, ref in enumerate((cbu, cbv)):
        x = jnp.where(wide < rank_b[0, 0, 0], ref[...].astype(F32), 0.0)
        narrow = x.astype(BF16)
        x1 = dot(extra[0], narrow, (1, 0))
        x2 = dot(extra[1], narrow, (1, 0))
        for g in range(N):
            rows = slice(8 * g, 8 * g + 8)
            for m in range(4):
                lanes = slice(128 * m, 128 * m + 128)
                c = 2 * m + side
                cols = slice(8 * c, 8 * c + 8)
                send[g * N + c] = jnp.concatenate(
                    [
                        x[rows, lanes],
                        col_v[rows] + x1[rows, lanes],
                        row_u[cols] + x2[rows, lanes],
                    ]
                    + pivot
                    + [thin[g][0][cols] + thin[c][1][rows] + parts],
                    axis=0,
                ).astype(BF16)


def spread(tiles):
    lane = iota(tiles[0].shape, 1)
    halves = ([], [])
    for m in range(N // 2):
        x, y = tiles[2 * m], tiles[2 * m + 1]
        halves[0].append(jnp.where(lane < 64, x, pltpu.roll(y, 64, 1)))
        halves[1].append(jnp.where(lane < 64, pltpu.roll(x, 64, 1), y))
    return [jnp.concatenate(h, axis=1) for h in halves]


def route(got, mapping, send, inverse, t0, g0, g1, lower_ref, right_ref, row_ref, col_ref):
    fill_inverse(mapping, inverse)
    sub = iota((8, 128), 0)
    valid = sub < 6
    zero = jnp.zeros((8, 128), F32)
    t0[64] = zero
    g0[64] = zero
    g1[64] = zero
    left = [[], []]
    diag = []
    right = [[] for _ in range(N)]
    thin = [zero] * N
    group = (iota((8, 128), 1) // 8) % 8
    for i in range(N):
        row_tiles = []
        total = zero
        thick = zero
        for j in range(N):
            k = i * N + j
            x = got[k, 0:24, :].astype(F32)
            a, b = x[8:16], x[16:24]
            t0[k] = x[0:8]
            g0[k] = jnp.where(sub >= 6, a, jnp.where(sub >= 4, pltpu.roll(b, 6, 0), 0.0))
            g1[k] = jnp.where(
                sub >= 4, 0.0, jnp.where(sub >= 2, pltpu.roll(a, 4, 0), pltpu.roll(b, 2, 0))
            )
            row_tiles.append(jnp.where(valid, a, 0.0))
            right[j].append(jnp.where(valid, b, 0.0))
            tail = got[k, 56:64, :].astype(F32)
            thin[j] = thin[j] + jnp.where(valid & (group == i), tail, 0.0)
            if i == j:
                x = jnp.where(valid & (group == (j + 1) % N), tail, 0.0)
                thick = thick + pltpu.roll(x, 56 if j == N - 1 else 120, 1)
            else:
                thick = thick + jnp.where(valid & (group == j), tail, 0.0)
            total = total + tail
        col_ref[i] = thick
        parts = spread(row_tiles)
        left[0].append(parts[0])
        left[1].append(parts[1])
        top = total[6:7]
        diag.append(top + pltpu.roll(top, 64, 1) + total[7:8])
    lane = iota((1, 128), 1)
    inv = jnp.concatenate(
        [
            jnp.where(lane < 64, diag[2 * m], pltpu.roll(diag[2 * m + 1], 64, 1))
            for m in range(4)
        ],
        axis=1,
    )
    inv = 1.0 / inv
    off = jnp.concatenate(
        [
            got[:, 24 + 8 * m : 32 + 8 * m, :].astype(F32).reshape(TILE, 128).astype(BF16)
            for m in range(4)
        ],
        axis=1,
    )

    def times(x):
        high = x.astype(BF16)
        low = (x - high.astype(F32)).astype(BF16)
        both = dot(jnp.concatenate([high, low], axis=0), off, (1, 0))
        return (both[:128] + both[128:]) * inv

    v = jnp.concatenate(left[0] + left[1], axis=0) * inv
    y = v - times(v)
    z = y + times(y)
    lower = 2.0 * y - z + times(z)
    for k in range(2 * N):
        lower_ref[k] = lower[8 * k : 8 * k + 8]
    lower_ref[2 * N] = jnp.zeros((8, TILE), F32)
    right_ref[2 * N] = jnp.zeros((8, TILE), F32)
    for j in range(N):
        parts = spread(right[j])
        right_ref[2 * j] = parts[0]
        right_ref[2 * j + 1] = parts[1]
        row_ref[j] = thin[j]
    row_ref[N] = zero
    col_ref[N] = zero
    rows = []
    for half in range(2):
        for s in range(2):
            for r in range(N):
                i = inverse[2 * r + s]
                rows.append(lower_ref[jnp.where(i < N, half * N + i, 2 * N)])
    cols = []
    for k in range(2 * N):
        j = inverse[k]
        for half in range(2):
            cols.append(right_ref[jnp.where(j < N, 2 * j + half, 2 * N)])
    core = dot(
        jnp.concatenate(rows, axis=0).astype(BF16), jnp.concatenate(cols, axis=0).astype(BF16), (1, 1)
    )
    core = core.astype(BF16).astype(F32)
    group = iota((64, 128), 1) // 16
    for k in range(2 * N):
        c, h = k // 2, k % 2
        total = jnp.zeros((64, 128), F32)
        for combo in range(4):
            x = core[64 * combo : 64 * combo + 64, 128 * (k // 8) : 128 * (k // 8) + 128]
            shift = (16 * combo - 16 * (k % 8)) % 128
            total = jnp.where(group == combo, pltpu.roll(x, shift, 1) if shift else x, total)
        j = inverse[k]
        tail = row_ref[j]
        for r in range(N):
            part = total[8 * r : 8 * r + 8]
            i0 = inverse[2 * r]
            i1 = inverse[2 * r + 1]
            at0 = jnp.where((i0 < N) & (j < N), i0 * N + j, 64)
            at1 = jnp.where((i1 < N) & (j < N), i1 * N + j, 64)
            send[(h * N + r) * N + c] = jnp.concatenate(
                [
                    t0[at0],
                    t0[at1],
                    g0[at0] + g1[at1],
                    jnp.where(valid, tail, pltpu.roll(part, 6, 0)),
                    jnp.where(valid, col_ref[i0], pltpu.roll(part, 4, 0)),
                    jnp.where(valid, col_ref[i1], pltpu.roll(part, 2, 0)),
                ],
                axis=0,
            ).astype(BF16)


def finish(blocks, out):
    def tile(f, g, c, at):
        return blocks[f * 64 + g * N + c, 8 * at : 8 * at + 8, :].astype(F32)

    lefts, rights = [], []
    for f in range(2):
        for side, into in ((0, lefts), (1, rights)):
            lanes = []
            for m in range(4):
                c = 2 * m + side
                lanes.append(
                    jnp.concatenate(
                        [blocks[f * 64 + g * N + c, 0:24, :].astype(F32) for g in range(N)], axis=0
                    )
                )
            into.append(jnp.concatenate(lanes, axis=1))
    left = jnp.concatenate(lefts, axis=0)
    row = iota(left.shape, 0) % 24
    of_slot = (
        (row < 8) | (row >= 20),
        (row >= 8) & (row < 20),
    )
    sub = iota((8, 128), 0)
    group = iota((64, 128), 1) // 16
    updates = [[], []]
    mixed = []
    for f in range(2):
        parts = []
        for c in range(N):
            rows = []
            for g in range(N):
                x = jnp.where(sub < 4, pltpu.roll(tile(f, g, c, 4), 4, 0), pltpu.roll(tile(f, g, c, 5), 6, 0))
                x = jnp.where(sub < 2, pltpu.roll(tile(f, g, c, 3), 2, 0), x)
                rows.append(jnp.where(sub < 6, x, 0.0))
            parts.append(jnp.concatenate(rows, axis=0))
        for s in range(2):
            halves = []
            for half in range(2):
                total = jnp.zeros((64, 128), F32)
                combo = 2 * half + s
                for c in range(N):
                    shift = (16 * c - 16 * combo) % 128
                    x = pltpu.roll(parts[c], shift, 1) if shift else parts[c]
                    total = jnp.where(group == c, x, total)
                halves.append(total)
            core = jnp.concatenate(halves, axis=0).astype(BF16)
            col_u = [[], []]
            for g in range(N):
                for half, x in enumerate(spread([tile(f, g, c, 4 + s) for c in range(N)])):
                    col_u[half].append(x)
            col_u = jnp.concatenate(col_u[0] + col_u[1], axis=0).astype(BF16)
            updates[s].append(-dot(core, col_u, (0, 0)))
        for c in range(N):
            mixed += spread([tile(f, g, c, 3) for g in range(N)])
    k = iota((TILE, TILE), 0)
    target = 64 * ((k // 8) % 8) + 8 * (k // 64) + k % 8
    order = (target == iota((TILE, TILE), 1)).astype(BF16)
    panels = jnp.concatenate(mixed + updates[0] + updates[1], axis=0).astype(BF16)
    panels = dot(panels, order, (1, 0))
    right = jnp.concatenate(rights + [panels[:256]], axis=0).astype(BF16)
    for s in range(2):
        update = panels[256 + 256 * s : 512 + 256 * s]
        both = jnp.concatenate([jnp.where(of_slot[s], left, 0.0), update], axis=0).astype(BF16)
        out[s] = dot(both, right, (0, 0)).astype(BF16)


def exchange(x, axes, name):
    with jax.named_scope(name):
        return lax.all_to_all(x, axes, split_axis=0, concat_axis=0, tiled=True)


def shards(
    pivot, col_ut, col_vt, col_rank, row_ut, row_vt, row_rank, cb_ut, cb_vt, cb_rank, parent_map
):
    sds = jax.ShapeDtypeStruct
    (send,) = call(
        pack,
        (sds((64, 64, 128), BF16),),
        (
            pivot[0],
            col_ut[0, 0].T,
            col_vt[0, 0].T,
            row_ut[0, 0].T,
            row_vt[0, 0].T,
            cb_ut[0, 0, 0],
            cb_vt[0, 0, 0],
            col_rank,
            row_rank,
            cb_rank,
        ),
        (VMEM,) * 7 + (SMEM,) * 3,
        name="pack",
    )
    got = exchange(send, ("row", "col"), "scatter")
    (send,) = call(
        route,
        (sds((128, 48, 128), BF16),),
        (got, parent_map),
        (VMEM, SMEM),
        (SMEM((2 * N,), jnp.int32),)
        + (VMEM((65, 8, 128), F32),) * 3
        + (VMEM((2 * N + 1, 8, TILE), F32),) * 2
        + (VMEM((N + 1, 8, 128), F32),) * 2,
        name="route",
    )
    blocks = exchange(send, ("side", "row", "col"), "gather")
    (out,) = call(finish, (sds((2, TILE, TILE), BF16),), (blocks,), (VMEM,), name="finish")
    return out[None, :, None]


def solution(mesh):
    front = ("pair", "side")
    split = Mesh(mesh.devices.reshape(4, 2, N, N), ("pair", "side", "row", "col"))
    placed = (
        P(front, ("row", "col"), None),
        P(front, "row", None, "col"),
        P(front, "row", None, "col"),
        P(front, "row"),
        P(front, "col", None, "row"),
        P(front, "col", None, "row"),
        P(front, "col"),
        P(front, "row", "col", None, None),
        P(front, "row", "col", None, None),
        P(front, "row", "col"),
        P(front, None),
    )

    return jax.shard_map(
        shards,
        mesh=split,
        in_specs=placed,
        out_specs=P(front, "row", "col", None, None),
        check_vma=False,
    )
```

```python
import jax
import jax.numpy as jnp
from jax import lax
from jax.experimental import pallas as pl
from jax.experimental.pallas import tpu as pltpu
from jax.sharding import Mesh, PartitionSpec as P

F32 = jnp.float32
BF16 = jnp.bfloat16
RANK = 96
TILE = 512
N = 8
SMEM = pltpu.SMEM
VMEM = pltpu.VMEM


def iota(shape, dim):
    return lax.broadcasted_iota(jnp.int32, shape, dim)


def dot(a, b, contract):
    return lax.dot_general(
        a, b, ((contract[:1], contract[1:]), ((), ())), preferred_element_type=F32
    )


def call(body, outs, args, specs, scratch=(), name=None):
    kernel = pl.pallas_call(
        body,
        out_shape=outs,
        in_specs=[pl.BlockSpec(memory_space=s) for s in specs],
        out_specs=[pl.BlockSpec(memory_space=VMEM) for _ in outs],
        scratch_shapes=scratch,
        name=name,
    )
    with jax.named_scope("do_" + name):
        return kernel(*args)


def fill_inverse(mapping, inverse):
    for k in range(2 * N):
        inverse[k] = N
    for k in range(N):
        inverse[mapping[0, k]] = k


def onehot(offset):
    row = iota((64, RANK), 0)
    level = iota((64, RANK), 1)
    t = row % 8
    return ((t < 6) & (level == 12 * (row // 8) + offset + t)).astype(BF16)


def pack(piv, cu, cv, ru, rv, cbu, cbv, rank_c, rank_r, rank_b, send):
    level = iota((64, RANK), 1)
    even = onehot(0)
    odd = onehot(6)

    def panel(ref, rank):
        x = jnp.where(level < rank, ref[...].astype(F32), 0.0).astype(BF16)
        return jnp.concatenate([dot(even, x, (1, 1)), dot(odd, x, (1, 1))], axis=1)

    col_u = panel(cu, rank_c[0, 0]).astype(BF16)
    col_v = panel(cv, rank_c[0, 0])
    row_u = panel(ru, rank_r[0, 0])
    row_v = panel(rv, rank_r[0, 0]).astype(BF16)
    r = lax.axis_index("row")
    c0 = lax.axis_index("col")
    q = r * N + c0
    full = piv[...]
    on_diag = iota((8, TILE), 1) == 8 * q + iota((8, TILE), 0)
    diag = jnp.sum(jnp.where(on_diag, full, 0.0), axis=1, keepdims=True)
    off = jnp.where(on_diag, 0.0, full)
    lane = iota((8, 128), 1)
    sub = iota((8, 128), 0)
    here = 8 * c0 + sub
    high = diag.astype(BF16).astype(F32)
    rest = diag - high
    mid = rest.astype(BF16).astype(F32)
    low = rest - mid
    zero = jnp.zeros((8, 128), F32)
    first = jnp.where(lane == here, high, jnp.where(lane == 64 + here, mid, zero))
    first = jnp.sum(first, axis=0, keepdims=True)
    last = jnp.sum(jnp.where(lane == here, low, zero), axis=0, keepdims=True)
    parts = jnp.where(sub == 6, first, jnp.where(sub == 7, last, zero))
    pivot = [off[:, 128 * m : 128 * m + 128] for m in range(4)]
    wide = iota((RANK, TILE), 0)
    row = iota((64, RANK), 0)
    lev = iota((64, RANK), 1)
    t = row % 8
    extra = [
        ((t >= 6) & (lev == 64 + 4 * (row // 8) + 2 * e + t - 6)).astype(BF16) for e in range(2)
    ]
    from_lane = iota((128, 128), 0)
    to_lane = iota((128, 128), 1)
    col_group = (c0 + jnp.where(c0 == r, 1, 0)) % N
    same = from_lane // 64 == to_lane // 64
    to_group = (to_lane // 8) % 8
    thin = []
    for g in range(N):
        move = same & (from_lane % 64 == 8 * g + to_lane % 8)
        thin.append(
            (
                dot(row_v, (move & (to_group == r)).astype(BF16), (1, 0)),
                dot(col_u, (move & (to_group == col_group)).astype(BF16), (1, 0)),
            )
        )
    for side, ref in enumerate((cbu, cbv)):
        x = jnp.where(wide < rank_b[0, 0, 0], ref[...].astype(F32), 0.0)
        narrow = x.astype(BF16)
        x1 = dot(extra[0], narrow, (1, 0))
        x2 = dot(extra[1], narrow, (1, 0))
        for g in range(N):
            rows = slice(8 * g, 8 * g + 8)
            for m in range(4):
                lanes = slice(128 * m, 128 * m + 128)
                c = 2 * m + side
                cols = slice(8 * c, 8 * c + 8)
                send[g * N + c] = jnp.concatenate(
                    [
                        x[rows, lanes],
                        col_v[rows] + x1[rows, lanes],
                        row_u[cols] + x2[rows, lanes],
                    ]
                    + pivot
                    + [thin[g][0][cols] + thin[c][1][rows] + parts],
                    axis=0,
                ).astype(BF16)


def spread(tiles):
    lane = iota(tiles[0].shape, 1)
    halves = ([], [])
    for m in range(N // 2):
        x, y = tiles[2 * m], tiles[2 * m + 1]
        halves[0].append(jnp.where(lane < 64, x, pltpu.roll(y, 64, 1)))
        halves[1].append(jnp.where(lane < 64, pltpu.roll(x, 64, 1), y))
    return [jnp.concatenate(h, axis=1) for h in halves]


def route(got, mapping, send, inverse, t0, g0, g1, lower_ref, right_ref, row_ref, col_ref):
    fill_inverse(mapping, inverse)
    sub = iota((8, 128), 0)
    valid = sub < 6
    zero = jnp.zeros((8, 128), F32)
    t0[64] = zero
    g0[64] = zero
    g1[64] = zero
    left = [[], []]
    diag = []
    right = [[] for _ in range(N)]
    thin = [zero] * N
    group = (iota((8, 128), 1) // 8) % 8
    for i in range(N):
        row_tiles = []
        total = zero
        thick = zero
        for j in range(N):
            k = i * N + j
            x = got[k, 0:24, :].astype(F32)
            a, b = x[8:16], x[16:24]
            t0[k] = x[0:8]
            g0[k] = jnp.where(sub >= 6, a, jnp.where(sub >= 4, pltpu.roll(b, 6, 0), 0.0))
            g1[k] = jnp.where(
                sub >= 4, 0.0, jnp.where(sub >= 2, pltpu.roll(a, 4, 0), pltpu.roll(b, 2, 0))
            )
            row_tiles.append(jnp.where(valid, a, 0.0))
            right[j].append(jnp.where(valid, b, 0.0))
            tail = got[k, 56:64, :].astype(F32)
            thin[j] = thin[j] + jnp.where(valid & (group == i), tail, 0.0)
            if i == j:
                x = jnp.where(valid & (group == (j + 1) % N), tail, 0.0)
                thick = thick + pltpu.roll(x, 56 if j == N - 1 else 120, 1)
            else:
                thick = thick + jnp.where(valid & (group == j), tail, 0.0)
            total = total + tail
        col_ref[i] = thick
        parts = spread(row_tiles)
        left[0].append(parts[0])
        left[1].append(parts[1])
        top = total[6:7]
        diag.append(top + pltpu.roll(top, 64, 1) + total[7:8])
    lane = iota((1, 128), 1)
    inv = jnp.concatenate(
        [
            jnp.where(lane < 64, diag[2 * m], pltpu.roll(diag[2 * m + 1], 64, 1))
            for m in range(4)
        ],
        axis=1,
    )
    inv = 1.0 / inv
    off = jnp.concatenate(
        [
            got[:, 24 + 8 * m : 32 + 8 * m, :].astype(F32).reshape(TILE, 128).astype(BF16)
            for m in range(4)
        ],
        axis=1,
    )

    def times(x):
        high = x.astype(BF16)
        low = (x - high.astype(F32)).astype(BF16)
        both = dot(jnp.concatenate([high, low], axis=0), off, (1, 0))
        return (both[:128] + both[128:]) * inv

    v = jnp.concatenate(left[0] + left[1], axis=0) * inv
    y = v - times(v)
    z = y + times(y)
    lower = 2.0 * y - z + times(z)
    for k in range(2 * N):
        lower_ref[k] = lower[8 * k : 8 * k + 8]
    lower_ref[2 * N] = jnp.zeros((8, TILE), F32)
    right_ref[2 * N] = jnp.zeros((8, TILE), F32)
    for j in range(N):
        parts = spread(right[j])
        right_ref[2 * j] = parts[0]
        right_ref[2 * j + 1] = parts[1]
        row_ref[j] = thin[j]
    row_ref[N] = zero
    col_ref[N] = zero
    rows = []
    for half in range(2):
        for s in range(2):
            for r in range(N):
                i = inverse[2 * r + s]
                rows.append(lower_ref[jnp.where(i < N, half * N + i, 2 * N)])
    cols = []
    for k in range(2 * N):
        j = inverse[k]
        for half in range(2):
            cols.append(right_ref[jnp.where(j < N, 2 * j + half, 2 * N)])
    core = dot(
        jnp.concatenate(rows, axis=0).astype(BF16), jnp.concatenate(cols, axis=0).astype(BF16), (1, 1)
    )
    core = core.astype(BF16).astype(F32)
    group = iota((64, 128), 1) // 16
    for k in range(2 * N):
        c, h = k // 2, k % 2
        total = jnp.zeros((64, 128), F32)
        for combo in range(4):
            x = core[64 * combo : 64 * combo + 64, 128 * (k // 8) : 128 * (k // 8) + 128]
            shift = (16 * combo - 16 * (k % 8)) % 128
            total = jnp.where(group == combo, pltpu.roll(x, shift, 1) if shift else x, total)
        j = inverse[k]
        tail = row_ref[j]
        for r in range(N):
            part = total[8 * r : 8 * r + 8]
            i0 = inverse[2 * r]
            i1 = inverse[2 * r + 1]
            at0 = jnp.where((i0 < N) & (j < N), i0 * N + j, 64)
            at1 = jnp.where((i1 < N) & (j < N), i1 * N + j, 64)
            send[(h * N + r) * N + c] = jnp.concatenate(
                [
                    t0[at0],
                    t0[at1],
                    g0[at0] + g1[at1],
                    jnp.where(valid, tail, pltpu.roll(part, 6, 0)),
                    jnp.where(valid, col_ref[i0], pltpu.roll(part, 4, 0)),
                    jnp.where(valid, col_ref[i1], pltpu.roll(part, 2, 0)),
                ],
                axis=0,
            ).astype(BF16)


def finish(blocks, out):
    def tile(f, g, c, at):
        return blocks[f * 64 + g * N + c, 8 * at : 8 * at + 8, :].astype(F32)

    lefts, rights = [], []
    for f in range(2):
        for side, into in ((0, lefts), (1, rights)):
            lanes = []
            for m in range(4):
                c = 2 * m + side
                lanes.append(
                    jnp.concatenate(
                        [blocks[f * 64 + g * N + c, 0:24, :].astype(F32) for g in range(N)], axis=0
                    )
                )
            into.append(jnp.concatenate(lanes, axis=1))
    left = jnp.concatenate(lefts, axis=0)
    row = iota(left.shape, 0) % 24
    of_slot = (
        (row < 8) | (row >= 20),
        (row >= 8) & (row < 20),
    )
    sub = iota((8, 128), 0)
    group = iota((64, 128), 1) // 16
    updates = [[], []]
    mixed = []
    for f in range(2):
        parts = []
        for c in range(N):
            rows = []
            for g in range(N):
                x = jnp.where(sub < 4, pltpu.roll(tile(f, g, c, 4), 4, 0), pltpu.roll(tile(f, g, c, 5), 6, 0))
                x = jnp.where(sub < 2, pltpu.roll(tile(f, g, c, 3), 2, 0), x)
                rows.append(jnp.where(sub < 6, x, 0.0))
            parts.append(jnp.concatenate(rows, axis=0))
        for s in range(2):
            halves = []
            for half in range(2):
                total = jnp.zeros((64, 128), F32)
                combo = 2 * half + s
                for c in range(N):
                    shift = (16 * c - 16 * combo) % 128
                    x = pltpu.roll(parts[c], shift, 1) if shift else parts[c]
                    total = jnp.where(group == c, x, total)
                halves.append(total)
            core = jnp.concatenate(halves, axis=0).astype(BF16)
            col_u = [[], []]
            for g in range(N):
                for half, x in enumerate(spread([tile(f, g, c, 4 + s) for c in range(N)])):
                    col_u[half].append(x)
            col_u = jnp.concatenate(col_u[0] + col_u[1], axis=0).astype(BF16)
            updates[s].append(-dot(core, col_u, (0, 0)))
        for c in range(N):
            mixed += spread([tile(f, g, c, 3) for g in range(N)])
    k = iota((TILE, TILE), 0)
    target = 64 * ((k // 8) % 8) + 8 * (k // 64) + k % 8
    order = (target == iota((TILE, TILE), 1)).astype(BF16)
    panels = jnp.concatenate(mixed + updates[0] + updates[1], axis=0).astype(BF16)
    panels = dot(panels, order, (1, 0))
    right = jnp.concatenate(rights + [panels[:256]], axis=0).astype(BF16)
    for s in range(2):
        update = panels[256 + 256 * s : 512 + 256 * s]
        both = jnp.concatenate([jnp.where(of_slot[s], left, 0.0), update], axis=0).astype(BF16)
        out[s] = dot(both, right, (0, 0)).astype(BF16)


def exchange(x, axes, name):
    with jax.named_scope(name):
        return lax.all_to_all(x, axes, split_axis=0, concat_axis=0, tiled=True)


def shards(
    pivot, col_ut, col_vt, col_rank, row_ut, row_vt, row_rank, cb_ut, cb_vt, cb_rank, parent_map
):
    sds = jax.ShapeDtypeStruct
    (send,) = call(
        pack,
        (VMEM((64, 64, 128), BF16),),
        (
            pivot[0],
            col_ut[0, 0].T,
            col_vt[0, 0].T,
            row_ut[0, 0].T,
            row_vt[0, 0].T,
            cb_ut[0, 0, 0],
            cb_vt[0, 0, 0],
            col_rank,
            row_rank,
            cb_rank,
        ),
        (VMEM,) * 7 + (SMEM,) * 3,
        name="pack",
    )
    got = exchange(send, ("row", "col"), "scatter")
    (send,) = call(
        route,
        (VMEM((128, 48, 128), BF16),),
        (got, parent_map),
        (VMEM, SMEM),
        (SMEM((2 * N,), jnp.int32),)
        + (VMEM((65, 8, 128), F32),) * 3
        + (VMEM((2 * N + 1, 8, TILE), F32),) * 2
        + (VMEM((N + 1, 8, 128), F32),) * 2,
        name="route",
    )
    blocks = exchange(send, ("side", "row", "col"), "gather")
    (out,) = call(finish, (sds((2, TILE, TILE), BF16),), (blocks,), (VMEM,), name="finish")
    return out[None, :, None]


def solution(mesh):
    front = ("pair", "side")
    split = Mesh(mesh.devices.reshape(4, 2, N, N), ("pair", "side", "row", "col"))
    placed = (
        P(front, ("row", "col"), None),
        P(front, "row", None, "col"),
        P(front, "row", None, "col"),
        P(front, "row"),
        P(front, "col", None, "row"),
        P(front, "col", None, "row"),
        P(front, "col"),
        P(front, "row", "col", None, None),
        P(front, "row", "col", None, None),
        P(front, "row", "col"),
        P(front, None),
    )

    return jax.shard_map(
        shards,
        mesh=split,
        in_specs=placed,
        out_specs=P(front, "row", "col", None, None),
        check_vma=False,
    )
```

```python
import jax
import jax.numpy as jnp
from jax import lax
from jax.experimental import pallas as pl
from jax.experimental.pallas import tpu as pltpu
from jax.sharding import Mesh, PartitionSpec as P

F32 = jnp.float32
BF16 = jnp.bfloat16
RANK = 96
TILE = 512
N = 8
SMEM = pltpu.SMEM
VMEM = pltpu.VMEM


def iota(shape, dim):
    return lax.broadcasted_iota(jnp.int32, shape, dim)


def dot(a, b, contract):
    return lax.dot_general(
        a, b, ((contract[:1], contract[1:]), ((), ())), preferred_element_type=F32
    )


def call(body, outs, args, specs, scratch=(), name=None, into=VMEM):
    kernel = pl.pallas_call(
        body,
        out_shape=outs,
        in_specs=[pl.BlockSpec(memory_space=s) for s in specs],
        out_specs=[pl.BlockSpec(memory_space=into) for _ in outs],
        scratch_shapes=scratch,
        name=name,
    )
    with jax.named_scope("do_" + name):
        return kernel(*args)


def fill_inverse(mapping, inverse):
    for k in range(2 * N):
        inverse[k] = N
    for k in range(N):
        inverse[mapping[0, k]] = k


def onehot(offset):
    row = iota((64, RANK), 0)
    level = iota((64, RANK), 1)
    t = row % 8
    return ((t < 6) & (level == 12 * (row // 8) + offset + t)).astype(BF16)


def pack(piv, cu, cv, ru, rv, cbu, cbv, rank_c, rank_r, rank_b, send):
    level = iota((64, RANK), 1)
    even = onehot(0)
    odd = onehot(6)

    def panel(ref, rank):
        x = jnp.where(level < rank, ref[...].astype(F32), 0.0).astype(BF16)
        return jnp.concatenate([dot(even, x, (1, 1)), dot(odd, x, (1, 1))], axis=1)

    col_u = panel(cu, rank_c[0, 0]).astype(BF16)
    col_v = panel(cv, rank_c[0, 0])
    row_u = panel(ru, rank_r[0, 0])
    row_v = panel(rv, rank_r[0, 0]).astype(BF16)
    first_half = iota((64, 128), 1) < 64
    col_v = (
        jnp.where(first_half, col_v, 0.0),
        jnp.where(first_half, pltpu.roll(col_v, 64, 1), 0.0),
    )
    q = lax.axis_index("row") * N + lax.axis_index("col")
    full = piv[...]
    on_diag = iota((8, TILE), 1) == 8 * q + iota((8, TILE), 0)
    diag = jnp.sum(jnp.where(on_diag, full, 0.0), axis=1, keepdims=True)
    off = jnp.where(on_diag, 0.0, full)
    high = diag.astype(BF16).astype(F32)
    rest = diag - high
    mid = rest.astype(BF16).astype(F32)
    lane = iota((8, 128), 1)
    sub = iota((8, 128), 0)
    parts = jnp.zeros((8, 128), F32)
    for k, x in enumerate((high, mid, rest - mid)):
        parts = jnp.where(lane == 96 + 8 * k + sub, x, parts)
    parts = jnp.where(sub == 0, jnp.sum(parts, axis=0, keepdims=True), 0.0)
    pivot = [off[:, 128 * m : 128 * m + 128] for m in range(4)]
    wide = iota((RANK, TILE), 0)
    row = iota((64, RANK), 0)
    lev = iota((64, RANK), 1)
    t = row % 8
    extra = [
        ((t >= 6) & (lev == 64 + 4 * (row // 8) + 2 * e + t - 6)).astype(BF16) for e in range(2)
    ]
    from_lane = iota((128, 128), 0)
    place = iota((128, 128), 1) - 8 * (from_lane // 64) - from_lane % 64
    inside = from_lane % 64 // 8
    thin = []
    for g in range(N):
        thin.append(
            [
                dot(x, ((inside == g) & (place == at - 8 * g)).astype(BF16), (1, 0))
                for x, at in ((row_v, 64), (col_u, 80))
            ]
        )
    for side, ref in enumerate((cbu, cbv)):
        x = jnp.where(wide < rank_b[0, 0, 0], ref[...].astype(F32), 0.0)
        narrow = x.astype(BF16)
        x1 = dot(extra[0], narrow, (1, 0))
        x2 = dot(extra[1], narrow, (1, 0))
        for g in range(N):
            rows = slice(8 * g, 8 * g + 8)
            for m in range(4):
                lanes = slice(128 * m, 128 * m + 128)
                c = 2 * m + side
                cols = slice(8 * c, 8 * c + 8)
                send[g * N + c] = jnp.concatenate(
                    [
                        x[rows, lanes],
                        row_u[cols] + x1[rows, lanes],
                        col_v[side][rows] + thin[g][0][cols] + thin[c][1][rows] + parts + x2[rows, lanes],
                        pivot[2 * side],
                        pivot[2 * side + 1],
                    ],
                    axis=0,
                ).astype(BF16)


def spread(tiles):
    lane = iota(tiles[0].shape, 1)
    halves = ([], [])
    for m in range(N // 2):
        x, y = tiles[2 * m], tiles[2 * m + 1]
        halves[0].append(jnp.where(lane < 64, x, pltpu.roll(y, 64, 1)))
        halves[1].append(jnp.where(lane < 64, pltpu.roll(x, 64, 1), y))
    return [jnp.concatenate(h, axis=1) for h in halves]


def route(
    got, other, mapping, send, inverse, t0, g0, g1, lower_ref, right_ref, row_ref, col_ref, off_ref
):
    fill_inverse(mapping, inverse)
    core_id = lax.axis_index("col") % 2
    sub = iota((8, 128), 0)
    lane = iota((8, 128), 1)
    valid = sub < 6
    zero = jnp.zeros((8, 128), F32)
    t0[64] = zero
    g0[64] = zero
    g1[64] = zero
    right = [[] for _ in range(N)]
    thin = [zero] * N
    diag = [zero] * 4
    group = lane // 8

    def move(x, start, to):
        return pltpu.roll(x, (to - start) % 128, 1) if (to - start) % 128 else x

    def halves(ref, i):
        x = [jnp.where(valid, ref[i * N + j, 16:24, :].astype(F32), 0.0) for j in range(N)]
        return jnp.concatenate(
            [jnp.where(lane < 64, x[2 * m], pltpu.roll(x[2 * m + 1], 64, 1)) for m in range(4)], axis=1
        )

    def columns(ref):
        return jnp.concatenate(
            [
                ref[:, 24 + 8 * m : 32 + 8 * m, :].astype(F32).reshape(TILE, 128).astype(BF16)
                for m in range(2)
            ],
            axis=1,
        )

    for i in range(N):
        thick = zero
        for j in range(N):
            k = i * N + j
            x = got[k, 0:24, :].astype(F32)
            a, b = x[8:16], x[16:24]
            t0[k] = x[0:8]
            g0[k] = jnp.where(sub >= 6, a, jnp.where(sub >= 4, pltpu.roll(b, 6, 0), 0.0))
            g1[k] = jnp.where(
                sub >= 4, 0.0, jnp.where(sub >= 2, pltpu.roll(a, 4, 0), pltpu.roll(b, 2, 0))
            )
            right[j].append(jnp.where(valid, a, 0.0))
            for half in range(2):
                thin[j] = jnp.where(group == 8 * half + i, move(b, 64 + 8 * half, 64 * half + 8 * i), thin[j])
                thick = jnp.where(group == 8 * half + j, move(b, 80 + 8 * half, 64 * half + 8 * j), thick)
            total = b + pltpu.roll(b, 120, 1) + pltpu.roll(b, 112, 1)
            to = 64 * (i % 2) + 8 * j
            diag[i // 2] = jnp.where(group == to // 8, move(total, 96, to), diag[i // 2])
        col_ref[i] = jnp.where(valid, thick, 0.0)
    left = [halves(got, i) for i in range(N)]
    off_ref[core_id] = columns(got)
    inv = 1.0 / jnp.concatenate([x[0:1] for x in diag], axis=1)
    left += [halves(other, i) for i in range(N)]
    off_ref[1 - core_id] = columns(other)
    off = jnp.concatenate([off_ref[0], off_ref[1]], axis=1)

    def times(x):
        high = x.astype(BF16)
        low = (x - high.astype(F32)).astype(BF16)
        both = dot(jnp.concatenate([high, low], axis=0), off, (1, 0))
        return (both[:128] + both[128:]) * inv

    v = jnp.concatenate(left, axis=0) * inv
    y = v - times(v)
    z = y + times(y)
    lower = 2.0 * y - z + times(z)
    for k in range(2 * N):
        lower_ref[k] = lower[8 * k : 8 * k + 8]
    lower_ref[2 * N] = jnp.zeros((8, TILE), F32)
    right_ref[2 * N] = jnp.zeros((8, TILE), F32)
    for j in range(N):
        parts = spread(right[j])
        right_ref[2 * j] = parts[0]
        right_ref[2 * j + 1] = parts[1]
        row_ref[j] = jnp.where(valid, thin[j], 0.0)
    row_ref[N] = zero
    col_ref[N] = zero
    rows = []
    for half in range(2):
        for s in range(2):
            for r in range(N):
                i = inverse[2 * r + s]
                at = jnp.bitwise_xor(half, core_id) * N + i
                rows.append(lower_ref[jnp.where(i < N, at, 2 * N)])
    cols = []
    for k in range(2 * N):
        j = inverse[k]
        for half in range(2):
            cols.append(right_ref[jnp.where(j < N, 2 * j + half, 2 * N)])
    core = dot(
        jnp.concatenate(rows, axis=0).astype(BF16), jnp.concatenate(cols, axis=0).astype(BF16), (1, 1)
    )
    core = core.astype(BF16).astype(F32)
    place = iota((64, 128), 1) // 16
    for k in range(2 * N):
        c, h = k // 2, k % 2
        total = jnp.zeros((64, 128), F32)
        for combo in range(4):
            x = core[64 * combo : 64 * combo + 64, 128 * (k // 8) : 128 * (k // 8) + 128]
            shift = (16 * combo - 16 * (k % 8)) % 128
            total = jnp.where(place == combo, pltpu.roll(x, shift, 1) if shift else x, total)
        j = inverse[k]
        tail = row_ref[j]
        for r in range(N):
            part = total[8 * r : 8 * r + 8]
            i0 = inverse[2 * r]
            i1 = inverse[2 * r + 1]
            at0 = jnp.where((i0 < N) & (j < N), i0 * N + j, 64)
            at1 = jnp.where((i1 < N) & (j < N), i1 * N + j, 64)
            send[(h * N + r) * N + c] = jnp.concatenate(
                [
                    t0[at0],
                    t0[at1],
                    g0[at0] + g1[at1],
                    jnp.where(valid, tail, pltpu.roll(part, 6, 0)),
                    jnp.where(valid, col_ref[i0], pltpu.roll(part, 4, 0)),
                    jnp.where(valid, col_ref[i1], pltpu.roll(part, 2, 0)),
                ],
                axis=0,
            ).astype(BF16)


def finish(source, out, blocks, made, sems):
    fetch = [
        pltpu.make_async_copy(source.at[64 * f : 64 * f + 64], blocks.at[64 * f : 64 * f + 64], sems.at[f])
        for f in range(2)
    ]
    for copy in fetch:
        copy.start()

    def tile(f, g, c, at):
        return blocks[f * 64 + g * N + c, 8 * at : 8 * at + 8, :].astype(F32)

    lefts, rights = [], []
    sub = iota((8, 128), 0)
    group = iota((64, 128), 1) // 16
    updates = [[], []]
    mixed = []
    k = iota((TILE, TILE), 0)
    target = 64 * ((k // 8) % 8) + 8 * (k // 64) + k % 8
    order = (target == iota((TILE, TILE), 1)).astype(BF16)
    for f in range(2):
        fetch[f].wait()
        for side, into in ((0, lefts), (1, rights)):
            lanes = []
            for m in range(4):
                c = 2 * m + side
                lanes.append(
                    jnp.concatenate(
                        [blocks[f * 64 + g * N + c, 0:24, :].astype(F32) for g in range(N)], axis=0
                    )
                )
            into.append(jnp.concatenate(lanes, axis=1))
        parts = []
        for c in range(N):
            rows = []
            for g in range(N):
                x = jnp.where(sub < 4, pltpu.roll(tile(f, g, c, 4), 4, 0), pltpu.roll(tile(f, g, c, 5), 6, 0))
                x = jnp.where(sub < 2, pltpu.roll(tile(f, g, c, 3), 2, 0), x)
                rows.append(jnp.where(sub < 6, x, 0.0))
            parts.append(jnp.concatenate(rows, axis=0))
        for s in range(2):
            halves = []
            for half in range(2):
                total = jnp.zeros((64, 128), F32)
                combo = 2 * half + s
                for c in range(N):
                    shift = (16 * c - 16 * combo) % 128
                    x = pltpu.roll(parts[c], shift, 1) if shift else parts[c]
                    total = jnp.where(group == c, x, total)
                halves.append(total)
            core = jnp.concatenate(halves, axis=0).astype(BF16)
            col_u = [[], []]
            for g in range(N):
                for half, x in enumerate(spread([tile(f, g, c, 4 + s) for c in range(N)])):
                    col_u[half].append(x)
            col_u = jnp.concatenate(col_u[0] + col_u[1], axis=0).astype(BF16)
            updates[s].append(-dot(core, col_u, (0, 0)))
        for c in range(N):
            mixed += spread([tile(f, g, c, 3) for g in range(N)])
    left = jnp.concatenate(lefts, axis=0)
    row = iota(left.shape, 0) % 24
    of_slot = (
        (row < 8) | (row >= 20),
        (row >= 8) & (row < 20),
    )
    panels = jnp.concatenate(mixed + updates[0] + updates[1], axis=0).astype(BF16)
    panels = dot(panels, order, (1, 0))
    right = jnp.concatenate(rights + [panels[:256]], axis=0).astype(BF16)
    stores = []
    for s in range(2):
        update = panels[256 + 256 * s : 512 + 256 * s]
        both = jnp.concatenate([jnp.where(of_slot[s], left, 0.0), update], axis=0).astype(BF16)
        for part in range(2):
            rows = slice(256 * part, 256 * part + 256)
            made[s, rows, :] = dot(both[:, rows], right, (0, 0)).astype(BF16)
            copy = pltpu.make_async_copy(made.at[s, rows], out.at[s, rows], sems.at[2 + 2 * s + part])
            copy.start()
            stores.append(copy)
    for copy in stores:
        copy.wait()


def exchange(x, axes, name):
    with jax.named_scope(name):
        return lax.all_to_all(x, axes, split_axis=0, concat_axis=0, tiled=True)


def in_vmem(x):
    return pltpu.with_memory_space_constraint(x, VMEM)


def shards(
    pivot, col_ut, col_vt, col_rank, row_ut, row_vt, row_rank, cb_ut, cb_vt, cb_rank, parent_map
):
    sds = jax.ShapeDtypeStruct
    (send,) = call(
        pack,
        (VMEM((64, 40, 128), BF16),),
        (
            pivot[0],
            col_ut[0, 0].T,
            col_vt[0, 0].T,
            row_ut[0, 0].T,
            row_vt[0, 0].T,
            cb_ut[0, 0, 0],
            cb_vt[0, 0, 0],
            col_rank,
            row_rank,
            cb_rank,
        ),
        (VMEM,) * 7 + (SMEM,) * 3,
        name="pack",
    )
    got = exchange(send, ("row", "col"), "scatter")
    twin = lax.ppermute(got, "col", [(k, k ^ 1) for k in range(N)])
    (send,) = call(
        route,
        (VMEM((128, 48, 128), BF16),),
        (in_vmem(got), in_vmem(twin), parent_map),
        (VMEM, VMEM, SMEM),
        (SMEM((2 * N,), jnp.int32),)
        + (VMEM((65, 8, 128), F32),) * 3
        + (VMEM((2 * N + 1, 8, TILE), F32),) * 2
        + (VMEM((N + 1, 8, 128), F32),) * 2
        + (VMEM((2, TILE, TILE // 2), BF16),),
        name="route",
    )
    blocks = exchange(send, ("side", "row", "col"), "gather")
    (out,) = call(
        finish,
        (sds((2, TILE, TILE), BF16),),
        (blocks,),
        (pl.ANY,),
        (
            VMEM((128, 48, 128), BF16),
            VMEM((2, TILE, TILE), BF16),
            pltpu.SemaphoreType.DMA((6,)),
        ),
        name="finish",
        into=pl.ANY,
    )
    return out[None, :, None]


def solution(mesh):
    front = ("pair", "side")
    split = Mesh(mesh.devices.reshape(4, 2, N, N), ("pair", "side", "row", "col"))
    placed = (
        P(front, ("row", "col"), None),
        P(front, "row", None, "col"),
        P(front, "row", None, "col"),
        P(front, "row"),
        P(front, "col", None, "row"),
        P(front, "col", None, "row"),
        P(front, "col"),
        P(front, "row", "col", None, None),
        P(front, "row", "col", None, None),
        P(front, "row", "col"),
        P(front, None),
    )

    return jax.shard_map(
        shards,
        mesh=split,
        in_specs=placed,
        out_specs=P(front, "row", "col", None, None),
        check_vma=False,
    )
```

```python
import jax
import jax.numpy as jnp
from jax import lax
from jax.experimental import pallas as pl
from jax.experimental.pallas import tpu as pltpu
from jax.sharding import Mesh, PartitionSpec as P

F32 = jnp.float32
BF16 = jnp.bfloat16
RANK = 96
TILE = 512
N = 8
SMEM = pltpu.SMEM
VMEM = pltpu.VMEM


def iota(shape, dim):
    return lax.broadcasted_iota(jnp.int32, shape, dim)


def dot(a, b, contract):
    return lax.dot_general(
        a, b, ((contract[:1], contract[1:]), ((), ())), preferred_element_type=F32
    )


def call(body, outs, args, specs, scratch=(), name=None, into=VMEM, limit=24 * 2**20):
    kernel = pl.pallas_call(
        body,
        out_shape=outs,
        in_specs=[pl.BlockSpec(memory_space=s) for s in specs],
        out_specs=[pl.BlockSpec(memory_space=into) for _ in outs],
        scratch_shapes=scratch,
        compiler_params=pltpu.CompilerParams(vmem_limit_bytes=limit),
        name=name,
    )
    with jax.named_scope("do_" + name):
        return kernel(*args)


def fill_inverse(mapping, inverse):
    for k in range(2 * N):
        inverse[k] = N
    for k in range(N):
        inverse[mapping[0, k]] = k


def onehot(offset):
    row = iota((64, RANK), 0)
    level = iota((64, RANK), 1)
    t = row % 8
    return ((t < 6) & (level == 12 * (row // 8) + offset + t)).astype(BF16)


def pack(piv, cu, cv, ru, rv, cbu, cbv, rank_c, rank_r, rank_b, send):
    level = iota((64, RANK), 1)
    even = onehot(0)
    odd = onehot(6)

    def panel(ref, rank):
        x = jnp.where(level < rank, ref[...].astype(F32), 0.0).astype(BF16)
        return jnp.concatenate([dot(even, x, (1, 1)), dot(odd, x, (1, 1))], axis=1)

    col_u = panel(cu, rank_c[0, 0]).astype(BF16)
    col_v = panel(cv, rank_c[0, 0])
    row_u = panel(ru, rank_r[0, 0])
    row_v = panel(rv, rank_r[0, 0]).astype(BF16)
    first_half = iota((64, 128), 1) < 64
    col_v = (
        jnp.where(first_half, col_v, 0.0),
        jnp.where(first_half, pltpu.roll(col_v, 64, 1), 0.0),
    )
    q = lax.axis_index("row") * N + lax.axis_index("col")
    full = piv[...]
    on_diag = iota((8, TILE), 1) == 8 * q + iota((8, TILE), 0)
    diag = jnp.sum(jnp.where(on_diag, full, 0.0), axis=1, keepdims=True)
    off = jnp.where(on_diag, 0.0, full)
    high = diag.astype(BF16).astype(F32)
    rest = diag - high
    mid = rest.astype(BF16).astype(F32)
    lane = iota((8, 128), 1)
    sub = iota((8, 128), 0)
    parts = jnp.zeros((8, 128), F32)
    for k, x in enumerate((high, mid, rest - mid)):
        parts = jnp.where(lane == 96 + 8 * k + sub, x, parts)
    parts = jnp.where(sub == 0, jnp.sum(parts, axis=0, keepdims=True), 0.0)
    pivot = [off[:, 128 * m : 128 * m + 128] for m in range(4)]
    wide = iota((RANK, TILE), 0)
    row = iota((64, RANK), 0)
    lev = iota((64, RANK), 1)
    t = row % 8
    extra = [
        ((t >= 6) & (lev == 64 + 4 * (row // 8) + 2 * e + t - 6)).astype(BF16) for e in range(2)
    ]
    from_lane = iota((128, 128), 0)
    place = iota((128, 128), 1) - 8 * (from_lane // 64) - from_lane % 64
    inside = from_lane % 64 // 8
    thin = []
    for g in range(N):
        thin.append(
            [
                dot(x, ((inside == g) & (place == at - 8 * g)).astype(BF16), (1, 0))
                for x, at in ((row_v, 64), (col_u, 80))
            ]
        )
    for side, ref in enumerate((cbu, cbv)):
        x = jnp.where(wide < rank_b[0, 0, 0], ref[...].astype(F32), 0.0)
        narrow = x.astype(BF16)
        x1 = dot(extra[0], narrow, (1, 0))
        x2 = dot(extra[1], narrow, (1, 0))
        for g in range(N):
            rows = slice(8 * g, 8 * g + 8)
            for m in range(4):
                lanes = slice(128 * m, 128 * m + 128)
                c = 2 * m + side
                cols = slice(8 * c, 8 * c + 8)
                send[g * N + c] = jnp.concatenate(
                    [
                        x[rows, lanes],
                        row_u[cols] + x1[rows, lanes],
                        col_v[side][rows] + thin[g][0][cols] + thin[c][1][rows] + parts + x2[rows, lanes],
                        pivot[2 * side],
                        pivot[2 * side + 1],
                    ],
                    axis=0,
                ).astype(BF16)


def spread(tiles):
    lane = iota(tiles[0].shape, 1)
    halves = ([], [])
    for m in range(N // 2):
        x, y = tiles[2 * m], tiles[2 * m + 1]
        halves[0].append(jnp.where(lane < 64, x, pltpu.roll(y, 64, 1)))
        halves[1].append(jnp.where(lane < 64, pltpu.roll(x, 64, 1), y))
    return [jnp.concatenate(h, axis=1) for h in halves]


def move(x, start, to):
    return pltpu.roll(x, (to - start) % 128, 1) if (to - start) % 128 else x


def panel_half(ref, i):
    sub = iota((8, 128), 0)
    lane = iota((8, 128), 1)
    x = [jnp.where(sub < 6, ref[i * N + j, 16:24, :].astype(F32), 0.0) for j in range(N)]
    return jnp.concatenate(
        [jnp.where(lane < 64, x[2 * m], pltpu.roll(x[2 * m + 1], 64, 1)) for m in range(4)], axis=1
    )


def pivot_half(ref):
    return jnp.concatenate(
        [
            ref[:, 24 + 8 * m : 32 + 8 * m, :].astype(F32).reshape(TILE, 128).astype(BF16)
            for m in range(2)
        ],
        axis=1,
    )


def sort(got, mapping, t0, g0, g1, left, right_ref, row_ref, pair_ref, off, inv, inverse, col_ref):
    fill_inverse(mapping, inverse)
    sub = iota((8, 128), 0)
    lane = iota((8, 128), 1)
    valid = sub < 6
    zero = jnp.zeros((8, 128), F32)
    t0[64] = zero
    g0[64] = zero
    g1[64] = zero
    right = [[] for _ in range(N)]
    thin = [zero] * N
    diag = [zero] * 4
    group = lane // 8
    for i in range(N):
        thick = zero
        for j in range(N):
            k = i * N + j
            x = got[k, 0:24, :].astype(F32)
            a, b = x[8:16], x[16:24]
            t0[k] = x[0:8]
            g0[k] = jnp.where(sub >= 6, a, jnp.where(sub >= 4, pltpu.roll(b, 6, 0), 0.0))
            g1[k] = jnp.where(
                sub >= 4, 0.0, jnp.where(sub >= 2, pltpu.roll(a, 4, 0), pltpu.roll(b, 2, 0))
            )
            right[j].append(jnp.where(valid, a, 0.0))
            for half in range(2):
                thin[j] = jnp.where(group == 8 * half + i, move(b, 64 + 8 * half, 64 * half + 8 * i), thin[j])
                thick = jnp.where(group == 8 * half + j, move(b, 80 + 8 * half, 64 * half + 8 * j), thick)
            total = b + pltpu.roll(b, 120, 1) + pltpu.roll(b, 112, 1)
            to = 64 * (i % 2) + 8 * j
            diag[i // 2] = jnp.where(group == to // 8, move(total, 96, to), diag[i // 2])
        col_ref[i] = jnp.where(valid, thick, 0.0)
        left[8 * i : 8 * i + 8, :] = panel_half(got, i)
    col_ref[N] = zero
    for r in range(N):
        x = col_ref[inverse[2 * r]]
        y = col_ref[inverse[2 * r + 1]]
        pair_ref[2 * r] = jnp.where(lane < 64, x, pltpu.roll(y, 64, 1))
        pair_ref[2 * r + 1] = jnp.where(lane < 64, pltpu.roll(x, 64, 1), y)
    off[...] = pivot_half(got)
    full = 1.0 / jnp.concatenate([x[0:1] for x in diag], axis=1)
    inv[...] = jnp.broadcast_to(full, (8, TILE))
    right_ref[2 * N] = jnp.zeros((8, TILE), F32)
    row_ref[N] = zero
    for j in range(N):
        parts = spread(right[j])
        right_ref[2 * j] = parts[0]
        right_ref[2 * j + 1] = parts[1]
        row_ref[j] = jnp.where(valid, thin[j], 0.0)


def route(
    other, t0, g0, g1, left, right_ref, row_ref, pair_ref, off, inv, mapping, send, inverse, lower_ref, off_ref
):
    fill_inverse(mapping, inverse)
    core_id = lax.axis_index("col") % 2
    sub = iota((8, 128), 0)
    valid = sub < 6
    off_ref[core_id] = off[...]
    off_ref[1 - core_id] = pivot_half(other)
    whole = jnp.concatenate([off_ref[0], off_ref[1]], axis=1)
    scale = inv[0:1, :]

    def times(x):
        high = x.astype(BF16)
        low = (x - high.astype(F32)).astype(BF16)
        both = dot(jnp.concatenate([high, low], axis=0), whole, (1, 0))
        return (both[:128] + both[128:]) * scale

    v = jnp.concatenate([left[...]] + [panel_half(other, i) for i in range(N)], axis=0) * scale
    y = v - times(v)
    z = y + times(y)
    lower = 2.0 * y - z + times(z)
    for k in range(2 * N):
        lower_ref[k] = lower[8 * k : 8 * k + 8]
    lower_ref[2 * N] = jnp.zeros((8, TILE), F32)
    rows = []
    for half in range(2):
        for s in range(2):
            for r in range(N):
                i = inverse[2 * r + s]
                at = jnp.bitwise_xor(half, core_id) * N + i
                rows.append(lower_ref[jnp.where(i < N, at, 2 * N)])
    cols = []
    for k in range(2 * N):
        j = inverse[k]
        for half in range(2):
            cols.append(right_ref[jnp.where(j < N, 2 * j + half, 2 * N)])
    core = dot(
        jnp.concatenate(rows, axis=0).astype(BF16), jnp.concatenate(cols, axis=0).astype(BF16), (1, 1)
    )
    core = core.astype(BF16).astype(F32)
    place = iota((64, 128), 1) // 16
    low_lanes = iota((8, 128), 1) < 64
    for k in range(2 * N):
        c, h = k // 2, k % 2
        total = jnp.zeros((64, 128), F32)
        for combo in range(4):
            x = core[64 * combo : 64 * combo + 64, 128 * (k // 8) : 128 * (k // 8) + 128]
            total = jnp.where(place == combo, move(x, 16 * (k % 8), 16 * combo), total)
        beside = pltpu.roll(total, 64, 1)
        j = inverse[k]
        tail = row_ref[j]
        for r in range(N):
            part = total[8 * r : 8 * r + 8]
            shifted = beside[8 * r : 8 * r + 8]
            i0 = inverse[2 * r]
            i1 = inverse[2 * r + 1]
            at0 = jnp.where((i0 < N) & (j < N), i0 * N + j, 64)
            at1 = jnp.where((i1 < N) & (j < N), i1 * N + j, 64)
            spare = jnp.where(low_lanes, pltpu.roll(part, 6, 0), pltpu.roll(shifted, 4, 0))
            send[(h * N + r) * N + c] = jnp.concatenate(
                [
                    t0[at0],
                    t0[at1],
                    g0[at0] + g1[at1],
                    jnp.where(valid, tail, spare),
                    jnp.where(valid, pair_ref[2 * r + c % 2], pltpu.roll(part, 2, 0)),
                ],
                axis=0,
            ).astype(BF16)


def gather_up(blocks, lefts, rights, cores, order_out):
    def tile(f, g, c, at):
        return blocks[f * 64 + g * N + c, 8 * at : 8 * at + 8, :].astype(F32)

    k = iota((TILE, TILE), 0)
    target = 64 * ((k // 8) % 8) + 8 * (k // 64) + k % 8
    order = (target == iota((TILE, TILE), 1)).astype(BF16)
    order_out[...] = order
    sub = iota((8, 128), 0)
    group = iota((64, 128), 1) // 16
    core_id = lax.axis_index("col") % 2
    row = iota((192, TILE), 0) % 24
    of_slot = (
        (row < 8) | (row >= 20),
        (row >= 8) & (row < 20),
    )
    mixed = []
    for f in range(2):
        for side in range(2):
            lanes = []
            for m in range(4):
                c = 2 * m + side
                lanes.append(
                    jnp.concatenate(
                        [blocks[f * 64 + g * N + c, 0:24, :].astype(F32) for g in range(N)], axis=0
                    )
                )
            x = jnp.concatenate(lanes, axis=1)
            if side == 0:
                for s in range(2):
                    lefts[s, 192 * f : 192 * f + 192, :] = jnp.where(of_slot[s], x, 0.0).astype(BF16)
            else:
                rights[192 * f : 192 * f + 192, :] = x.astype(BF16)
        parts = []
        for c in range(N):
            rows = []
            for g in range(N):
                x = tile(f, g, c, 3)
                y = tile(f, g, c, 4)
                y = jnp.where(sub < 4, pltpu.roll(pltpu.roll(x, 64, 1), 4, 0), pltpu.roll(y, 6, 0))
                y = jnp.where(sub < 2, pltpu.roll(x, 2, 0), y)
                rows.append(jnp.where(sub < 6, y, 0.0))
            parts.append(jnp.concatenate(rows, axis=0))
        for s in range(2):
            halves = []
            for half in range(2):
                total = jnp.zeros((64, 128), F32)
                combo = 2 * half + s
                for c in range(N):
                    total = jnp.where(group == c, move(parts[c], 16 * combo, 16 * c), total)
                halves.append(total)
            first = jnp.where(core_id == 0, halves[0], halves[1])
            second = jnp.where(core_id == 0, halves[1], halves[0])
            cores[2 * f + s] = jnp.concatenate([first, second], axis=0).astype(BF16)
        for c in range(N):
            mixed += spread([tile(f, g, c, 3) for g in range(N)])
    row_v = jnp.concatenate(mixed, axis=0).astype(BF16)
    rights[384:640, :] = dot(row_v, order, (1, 0)).astype(BF16)


def finish(blocks, twin, lefts, rights, cores, order, out, made, sems):
    updates = [[], []]
    for f in range(2):
        col_u = [[], []]
        for ref in (blocks, twin):
            for g in range(N):
                at = f * 64 + g * N
                tiles = [ref[at + c, 32:40, :].astype(F32) for c in range(N)]
                for s, x in enumerate(spread(tiles)):
                    col_u[s].append(x)
        for s in range(2):
            x = jnp.concatenate(col_u[s], axis=0).astype(BF16)
            updates[s].append(-dot(cores[2 * f + s], x, (0, 0)))
    update = jnp.concatenate(updates[0] + updates[1], axis=0).astype(BF16)
    update = dot(update, order[...], (1, 0)).astype(BF16)
    right = rights[...]
    stores = []
    for s in range(2):
        both = jnp.concatenate([lefts[s], update[256 * s : 256 * s + 256]], axis=0)
        for part in range(2):
            rows = slice(256 * part, 256 * part + 256)
            made[s, rows, :] = dot(both[:, rows], right, (0, 0)).astype(BF16)
            copy = pltpu.make_async_copy(made.at[s, rows], out.at[s, rows], sems.at[2 * s + part])
            copy.start()
            stores.append(copy)
    for copy in stores:
        copy.wait()


def exchange(x, axes, name):
    with jax.named_scope(name):
        return lax.all_to_all(x, axes, split_axis=0, concat_axis=0, tiled=True)


def swap(x):
    return lax.ppermute(x, "col", [(k, k ^ 1) for k in range(N)])


def in_vmem(x):
    return pltpu.with_memory_space_constraint(x, VMEM)


def shards(
    pivot, col_ut, col_vt, col_rank, row_ut, row_vt, row_rank, cb_ut, cb_vt, cb_rank, parent_map
):
    sds = jax.ShapeDtypeStruct
    (send,) = call(
        pack,
        (VMEM((64, 40, 128), BF16),),
        (
            pivot[0],
            col_ut[0, 0].T,
            col_vt[0, 0].T,
            row_ut[0, 0].T,
            row_vt[0, 0].T,
            cb_ut[0, 0, 0],
            cb_vt[0, 0, 0],
            col_rank,
            row_rank,
            cb_rank,
        ),
        (VMEM,) * 7 + (SMEM,) * 3,
        name="pack",
        limit=None,
    )
    got = exchange(send, ("row", "col"), "scatter")
    got = in_vmem(got)
    other = in_vmem(swap(got))
    sorted_out = call(
        sort,
        (VMEM((65, 8, 128), F32),) * 3
        + (
            VMEM((64, TILE), F32),
            VMEM((2 * N + 1, 8, TILE), F32),
            VMEM((N + 1, 8, 128), F32),
            VMEM((2 * N, 8, 128), F32),
            VMEM((TILE, TILE // 2), BF16),
            VMEM((8, TILE), F32),
        ),
        (got, parent_map),
        (VMEM, SMEM),
        (SMEM((2 * N,), jnp.int32), VMEM((N + 1, 8, 128), F32)),
        name="sort",
    )
    (send,) = call(
        route,
        (VMEM((128, 40, 128), BF16),),
        (other, *(in_vmem(x) for x in sorted_out), parent_map),
        (VMEM,) * 10 + (SMEM,),
        (
            SMEM((2 * N,), jnp.int32),
            VMEM((2 * N + 1, 8, TILE), F32),
            VMEM((2, TILE, TILE // 2), BF16),
        ),
        name="route",
    )
    blocks = in_vmem(exchange(send, ("side", "row", "col"), "gather"))
    twin = in_vmem(swap(blocks))
    gathered = call(
        gather_up,
        (
            VMEM((2, 384, TILE), BF16),
            VMEM((640, TILE), BF16),
            VMEM((4, 128, 128), BF16),
            VMEM((TILE, TILE), BF16),
        ),
        (blocks,),
        (VMEM,),
        name="gather_up",
    )
    (out,) = call(
        finish,
        (sds((2, TILE, TILE), BF16),),
        (blocks, twin, *(in_vmem(x) for x in gathered)),
        (VMEM,) * 6,
        (
            VMEM((2, TILE, TILE), BF16),
            pltpu.SemaphoreType.DMA((4,)),
        ),
        name="finish",
        into=pl.ANY,
    )
    return out[None, :, None]


def solution(mesh):
    front = ("pair", "side")
    split = Mesh(mesh.devices.reshape(4, 2, N, N), ("pair", "side", "row", "col"))
    placed = (
        P(front, ("row", "col"), None),
        P(front, "row", None, "col"),
        P(front, "row", None, "col"),
        P(front, "row"),
        P(front, "col", None, "row"),
        P(front, "col", None, "row"),
        P(front, "col"),
        P(front, "row", "col", None, None),
        P(front, "row", "col", None, None),
        P(front, "row", "col"),
        P(front, None),
    )

    return jax.shard_map(
        shards,
        mesh=split,
        in_specs=placed,
        out_specs=P(front, "row", "col", None, None),
        check_vma=False,
    )
```

```python
import jax
import jax.numpy as jnp
from jax import lax
from jax.experimental import pallas as pl
from jax.experimental.pallas import tpu as pltpu
from jax.sharding import Mesh, PartitionSpec as P

F32 = jnp.float32
BF16 = jnp.bfloat16
RANK = 96
TILE = 512
N = 8
SMEM = pltpu.SMEM
VMEM = pltpu.VMEM


def iota(shape, dim):
    return lax.broadcasted_iota(jnp.int32, shape, dim)


def dot(a, b, contract):
    return lax.dot_general(
        a, b, ((contract[:1], contract[1:]), ((), ())), preferred_element_type=F32
    )


def call(body, outs, args, specs, scratch=(), name=None, into=VMEM, limit=24 * 2**20):
    kernel = pl.pallas_call(
        body,
        out_shape=outs,
        in_specs=[pl.BlockSpec(memory_space=s) for s in specs],
        out_specs=[pl.BlockSpec(memory_space=into) for _ in outs],
        scratch_shapes=scratch,
        compiler_params=pltpu.CompilerParams(vmem_limit_bytes=limit),
        name=name,
    )
    with jax.named_scope("do_" + name):
        return kernel(*args)


def fill_inverse(mapping, inverse):
    for k in range(2 * N):
        inverse[k] = N
    for k in range(N):
        inverse[mapping[0, k]] = k


def onehot(offset):
    row = iota((64, RANK), 0)
    level = iota((64, RANK), 1)
    t = row % 8
    return ((t < 6) & (level == 12 * (row // 8) + offset + t)).astype(BF16)


def pack(piv, cu, cv, ru, rv, cbu, cbv, rank_c, rank_r, rank_b, send):
    level = iota((64, RANK), 1)
    even = onehot(0)
    odd = onehot(6)

    def panel(ref, rank):
        x = jnp.where(level < rank, ref[...].astype(F32), 0.0).astype(BF16)
        return jnp.concatenate([dot(even, x, (1, 1)), dot(odd, x, (1, 1))], axis=1)

    col_u = panel(cu, rank_c[0, 0]).astype(BF16)
    col_v = panel(cv, rank_c[0, 0])
    row_u = panel(ru, rank_r[0, 0])
    row_v = panel(rv, rank_r[0, 0]).astype(BF16)
    first_half = iota((64, 128), 1) < 64
    col_v = (
        jnp.where(first_half, col_v, 0.0),
        jnp.where(first_half, pltpu.roll(col_v, 64, 1), 0.0),
    )
    q = lax.axis_index("row") * N + lax.axis_index("col")
    full = piv[...]
    on_diag = iota((8, TILE), 1) == 8 * q + iota((8, TILE), 0)
    diag = jnp.sum(jnp.where(on_diag, full, 0.0), axis=1, keepdims=True)
    off = jnp.where(on_diag, 0.0, full)
    high = diag.astype(BF16).astype(F32)
    rest = diag - high
    mid = rest.astype(BF16).astype(F32)
    lane = iota((8, 128), 1)
    sub = iota((8, 128), 0)
    parts = jnp.zeros((8, 128), F32)
    for k, x in enumerate((high, mid, rest - mid)):
        parts = jnp.where(lane == 96 + 8 * k + sub, x, parts)
    parts = jnp.where(sub == 0, jnp.sum(parts, axis=0, keepdims=True), 0.0)
    pivot = [off[:, 128 * m : 128 * m + 128] for m in range(4)]
    wide = iota((RANK, TILE), 0)
    row = iota((64, RANK), 0)
    lev = iota((64, RANK), 1)
    t = row % 8
    extra = [
        ((t >= 6) & (lev == 64 + 4 * (row // 8) + 2 * e + t - 6)).astype(BF16) for e in range(2)
    ]
    from_lane = iota((128, 128), 0)
    place = iota((128, 128), 1) - 8 * (from_lane // 64) - from_lane % 64
    inside = from_lane % 64 // 8
    thin = []
    for g in range(N):
        thin.append(
            [
                dot(x, ((inside == g) & (place == at - 8 * g)).astype(BF16), (1, 0))
                for x, at in ((row_v, 64), (col_u, 80))
            ]
        )
    for side, ref in enumerate((cbu, cbv)):
        x = jnp.where(wide < rank_b[0, 0, 0], ref[...].astype(F32), 0.0)
        narrow = x.astype(BF16)
        x1 = dot(extra[0], narrow, (1, 0))
        x2 = dot(extra[1], narrow, (1, 0))
        for g in range(N):
            rows = slice(8 * g, 8 * g + 8)
            for m in range(4):
                lanes = slice(128 * m, 128 * m + 128)
                c = 2 * m + side
                cols = slice(8 * c, 8 * c + 8)
                send[g * N + c] = jnp.concatenate(
                    [
                        x[rows, lanes],
                        row_u[cols] + x1[rows, lanes],
                        col_v[side][rows] + thin[g][0][cols] + thin[c][1][rows] + parts + x2[rows, lanes],
                        pivot[2 * side],
                        pivot[2 * side + 1],
                    ],
                    axis=0,
                ).astype(BF16)


def spread(tiles):
    lane = iota(tiles[0].shape, 1)
    halves = ([], [])
    for m in range(N // 2):
        x, y = tiles[2 * m], tiles[2 * m + 1]
        halves[0].append(jnp.where(lane < 64, x, pltpu.roll(y, 64, 1)))
        halves[1].append(jnp.where(lane < 64, pltpu.roll(x, 64, 1), y))
    return [jnp.concatenate(h, axis=1) for h in halves]


def move(x, start, to):
    return pltpu.roll(x, (to - start) % 128, 1) if (to - start) % 128 else x


def panel_half(ref, i):
    sub = iota((8, 128), 0)
    lane = iota((8, 128), 1)
    x = [jnp.where(sub < 6, ref[i * N + j, 16:24, :].astype(F32), 0.0) for j in range(N)]
    return jnp.concatenate(
        [jnp.where(lane < 64, x[2 * m], pltpu.roll(x[2 * m + 1], 64, 1)) for m in range(4)], axis=1
    )


def pivot_half(ref):
    return jnp.concatenate(
        [
            ref[:, 24 + 8 * m : 32 + 8 * m, :].astype(F32).reshape(TILE, 128).astype(BF16)
            for m in range(2)
        ],
        axis=1,
    )


def sort(got, mapping, t0, g0, g1, left, right_ref, row_ref, pair_ref, off, inv, inverse, col_ref):
    fill_inverse(mapping, inverse)
    sub = iota((8, 128), 0)
    lane = iota((8, 128), 1)
    valid = sub < 6
    zero = jnp.zeros((8, 128), F32)
    t0[64] = zero
    g0[64] = zero
    g1[64] = zero
    right = [[] for _ in range(N)]
    thin = [zero] * N
    diag = [zero] * 4
    group = lane // 8
    for i in range(N):
        thick = zero
        for j in range(N):
            k = i * N + j
            x = got[k, 0:24, :].astype(F32)
            a, b = x[8:16], x[16:24]
            t0[k] = x[0:8]
            g0[k] = jnp.where(sub >= 6, a, jnp.where(sub >= 4, pltpu.roll(b, 6, 0), 0.0))
            g1[k] = jnp.where(
                sub >= 4, 0.0, jnp.where(sub >= 2, pltpu.roll(a, 4, 0), pltpu.roll(b, 2, 0))
            )
            right[j].append(jnp.where(valid, a, 0.0))
            for half in range(2):
                thin[j] = jnp.where(group == 8 * half + i, move(b, 64 + 8 * half, 64 * half + 8 * i), thin[j])
                thick = jnp.where(group == 8 * half + j, move(b, 80 + 8 * half, 64 * half + 8 * j), thick)
            total = b + pltpu.roll(b, 120, 1) + pltpu.roll(b, 112, 1)
            to = 64 * (i % 2) + 8 * j
            diag[i // 2] = jnp.where(group == to // 8, move(total, 96, to), diag[i // 2])
        col_ref[i] = jnp.where(valid, thick, 0.0)
        left[8 * i : 8 * i + 8, :] = panel_half(got, i)
    col_ref[N] = zero
    for r in range(N):
        x = col_ref[inverse[2 * r]]
        y = col_ref[inverse[2 * r + 1]]
        pair_ref[2 * r] = jnp.where(lane < 64, x, pltpu.roll(y, 64, 1))
        pair_ref[2 * r + 1] = jnp.where(lane < 64, pltpu.roll(x, 64, 1), y)
    off[...] = pivot_half(got)
    full = 1.0 / jnp.concatenate([x[0:1] for x in diag], axis=1)
    inv[...] = jnp.broadcast_to(full, (8, TILE))
    right_ref[2 * N] = jnp.zeros((8, TILE), F32)
    row_ref[N] = zero
    for j in range(N):
        parts = spread(right[j])
        right_ref[2 * j] = parts[0]
        right_ref[2 * j + 1] = parts[1]
        row_ref[j] = jnp.where(valid, thin[j], 0.0)


def route(
    other, t0, g0, g1, left, right_ref, row_ref, pair_ref, off, inv, mapping, send, inverse, lower_ref, off_ref
):
    fill_inverse(mapping, inverse)
    core_id = lax.axis_index("col") % 2
    sub = iota((8, 128), 0)
    valid = sub < 6
    off_ref[core_id] = off[...]
    off_ref[1 - core_id] = pivot_half(other)
    whole = jnp.concatenate([off_ref[0], off_ref[1]], axis=1)
    scale = inv[0:1, :]

    def times(x):
        high = x.astype(BF16)
        low = (x - high.astype(F32)).astype(BF16)
        both = dot(jnp.concatenate([high, low], axis=0), whole, (1, 0))
        return (both[:128] + both[128:]) * scale

    v = jnp.concatenate([left[...]] + [panel_half(other, i) for i in range(N)], axis=0) * scale
    y = v - times(v)
    z = y + times(y)
    lower = 2.0 * y - z + times(z)
    for k in range(2 * N):
        lower_ref[k] = lower[8 * k : 8 * k + 8]
    lower_ref[2 * N] = jnp.zeros((8, TILE), F32)
    rows = []
    for half in range(2):
        for s in range(2):
            for r in range(N):
                i = inverse[2 * r + s]
                at = jnp.bitwise_xor(half, core_id) * N + i
                rows.append(lower_ref[jnp.where(i < N, at, 2 * N)])
    cols = []
    for k in range(2 * N):
        j = inverse[k]
        for half in range(2):
            cols.append(right_ref[jnp.where(j < N, 2 * j + half, 2 * N)])
    core = dot(
        jnp.concatenate(rows, axis=0).astype(BF16), jnp.concatenate(cols, axis=0).astype(BF16), (1, 1)
    )
    core = core.astype(BF16).astype(F32)
    place = iota((64, 128), 1) // 16
    low_lanes = iota((8, 128), 1) < 64
    for k in range(2 * N):
        c, h = k // 2, k % 2
        total = jnp.zeros((64, 128), F32)
        for combo in range(4):
            x = core[64 * combo : 64 * combo + 64, 128 * (k // 8) : 128 * (k // 8) + 128]
            total = jnp.where(place == combo, move(x, 16 * (k % 8), 16 * combo), total)
        beside = pltpu.roll(total, 64, 1)
        j = inverse[k]
        tail = row_ref[j]
        for r in range(N):
            part = total[8 * r : 8 * r + 8]
            shifted = beside[8 * r : 8 * r + 8]
            i0 = inverse[2 * r]
            i1 = inverse[2 * r + 1]
            at0 = jnp.where((i0 < N) & (j < N), i0 * N + j, 64)
            at1 = jnp.where((i1 < N) & (j < N), i1 * N + j, 64)
            spare = jnp.where(low_lanes, pltpu.roll(part, 6, 0), pltpu.roll(shifted, 4, 0))
            send[(h * N + r) * N + c] = jnp.concatenate(
                [
                    t0[at0],
                    t0[at1],
                    g0[at0] + g1[at1],
                    jnp.where(valid, tail, spare),
                    jnp.where(valid, pair_ref[2 * r + c % 2], pltpu.roll(part, 2, 0)),
                ],
                axis=0,
            ).astype(BF16)


def gather_up(blocks, lefts, rights, cores, order_out):
    def tile(f, g, c, at):
        return blocks[f * 64 + g * N + c, 8 * at : 8 * at + 8, :].astype(F32)

    k = iota((TILE, TILE), 0)
    target = 64 * ((k // 8) % 8) + 8 * (k // 64) + k % 8
    order = (target == iota((TILE, TILE), 1)).astype(BF16)
    order_out[...] = order
    sub = iota((8, 128), 0)
    group = iota((64, 128), 1) // 16
    core_id = lax.axis_index("col") % 2
    row = iota((192, TILE), 0) % 24
    of_slot = (
        (row < 8) | (row >= 20),
        (row >= 8) & (row < 20),
    )
    mixed = []
    for f in range(2):
        for side in range(2):
            lanes = []
            for m in range(4):
                c = 2 * m + side
                lanes.append(
                    jnp.concatenate(
                        [blocks[f * 64 + g * N + c, 0:24, :].astype(F32) for g in range(N)], axis=0
                    )
                )
            x = jnp.concatenate(lanes, axis=1)
            if side == 0:
                for s in range(2):
                    lefts[s, 192 * f : 192 * f + 192, :] = jnp.where(of_slot[s], x, 0.0).astype(BF16)
            else:
                rights[192 * f : 192 * f + 192, :] = x.astype(BF16)
        parts = []
        for c in range(N):
            rows = []
            for g in range(N):
                x = tile(f, g, c, 3)
                y = tile(f, g, c, 4)
                y = jnp.where(sub < 4, pltpu.roll(pltpu.roll(x, 64, 1), 4, 0), pltpu.roll(y, 6, 0))
                y = jnp.where(sub < 2, pltpu.roll(x, 2, 0), y)
                rows.append(jnp.where(sub < 6, y, 0.0))
            parts.append(jnp.concatenate(rows, axis=0))
        for s in range(2):
            halves = []
            for half in range(2):
                total = jnp.zeros((64, 128), F32)
                combo = 2 * half + s
                for c in range(N):
                    total = jnp.where(group == c, move(parts[c], 16 * combo, 16 * c), total)
                halves.append(total)
            first = jnp.where(core_id == 0, halves[0], halves[1])
            second = jnp.where(core_id == 0, halves[1], halves[0])
            cores[2 * f + s] = jnp.concatenate([first, second], axis=0).astype(BF16)
        for c in range(N):
            mixed += spread([tile(f, g, c, 3) for g in range(N)])
    row_v = jnp.concatenate(mixed, axis=0).astype(BF16)
    rights[384:640, :] = dot(row_v, order, (1, 0)).astype(BF16)


def finish(blocks, twin, lefts, rights, cores, order, out, made, sems):
    updates = [[], []]
    for f in range(2):
        col_u = [[], []]
        for ref, rows in ((blocks, slice(32, 40)), (twin, slice(0, 8))):
            for g in range(N):
                at = f * 64 + g * N
                tiles = [ref[at + c, rows, :].astype(F32) for c in range(N)]
                for s, x in enumerate(spread(tiles)):
                    col_u[s].append(x)
        for s in range(2):
            x = jnp.concatenate(col_u[s], axis=0).astype(BF16)
            updates[s].append(-dot(cores[2 * f + s], x, (0, 0)))
    update = jnp.concatenate(updates[0] + updates[1], axis=0).astype(BF16)
    update = dot(update, order[...], (1, 0)).astype(BF16)
    right = rights[...]
    stores = []
    for s in range(2):
        both = jnp.concatenate([lefts[s], update[256 * s : 256 * s + 256]], axis=0)
        for part in range(2):
            rows = slice(256 * part, 256 * part + 256)
            made[s, rows, :] = dot(both[:, rows], right, (0, 0)).astype(BF16)
            copy = pltpu.make_async_copy(made.at[s, rows], out.at[s, rows], sems.at[2 * s + part])
            copy.start()
            stores.append(copy)
    for copy in stores:
        copy.wait()


def exchange(x, axes, name):
    with jax.named_scope(name):
        return lax.all_to_all(x, axes, split_axis=0, concat_axis=0, tiled=True)


def swap(x):
    return lax.ppermute(x, "col", [(k, k ^ 1) for k in range(N)])


def in_vmem(x):
    return pltpu.with_memory_space_constraint(x, VMEM)


def shards(
    pivot, col_ut, col_vt, col_rank, row_ut, row_vt, row_rank, cb_ut, cb_vt, cb_rank, parent_map
):
    sds = jax.ShapeDtypeStruct
    (send,) = call(
        pack,
        (VMEM((64, 40, 128), BF16),),
        (
            pivot[0],
            col_ut[0, 0].T,
            col_vt[0, 0].T,
            row_ut[0, 0].T,
            row_vt[0, 0].T,
            cb_ut[0, 0, 0],
            cb_vt[0, 0, 0],
            col_rank,
            row_rank,
            cb_rank,
        ),
        (VMEM,) * 7 + (SMEM,) * 3,
        name="pack",
        limit=None,
    )
    got = exchange(send, ("row", "col"), "scatter")
    got = in_vmem(got)
    other = in_vmem(swap(got))
    sorted_out = call(
        sort,
        (VMEM((65, 8, 128), F32),) * 3
        + (
            VMEM((64, TILE), F32),
            VMEM((2 * N + 1, 8, TILE), F32),
            VMEM((N + 1, 8, 128), F32),
            VMEM((2 * N, 8, 128), F32),
            VMEM((TILE, TILE // 2), BF16),
            VMEM((8, TILE), F32),
        ),
        (got, parent_map),
        (VMEM, SMEM),
        (SMEM((2 * N,), jnp.int32), VMEM((N + 1, 8, 128), F32)),
        name="sort",
    )
    (send,) = call(
        route,
        (VMEM((128, 40, 128), BF16),),
        (other, *(in_vmem(x) for x in sorted_out), parent_map),
        (VMEM,) * 10 + (SMEM,),
        (
            SMEM((2 * N,), jnp.int32),
            VMEM((2 * N + 1, 8, TILE), F32),
            VMEM((2, TILE, TILE // 2), BF16),
        ),
        name="route",
    )
    blocks = exchange(send, ("side", "row", "col"), "gather")
    twin = in_vmem(swap(blocks[:, 32:40]))
    blocks = in_vmem(blocks)
    gathered = call(
        gather_up,
        (
            VMEM((2, 384, TILE), BF16),
            VMEM((640, TILE), BF16),
            VMEM((4, 128, 128), BF16),
            VMEM((TILE, TILE), BF16),
        ),
        (blocks,),
        (VMEM,),
        name="gather_up",
    )
    (out,) = call(
        finish,
        (sds((2, TILE, TILE), BF16),),
        (blocks, twin, *(in_vmem(x) for x in gathered)),
        (VMEM,) * 6,
        (
            VMEM((2, TILE, TILE), BF16),
            pltpu.SemaphoreType.DMA((4,)),
        ),
        name="finish",
        into=pl.ANY,
    )
    return out[None, :, None]


def solution(mesh):
    front = ("pair", "side")
    split = Mesh(mesh.devices.reshape(4, 2, N, N), ("pair", "side", "row", "col"))
    placed = (
        P(front, ("row", "col"), None),
        P(front, "row", None, "col"),
        P(front, "row", None, "col"),
        P(front, "row"),
        P(front, "col", None, "row"),
        P(front, "col", None, "row"),
        P(front, "col"),
        P(front, "row", "col", None, None),
        P(front, "row", "col", None, None),
        P(front, "row", "col"),
        P(front, None),
    )

    return jax.shard_map(
        shards,
        mesh=split,
        in_specs=placed,
        out_specs=P(front, "row", "col", None, None),
        check_vma=False,
    )
```

```python
import jax
import jax.numpy as jnp
from jax import lax
from jax.experimental import pallas as pl
from jax.experimental.pallas import tpu as pltpu
from jax.sharding import Mesh, PartitionSpec as P

F32 = jnp.float32
BF16 = jnp.bfloat16
RANK = 96
TILE = 512
N = 8
SMEM = pltpu.SMEM
VMEM = pltpu.VMEM
MAP = (SMEM((1, N), jnp.int32), pltpu.SemaphoreType.DMA((1,)), SMEM((2 * N,), jnp.int32))


def iota(shape, dim):
    return lax.broadcasted_iota(jnp.int32, shape, dim)


def dot(a, b, contract):
    return lax.dot_general(
        a, b, ((contract[:1], contract[1:]), ((), ())), preferred_element_type=F32
    )


def call(body, outs, args, specs, scratch=(), name=None, into=VMEM, limit=24 * 2**20):
    kernel = pl.pallas_call(
        body,
        out_shape=outs,
        in_specs=[pl.BlockSpec(memory_space=s) for s in specs],
        out_specs=[pl.BlockSpec(memory_space=into) for _ in outs],
        scratch_shapes=scratch,
        compiler_params=pltpu.CompilerParams(vmem_limit_bytes=limit),
        name=name,
    )
    with jax.named_scope("do_" + name):
        return kernel(*args)


def fetch_map(mapping, table, sem):
    copy = pltpu.make_async_copy(mapping, table, sem.at[0])
    copy.start()
    return copy


def fill_inverse(mapping, inverse):
    for k in range(2 * N):
        inverse[k] = N
    for k in range(N):
        inverse[mapping[0, k]] = k


def onehot(offset):
    row = iota((64, RANK), 0)
    level = iota((64, RANK), 1)
    t = row % 8
    return ((t < 6) & (level == 12 * (row // 8) + offset + t)).astype(BF16)


def pack(piv, cu, cv, ru, rv, cbu, cbv, rank_c, rank_r, rank_b, send):
    level = iota((64, RANK), 1)
    even = onehot(0)
    odd = onehot(6)

    def panel(ref, rank):
        x = jnp.where(level < rank, ref[...].astype(F32), 0.0).astype(BF16)
        return jnp.concatenate([dot(even, x, (1, 1)), dot(odd, x, (1, 1))], axis=1)

    col_u = panel(cu, rank_c[0, 0]).astype(BF16)
    col_v = panel(cv, rank_c[0, 0])
    row_u = panel(ru, rank_r[0, 0])
    row_v = panel(rv, rank_r[0, 0]).astype(BF16)
    first_half = iota((64, 128), 1) < 64
    col_v = (
        jnp.where(first_half, col_v, 0.0),
        jnp.where(first_half, pltpu.roll(col_v, 64, 1), 0.0),
    )
    q = lax.axis_index("row") * N + lax.axis_index("col")
    full = piv[...]
    on_diag = iota((8, TILE), 1) == 8 * q + iota((8, TILE), 0)
    diag = jnp.sum(jnp.where(on_diag, full, 0.0), axis=1, keepdims=True)
    off = jnp.where(on_diag, 0.0, full)
    high = diag.astype(BF16).astype(F32)
    rest = diag - high
    mid = rest.astype(BF16).astype(F32)
    lane = iota((8, 128), 1)
    sub = iota((8, 128), 0)
    parts = jnp.zeros((8, 128), F32)
    for k, x in enumerate((high, mid, rest - mid)):
        parts = jnp.where(lane == 96 + 8 * k + sub, x, parts)
    parts = jnp.where(sub == 0, jnp.sum(parts, axis=0, keepdims=True), 0.0)
    pivot = [off[:, 128 * m : 128 * m + 128] for m in range(4)]
    wide = iota((RANK, TILE), 0)
    row = iota((64, RANK), 0)
    lev = iota((64, RANK), 1)
    t = row % 8
    extra = [
        ((t >= 6) & (lev == 64 + 4 * (row // 8) + 2 * e + t - 6)).astype(BF16) for e in range(2)
    ]
    from_lane = iota((128, 128), 0)
    place = iota((128, 128), 1) - 8 * (from_lane // 64) - from_lane % 64
    inside = from_lane % 64 // 8
    thin = []
    for g in range(N):
        thin.append(
            [
                dot(x, ((inside == g) & (place == at - 8 * g)).astype(BF16), (1, 0))
                for x, at in ((row_v, 64), (col_u, 80))
            ]
        )
    for side, ref in enumerate((cbu, cbv)):
        x = jnp.where(wide < rank_b[0, 0, 0], ref[...].astype(F32), 0.0)
        narrow = x.astype(BF16)
        x1 = dot(extra[0], narrow, (1, 0))
        x2 = dot(extra[1], narrow, (1, 0))
        for g in range(N):
            rows = slice(8 * g, 8 * g + 8)
            for m in range(4):
                lanes = slice(128 * m, 128 * m + 128)
                c = 2 * m + side
                cols = slice(8 * c, 8 * c + 8)
                send[g * N + c] = jnp.concatenate(
                    [
                        x[rows, lanes],
                        row_u[cols] + x1[rows, lanes],
                        col_v[side][rows] + thin[g][0][cols] + thin[c][1][rows] + parts + x2[rows, lanes],
                        pivot[2 * side],
                        pivot[2 * side + 1],
                    ],
                    axis=0,
                ).astype(BF16)


def spread(tiles):
    lane = iota(tiles[0].shape, 1)
    halves = ([], [])
    for m in range(N // 2):
        x, y = tiles[2 * m], tiles[2 * m + 1]
        halves[0].append(jnp.where(lane < 64, x, pltpu.roll(y, 64, 1)))
        halves[1].append(jnp.where(lane < 64, pltpu.roll(x, 64, 1), y))
    return [jnp.concatenate(h, axis=1) for h in halves]


def move(x, start, to):
    return pltpu.roll(x, (to - start) % 128, 1) if (to - start) % 128 else x


def panel_half(ref, i):
    sub = iota((8, 128), 0)
    lane = iota((8, 128), 1)
    x = [jnp.where(sub < 6, ref[i * N + j, 16:24, :].astype(F32), 0.0) for j in range(N)]
    return jnp.concatenate(
        [jnp.where(lane < 64, x[2 * m], pltpu.roll(x[2 * m + 1], 64, 1)) for m in range(4)], axis=1
    )


def pivot_half(ref):
    return jnp.concatenate(
        [
            ref[:, 24 + 8 * m : 32 + 8 * m, :].astype(F32).reshape(TILE, 128).astype(BF16)
            for m in range(2)
        ],
        axis=1,
    )


def sort(
    got, mapping, t0, g0, g1, left, right_ref, row_ref, pair_ref, off, inv, table, sem, inverse, col_ref
):
    fetch = fetch_map(mapping, table, sem)
    sub = iota((8, 128), 0)
    lane = iota((8, 128), 1)
    valid = sub < 6
    zero = jnp.zeros((8, 128), F32)
    t0[64] = zero
    g0[64] = zero
    g1[64] = zero
    right = [[] for _ in range(N)]
    thin = [zero] * N
    diag = [zero] * 4
    group = lane // 8
    for i in range(N):
        thick = zero
        for j in range(N):
            k = i * N + j
            x = got[k, 0:24, :].astype(F32)
            a, b = x[8:16], x[16:24]
            t0[k] = x[0:8]
            g0[k] = jnp.where(sub >= 6, a, jnp.where(sub >= 4, pltpu.roll(b, 6, 0), 0.0))
            g1[k] = jnp.where(
                sub >= 4, 0.0, jnp.where(sub >= 2, pltpu.roll(a, 4, 0), pltpu.roll(b, 2, 0))
            )
            right[j].append(jnp.where(valid, a, 0.0))
            for half in range(2):
                thin[j] = jnp.where(group == 8 * half + i, move(b, 64 + 8 * half, 64 * half + 8 * i), thin[j])
                thick = jnp.where(group == 8 * half + j, move(b, 80 + 8 * half, 64 * half + 8 * j), thick)
            total = b + pltpu.roll(b, 120, 1) + pltpu.roll(b, 112, 1)
            to = 64 * (i % 2) + 8 * j
            diag[i // 2] = jnp.where(group == to // 8, move(total, 96, to), diag[i // 2])
        col_ref[i] = jnp.where(valid, thick, 0.0)
        left[8 * i : 8 * i + 8, :] = panel_half(got, i)
    col_ref[N] = zero
    off[...] = pivot_half(got)
    full = 1.0 / jnp.concatenate([x[0:1] for x in diag], axis=1)
    inv[...] = jnp.broadcast_to(full, (8, TILE))
    right_ref[2 * N] = jnp.zeros((8, TILE), F32)
    row_ref[N] = zero
    for j in range(N):
        parts = spread(right[j])
        right_ref[2 * j] = parts[0]
        right_ref[2 * j + 1] = parts[1]
        row_ref[j] = jnp.where(valid, thin[j], 0.0)
    fetch.wait()
    fill_inverse(table, inverse)
    for r in range(N):
        x = col_ref[inverse[2 * r]]
        y = col_ref[inverse[2 * r + 1]]
        pair_ref[2 * r] = jnp.where(lane < 64, x, pltpu.roll(y, 64, 1))
        pair_ref[2 * r + 1] = jnp.where(lane < 64, pltpu.roll(x, 64, 1), y)


def route(
    other, t0, g0, g1, left, right_ref, row_ref, pair_ref, off, inv, mapping, send, table, sem, inverse,
    lower_ref, off_ref
):
    fetch = fetch_map(mapping, table, sem)
    core_id = lax.axis_index("col") % 2
    sub = iota((8, 128), 0)
    valid = sub < 6
    off_ref[core_id] = off[...]
    off_ref[1 - core_id] = pivot_half(other)
    whole = jnp.concatenate([off_ref[0], off_ref[1]], axis=1)
    scale = inv[0:1, :]

    def times(x):
        high = x.astype(BF16)
        low = (x - high.astype(F32)).astype(BF16)
        both = dot(jnp.concatenate([high, low], axis=0), whole, (1, 0))
        return (both[:128] + both[128:]) * scale

    v = jnp.concatenate([left[...]] + [panel_half(other, i) for i in range(N)], axis=0) * scale
    y = v - times(v)
    z = y + times(y)
    lower = 2.0 * y - z + times(z)
    for k in range(2 * N):
        lower_ref[k] = lower[8 * k : 8 * k + 8]
    lower_ref[2 * N] = jnp.zeros((8, TILE), F32)
    fetch.wait()
    fill_inverse(table, inverse)
    rows = []
    for half in range(2):
        for s in range(2):
            for r in range(N):
                i = inverse[2 * r + s]
                at = jnp.bitwise_xor(half, core_id) * N + i
                rows.append(lower_ref[jnp.where(i < N, at, 2 * N)])
    cols = []
    for k in range(2 * N):
        j = inverse[k]
        for half in range(2):
            cols.append(right_ref[jnp.where(j < N, 2 * j + half, 2 * N)])
    core = dot(
        jnp.concatenate(rows, axis=0).astype(BF16), jnp.concatenate(cols, axis=0).astype(BF16), (1, 1)
    )
    core = core.astype(BF16).astype(F32)
    place = iota((64, 128), 1) // 16
    low_lanes = iota((8, 128), 1) < 64
    for k in range(2 * N):
        c, h = k // 2, k % 2
        total = jnp.zeros((64, 128), F32)
        for combo in range(4):
            x = core[64 * combo : 64 * combo + 64, 128 * (k // 8) : 128 * (k // 8) + 128]
            total = jnp.where(place == combo, move(x, 16 * (k % 8), 16 * combo), total)
        beside = pltpu.roll(total, 64, 1)
        j = inverse[k]
        tail = row_ref[j]
        for r in range(N):
            part = total[8 * r : 8 * r + 8]
            shifted = beside[8 * r : 8 * r + 8]
            i0 = inverse[2 * r]
            i1 = inverse[2 * r + 1]
            at0 = jnp.where((i0 < N) & (j < N), i0 * N + j, 64)
            at1 = jnp.where((i1 < N) & (j < N), i1 * N + j, 64)
            spare = jnp.where(low_lanes, pltpu.roll(part, 6, 0), pltpu.roll(shifted, 4, 0))
            send[(h * N + r) * N + c] = jnp.concatenate(
                [
                    t0[at0],
                    t0[at1],
                    g0[at0] + g1[at1],
                    jnp.where(valid, tail, spare),
                    jnp.where(valid, pair_ref[2 * r + c % 2], pltpu.roll(part, 2, 0)),
                ],
                axis=0,
            ).astype(BF16)


def gather_up(blocks, lefts, rights, row_v, cores, own_u, order_out):
    def tile(f, g, c, at):
        return blocks[f * 64 + g * N + c, 8 * at : 8 * at + 8, :].astype(F32)

    k = iota((TILE, TILE), 0)
    target = 64 * ((k // 8) % 8) + 8 * (k // 64) + k % 8
    order = (target == iota((TILE, TILE), 1)).astype(BF16)
    order_out[...] = order
    sub = iota((8, 128), 0)
    group = iota((64, 128), 1) // 16
    core_id = lax.axis_index("col") % 2
    of_slot = (sub >= 4, sub < 4)
    mixed = []
    own = []
    for f in range(2):
        for side, into in ((0, lefts), (1, rights)):
            lanes = ([], [])
            for m in range(4):
                x = [
                    blocks[f * 64 + g * N + 2 * m + side, 0:24, :].astype(F32) for g in range(N)
                ]
                for s in range(2):
                    rows = []
                    for y in x:
                        rest = y[16:24]
                        if side == 0:
                            rest = jnp.where(of_slot[s], rest, 0.0)
                        rows += [y[8 * s : 8 * s + 8], rest]
                    lanes[s].append(jnp.concatenate(rows, axis=0))
            for s in range(2):
                into[s, 128 * f : 128 * f + 128, :] = jnp.concatenate(lanes[s], axis=1).astype(BF16)
        parts = []
        for c in range(N):
            rows = []
            for g in range(N):
                x = tile(f, g, c, 3)
                y = tile(f, g, c, 4)
                y = jnp.where(sub < 4, pltpu.roll(pltpu.roll(x, 64, 1), 4, 0), pltpu.roll(y, 6, 0))
                y = jnp.where(sub < 2, pltpu.roll(x, 2, 0), y)
                rows.append(jnp.where(sub < 6, y, 0.0))
            parts.append(jnp.concatenate(rows, axis=0))
        for s in range(2):
            halves = []
            for half in range(2):
                total = jnp.zeros((64, 128), F32)
                combo = 2 * half + s
                for c in range(N):
                    total = jnp.where(group == c, move(parts[c], 16 * combo, 16 * c), total)
                halves.append(total)
            first = jnp.where(core_id == 0, halves[0], halves[1])
            second = jnp.where(core_id == 0, halves[1], halves[0])
            cores[2 * f + s] = jnp.concatenate([first, second], axis=0).astype(BF16)
        for c in range(N):
            mixed += spread([tile(f, g, c, 3) for g in range(N)])
        own += half_panels([[tile(f, g, c, 4) for c in range(N)] for g in range(N)])
    panels = jnp.concatenate(mixed + own, axis=0).astype(BF16)
    panels = dot(panels, order, (1, 0)).astype(BF16)
    row_v[...] = panels[:256]
    own_u[...] = panels[256:]


def half_panels(tiles):
    both = [spread(x) for x in tiles]
    return [jnp.concatenate([x[s] for x in both], axis=0) for s in range(2)]


def finish(twin, lefts, rights, row_v, cores, own_u, order, out, made, sems):
    other = []
    for f in range(2):
        other += half_panels(
            [[twin[f * 64 + g * N + c].astype(F32) for c in range(N)] for g in range(N)]
        )
    other = dot(jnp.concatenate(other, axis=0).astype(BF16), order[...], (1, 0)).astype(BF16)
    updates = [[], []]
    for f in range(2):
        for s in range(2):
            at = slice(64 * (2 * f + s), 64 * (2 * f + s) + 64)
            col_u = jnp.concatenate([own_u[at, :], other[at]], axis=0)
            updates[s].append((-dot(cores[2 * f + s], col_u, (0, 0))).astype(BF16))
    stores = []
    for s in range(2):
        both = jnp.concatenate([lefts[s]] + updates[s], axis=0)
        right = jnp.concatenate([rights[s], row_v[...]], axis=0)
        for part in range(2):
            rows = slice(256 * part, 256 * part + 256)
            made[s, rows, :] = dot(both[:, rows], right, (0, 0)).astype(BF16)
            copy = pltpu.make_async_copy(made.at[s, rows], out.at[s, rows], sems.at[2 * s + part])
            copy.start()
            stores.append(copy)
    for copy in stores:
        copy.wait()


def exchange(x, axes, name):
    with jax.named_scope(name):
        return lax.all_to_all(x, axes, split_axis=0, concat_axis=0, tiled=True)


def swap(x):
    return lax.ppermute(x, "col", [(k, k ^ 1) for k in range(N)])


def in_vmem(x):
    return pltpu.with_memory_space_constraint(x, VMEM)


def shards(
    pivot, col_ut, col_vt, col_rank, row_ut, row_vt, row_rank, cb_ut, cb_vt, cb_rank, parent_map
):
    sds = jax.ShapeDtypeStruct
    (send,) = call(
        pack,
        (VMEM((64, 40, 128), BF16),),
        (
            pivot[0],
            col_ut[0, 0].T,
            col_vt[0, 0].T,
            row_ut[0, 0].T,
            row_vt[0, 0].T,
            cb_ut[0, 0, 0],
            cb_vt[0, 0, 0],
            col_rank,
            row_rank,
            cb_rank,
        ),
        (VMEM,) * 7 + (SMEM,) * 3,
        name="pack",
        limit=None,
    )
    got = exchange(send, ("row", "col"), "scatter")
    got = in_vmem(got)
    other = in_vmem(swap(got))
    sorted_out = call(
        sort,
        (VMEM((65, 8, 128), F32),) * 3
        + (
            VMEM((64, TILE), F32),
            VMEM((2 * N + 1, 8, TILE), F32),
            VMEM((N + 1, 8, 128), F32),
            VMEM((2 * N, 8, 128), F32),
            VMEM((TILE, TILE // 2), BF16),
            VMEM((8, TILE), F32),
        ),
        (got, parent_map),
        (VMEM, pl.ANY),
        MAP + (VMEM((N + 1, 8, 128), F32),),
        name="sort",
    )
    (send,) = call(
        route,
        (VMEM((128, 40, 128), BF16),),
        (other, *(in_vmem(x) for x in sorted_out), parent_map),
        (VMEM,) * 10 + (pl.ANY,),
        MAP
        + (
            VMEM((2 * N + 1, 8, TILE), F32),
            VMEM((2, TILE, TILE // 2), BF16),
        ),
        name="route",
    )
    blocks = exchange(send, ("side", "row", "col"), "gather")
    twin = in_vmem(swap(blocks[:, 32:40]))
    blocks = in_vmem(blocks)
    gathered = call(
        gather_up,
        (
            VMEM((2, 256, TILE), BF16),
            VMEM((2, 256, TILE), BF16),
            VMEM((256, TILE), BF16),
            VMEM((4, 128, 128), BF16),
            VMEM((256, TILE), BF16),
            VMEM((TILE, TILE), BF16),
        ),
        (blocks,),
        (VMEM,),
        name="gather_up",
    )
    (out,) = call(
        finish,
        (sds((2, TILE, TILE), BF16),),
        (twin, *(in_vmem(x) for x in gathered)),
        (VMEM,) * 7,
        (
            VMEM((2, TILE, TILE), BF16),
            pltpu.SemaphoreType.DMA((4,)),
        ),
        name="finish",
        into=pl.ANY,
    )
    return out[None, :, None]


def solution(mesh):
    front = ("pair", "side")
    split = Mesh(mesh.devices.reshape(4, 2, N, N), ("pair", "side", "row", "col"))
    placed = (
        P(front, ("row", "col"), None),
        P(front, "row", None, "col"),
        P(front, "row", None, "col"),
        P(front, "row"),
        P(front, "col", None, "row"),
        P(front, "col", None, "row"),
        P(front, "col"),
        P(front, "row", "col", None, None),
        P(front, "row", "col", None, None),
        P(front, "row", "col"),
        P(front, None),
    )

    return jax.shard_map(
        shards,
        mesh=split,
        in_specs=placed,
        out_specs=P(front, "row", "col", None, None),
        check_vma=False,
    )
```

```python
import jax
import jax.numpy as jnp
from jax import lax
from jax.experimental import pallas as pl
from jax.experimental.pallas import tpu as pltpu
from jax.sharding import Mesh, PartitionSpec as P

F32 = jnp.float32
BF16 = jnp.bfloat16
RANK = 96
TILE = 512
N = 8
SMEM = pltpu.SMEM
VMEM = pltpu.VMEM


def iota(shape, dim):
    return lax.broadcasted_iota(jnp.int32, shape, dim)


def dot(a, b, contract):
    return lax.dot_general(
        a, b, ((contract[:1], contract[1:]), ((), ())), preferred_element_type=F32
    )


def call(body, outs, args, specs, scratch=(), name=None, into=VMEM, limit=24 * 2**20):
    kernel = pl.pallas_call(
        body,
        out_shape=outs,
        in_specs=[pl.BlockSpec(memory_space=s) for s in specs],
        out_specs=[pl.BlockSpec(memory_space=into) for _ in outs],
        scratch_shapes=scratch,
        compiler_params=pltpu.CompilerParams(vmem_limit_bytes=limit),
        name=name,
    )
    with jax.named_scope("do_" + name):
        return kernel(*args)


def fill_inverse(mapping, inverse):
    lane = iota((1, N), 1)
    x = mapping[...].astype(F32)
    scale = jnp.where(lane % 4 == 0, 1.0, jnp.where(lane % 4 == 1, 16.0, jnp.where(lane % 4 == 2, 256.0, 4096.0)))
    digits = [
        jnp.sum(jnp.where(lane // 4 == k, x * scale, 0.0)).astype(jnp.int32) for k in range(2)
    ]
    for k in range(2 * N):
        inverse[k] = N
    for k in range(N):
        inverse[(digits[k // 4] >> (4 * (k % 4))) & 15] = k


def onehot(offset):
    row = iota((64, RANK), 0)
    level = iota((64, RANK), 1)
    t = row % 8
    return ((t < 6) & (level == 12 * (row // 8) + offset + t)).astype(BF16)


def pack(piv, cu, cv, ru, rv, cbu, cbv, rank_c, rank_r, rank_b, send):
    level = iota((64, RANK), 1)
    even = onehot(0)
    odd = onehot(6)

    def panel(ref, rank):
        x = jnp.where(level < rank, ref[...].astype(F32), 0.0).astype(BF16)
        return jnp.concatenate([dot(even, x, (1, 1)), dot(odd, x, (1, 1))], axis=1)

    col_u = panel(cu, rank_c[0, 0]).astype(BF16)
    col_v = panel(cv, rank_c[0, 0])
    row_u = panel(ru, rank_r[0, 0])
    row_v = panel(rv, rank_r[0, 0]).astype(BF16)
    first_half = iota((64, 128), 1) < 64
    col_v = (
        jnp.where(first_half, col_v, 0.0),
        jnp.where(first_half, pltpu.roll(col_v, 64, 1), 0.0),
    )
    q = lax.axis_index("row") * N + lax.axis_index("col")
    full = piv[...]
    on_diag = iota((8, TILE), 1) == 8 * q + iota((8, TILE), 0)
    diag = jnp.sum(jnp.where(on_diag, full, 0.0), axis=1, keepdims=True)
    off = jnp.where(on_diag, 0.0, full)
    high = diag.astype(BF16).astype(F32)
    rest = diag - high
    mid = rest.astype(BF16).astype(F32)
    lane = iota((8, 128), 1)
    sub = iota((8, 128), 0)
    parts = jnp.zeros((8, 128), F32)
    for k, x in enumerate((high, mid, rest - mid)):
        parts = jnp.where(lane == 96 + 8 * k + sub, x, parts)
    parts = jnp.where(sub == 0, jnp.sum(parts, axis=0, keepdims=True), 0.0)
    pivot = [off[:, 128 * m : 128 * m + 128] for m in range(4)]
    wide = iota((RANK, TILE), 0)
    row = iota((64, RANK), 0)
    lev = iota((64, RANK), 1)
    t = row % 8
    extra = [
        ((t >= 6) & (lev == 64 + 4 * (row // 8) + 2 * e + t - 6)).astype(BF16) for e in range(2)
    ]
    from_lane = iota((128, 128), 0)
    place = iota((128, 128), 1) - 8 * (from_lane // 64) - from_lane % 64
    inside = from_lane % 64 // 8
    thin = []
    for g in range(N):
        thin.append(
            [
                dot(x, ((inside == g) & (place == at - 8 * g)).astype(BF16), (1, 0))
                for x, at in ((row_v, 64), (col_u, 80))
            ]
        )
    for side, ref in enumerate((cbu, cbv)):
        x = jnp.where(wide < rank_b[0, 0, 0], ref[...].astype(F32), 0.0)
        narrow = x.astype(BF16)
        x1 = dot(extra[0], narrow, (1, 0))
        x2 = dot(extra[1], narrow, (1, 0))
        for g in range(N):
            rows = slice(8 * g, 8 * g + 8)
            for m in range(4):
                lanes = slice(128 * m, 128 * m + 128)
                c = 2 * m + side
                cols = slice(8 * c, 8 * c + 8)
                send[g * N + c] = jnp.concatenate(
                    [
                        x[rows, lanes],
                        row_u[cols] + x1[rows, lanes],
                        col_v[side][rows] + thin[g][0][cols] + thin[c][1][rows] + parts + x2[rows, lanes],
                        pivot[2 * side],
                        pivot[2 * side + 1],
                    ],
                    axis=0,
                ).astype(BF16)


def spread(tiles):
    lane = iota(tiles[0].shape, 1)
    halves = ([], [])
    for m in range(N // 2):
        x, y = tiles[2 * m], tiles[2 * m + 1]
        halves[0].append(jnp.where(lane < 64, x, pltpu.roll(y, 64, 1)))
        halves[1].append(jnp.where(lane < 64, pltpu.roll(x, 64, 1), y))
    return [jnp.concatenate(h, axis=1) for h in halves]


def move(x, start, to):
    return pltpu.roll(x, (to - start) % 128, 1) if (to - start) % 128 else x


def panel_half(ref, i, at):
    sub = iota((8, 128), 0)
    lane = iota((8, 128), 1)
    x = [jnp.where(sub < 6, ref[i * N + j, at : at + 8, :].astype(F32), 0.0) for j in range(N)]
    return jnp.concatenate(
        [jnp.where(lane < 64, x[2 * m], pltpu.roll(x[2 * m + 1], 64, 1)) for m in range(4)], axis=1
    )


def pivot_half(ref, at):
    return jnp.concatenate(
        [
            ref[:, at + 8 * m : at + 8 * m + 8, :].astype(F32).reshape(TILE, 128).astype(BF16)
            for m in range(2)
        ],
        axis=1,
    )


def sort(
    got, mapping, t0, g0, g1, left, right_ref, row_ref, pair_ref, off, inv, inverse, col_ref
):
    fill_inverse(mapping, inverse)
    sub = iota((8, 128), 0)
    lane = iota((8, 128), 1)
    valid = sub < 6
    zero = jnp.zeros((8, 128), F32)
    t0[64] = zero
    g0[64] = zero
    g1[64] = zero
    right = [[] for _ in range(N)]
    thin = [zero] * N
    diag = [zero] * 4
    group = lane // 8
    for i in range(N):
        thick = zero
        for j in range(N):
            k = i * N + j
            x = got[k, 0:24, :].astype(F32)
            a, b = x[8:16], x[16:24]
            t0[k] = x[0:8]
            g0[k] = jnp.where(sub >= 6, a, jnp.where(sub >= 4, pltpu.roll(b, 6, 0), 0.0))
            g1[k] = jnp.where(
                sub >= 4, 0.0, jnp.where(sub >= 2, pltpu.roll(a, 4, 0), pltpu.roll(b, 2, 0))
            )
            right[j].append(jnp.where(valid, a, 0.0))
            for half in range(2):
                thin[j] = jnp.where(group == 8 * half + i, move(b, 64 + 8 * half, 64 * half + 8 * i), thin[j])
                thick = jnp.where(group == 8 * half + j, move(b, 80 + 8 * half, 64 * half + 8 * j), thick)
            total = b + pltpu.roll(b, 120, 1) + pltpu.roll(b, 112, 1)
            to = 64 * (i % 2) + 8 * j
            diag[i // 2] = jnp.where(group == to // 8, move(total, 96, to), diag[i // 2])
        col_ref[i] = jnp.where(valid, thick, 0.0)
        left[8 * i : 8 * i + 8, :] = panel_half(got, i, 16)
    col_ref[N] = zero
    off[...] = pivot_half(got, 24)
    full = 1.0 / jnp.concatenate([x[0:1] for x in diag], axis=1)
    inv[...] = jnp.broadcast_to(full, (8, TILE))
    right_ref[2 * N] = jnp.zeros((8, TILE), F32)
    row_ref[N] = zero
    for j in range(N):
        parts = spread(right[j])
        right_ref[2 * j] = parts[0]
        right_ref[2 * j + 1] = parts[1]
        row_ref[j] = jnp.where(valid, thin[j], 0.0)
    for r in range(N):
        x = col_ref[inverse[2 * r]]
        y = col_ref[inverse[2 * r + 1]]
        pair_ref[2 * r] = jnp.where(lane < 64, x, pltpu.roll(y, 64, 1))
        pair_ref[2 * r + 1] = jnp.where(lane < 64, pltpu.roll(x, 64, 1), y)


def route(
    other, t0, g0, g1, left, right_ref, row_ref, pair_ref, off, inv, mapping, send, inverse, lower_ref, off_ref
):
    fill_inverse(mapping, inverse)
    core_id = lax.axis_index("col") % 2
    sub = iota((8, 128), 0)
    valid = sub < 6
    off_ref[core_id] = off[...]
    off_ref[1 - core_id] = pivot_half(other, 8)
    whole = jnp.concatenate([off_ref[0], off_ref[1]], axis=1)
    scale = inv[0:1, :]

    def times(x):
        high = x.astype(BF16)
        low = (x - high.astype(F32)).astype(BF16)
        both = dot(jnp.concatenate([high, low], axis=0), whole, (1, 0))
        return (both[:128] + both[128:]) * scale

    v = jnp.concatenate([left[...]] + [panel_half(other, i, 0) for i in range(N)], axis=0) * scale
    y = v - times(v)
    z = y + times(y)
    lower = 2.0 * y - z + times(z)
    for k in range(2 * N):
        lower_ref[k] = lower[8 * k : 8 * k + 8]
    lower_ref[2 * N] = jnp.zeros((8, TILE), F32)
    rows = []
    for half in range(2):
        for s in range(2):
            for r in range(N):
                i = inverse[2 * r + s]
                at = jnp.bitwise_xor(half, core_id) * N + i
                rows.append(lower_ref[jnp.where(i < N, at, 2 * N)])
    cols = []
    for k in range(2 * N):
        j = inverse[k]
        for half in range(2):
            cols.append(right_ref[jnp.where(j < N, 2 * j + half, 2 * N)])
    core = dot(
        jnp.concatenate(rows, axis=0).astype(BF16), jnp.concatenate(cols, axis=0).astype(BF16), (1, 1)
    )
    core = core.astype(BF16).astype(F32)
    place = iota((64, 128), 1) // 16
    low_lanes = iota((8, 128), 1) < 64
    for k in range(2 * N):
        c, h = k // 2, k % 2
        total = jnp.zeros((64, 128), F32)
        for combo in range(4):
            x = core[64 * combo : 64 * combo + 64, 128 * (k // 8) : 128 * (k // 8) + 128]
            total = jnp.where(place == combo, move(x, 16 * (k % 8), 16 * combo), total)
        beside = pltpu.roll(total, 64, 1)
        j = inverse[k]
        tail = row_ref[j]
        for r in range(N):
            part = total[8 * r : 8 * r + 8]
            shifted = beside[8 * r : 8 * r + 8]
            i0 = inverse[2 * r]
            i1 = inverse[2 * r + 1]
            at0 = jnp.where((i0 < N) & (j < N), i0 * N + j, 64)
            at1 = jnp.where((i1 < N) & (j < N), i1 * N + j, 64)
            spare = jnp.where(low_lanes, pltpu.roll(part, 6, 0), pltpu.roll(shifted, 4, 0))
            send[(h * N + r) * N + c] = jnp.concatenate(
                [
                    t0[at0],
                    t0[at1],
                    g0[at0] + g1[at1],
                    jnp.where(valid, tail, spare),
                    jnp.where(valid, pair_ref[2 * r + c % 2], pltpu.roll(part, 2, 0)),
                ],
                axis=0,
            ).astype(BF16)


def gather_up(blocks, lefts, rights, row_v, cores, own_u, order_out):
    def tile(f, g, c, at):
        return blocks[f * 64 + g * N + c, 8 * at : 8 * at + 8, :].astype(F32)

    k = iota((TILE, TILE), 0)
    target = 64 * ((k // 8) % 8) + 8 * (k // 64) + k % 8
    order = (target == iota((TILE, TILE), 1)).astype(BF16)
    order_out[...] = order
    sub = iota((8, 128), 0)
    group = iota((64, 128), 1) // 16
    core_id = lax.axis_index("col") % 2
    of_slot = (sub >= 4, sub < 4)
    mixed = []
    own = []
    for f in range(2):
        for side, into in ((0, lefts), (1, rights)):
            lanes = ([], [])
            for m in range(4):
                x = [
                    blocks[f * 64 + g * N + 2 * m + side, 0:24, :].astype(F32) for g in range(N)
                ]
                for s in range(2):
                    rows = []
                    for y in x:
                        rest = y[16:24]
                        if side == 0:
                            rest = jnp.where(of_slot[s], rest, 0.0)
                        rows += [y[8 * s : 8 * s + 8], rest]
                    lanes[s].append(jnp.concatenate(rows, axis=0))
            for s in range(2):
                into[s, 128 * f : 128 * f + 128, :] = jnp.concatenate(lanes[s], axis=1).astype(BF16)
        parts = []
        for c in range(N):
            rows = []
            for g in range(N):
                x = tile(f, g, c, 3)
                y = tile(f, g, c, 4)
                y = jnp.where(sub < 4, pltpu.roll(pltpu.roll(x, 64, 1), 4, 0), pltpu.roll(y, 6, 0))
                y = jnp.where(sub < 2, pltpu.roll(x, 2, 0), y)
                rows.append(jnp.where(sub < 6, y, 0.0))
            parts.append(jnp.concatenate(rows, axis=0))
        for s in range(2):
            halves = []
            for half in range(2):
                total = jnp.zeros((64, 128), F32)
                combo = 2 * half + s
                for c in range(N):
                    total = jnp.where(group == c, move(parts[c], 16 * combo, 16 * c), total)
                halves.append(total)
            first = jnp.where(core_id == 0, halves[0], halves[1])
            second = jnp.where(core_id == 0, halves[1], halves[0])
            cores[2 * f + s] = jnp.concatenate([first, second], axis=0).astype(BF16)
        for c in range(N):
            mixed += spread([tile(f, g, c, 3) for g in range(N)])
        own += half_panels([[tile(f, g, c, 4) for c in range(N)] for g in range(N)])
    panels = jnp.concatenate(mixed + own, axis=0).astype(BF16)
    panels = dot(panels, order, (1, 0)).astype(BF16)
    row_v[...] = panels[:256]
    own_u[...] = panels[256:]


def half_panels(tiles):
    both = [spread(x) for x in tiles]
    return [jnp.concatenate([x[s] for x in both], axis=0) for s in range(2)]


def finish(twin, lefts, rights, row_v, cores, own_u, order, out, made, sems):
    other = []
    for f in range(2):
        other += half_panels(
            [[twin[f * 64 + g * N + c].astype(F32) for c in range(N)] for g in range(N)]
        )
    other = dot(jnp.concatenate(other, axis=0).astype(BF16), order[...], (1, 0)).astype(BF16)
    updates = [[], []]
    for f in range(2):
        for s in range(2):
            at = slice(64 * (2 * f + s), 64 * (2 * f + s) + 64)
            col_u = jnp.concatenate([own_u[at, :], other[at]], axis=0)
            updates[s].append((-dot(cores[2 * f + s], col_u, (0, 0))).astype(BF16))
    stores = []
    for s in range(2):
        both = jnp.concatenate([lefts[s]] + updates[s], axis=0)
        right = jnp.concatenate([rights[s], row_v[...]], axis=0)
        for part in range(2):
            rows = slice(256 * part, 256 * part + 256)
            made[s, rows, :] = dot(both[:, rows], right, (0, 0)).astype(BF16)
            copy = pltpu.make_async_copy(made.at[s, rows], out.at[s, rows], sems.at[2 * s + part])
            copy.start()
            stores.append(copy)
    for copy in stores:
        copy.wait()


def exchange(x, axes, name):
    with jax.named_scope(name):
        return lax.all_to_all(x, axes, split_axis=0, concat_axis=0, tiled=True)


def swap(x):
    return lax.ppermute(x, "col", [(k, k ^ 1) for k in range(N)])


def in_vmem(x):
    return pltpu.with_memory_space_constraint(x, VMEM)


def shards(
    pivot, col_ut, col_vt, col_rank, row_ut, row_vt, row_rank, cb_ut, cb_vt, cb_rank, parent_map
):
    sds = jax.ShapeDtypeStruct
    (send,) = call(
        pack,
        (VMEM((64, 40, 128), BF16),),
        (
            pivot[0],
            col_ut[0, 0].T,
            col_vt[0, 0].T,
            row_ut[0, 0].T,
            row_vt[0, 0].T,
            cb_ut[0, 0, 0],
            cb_vt[0, 0, 0],
            col_rank,
            row_rank,
            cb_rank,
        ),
        (VMEM,) * 7 + (SMEM,) * 3,
        name="pack",
        limit=None,
    )
    got = exchange(send, ("row", "col"), "scatter")
    other = in_vmem(swap(got[:, 16:40]))
    got = in_vmem(got)
    sorted_out = call(
        sort,
        (VMEM((65, 8, 128), F32),) * 3
        + (
            VMEM((64, TILE), F32),
            VMEM((2 * N + 1, 8, TILE), F32),
            VMEM((N + 1, 8, 128), F32),
            VMEM((2 * N, 8, 128), F32),
            VMEM((TILE, TILE // 2), BF16),
            VMEM((8, TILE), F32),
        ),
        (got, parent_map),
        (VMEM, VMEM),
        (SMEM((2 * N,), jnp.int32), VMEM((N + 1, 8, 128), F32)),
        name="sort",
    )
    (send,) = call(
        route,
        (VMEM((128, 40, 128), BF16),),
        (other, *(in_vmem(x) for x in sorted_out), parent_map),
        (VMEM,) * 11,
        (
            SMEM((2 * N,), jnp.int32),
            VMEM((2 * N + 1, 8, TILE), F32),
            VMEM((2, TILE, TILE // 2), BF16),
        ),
        name="route",
    )
    blocks = exchange(send, ("side", "row", "col"), "gather")
    twin = in_vmem(swap(blocks[:, 32:40]))
    blocks = in_vmem(blocks)
    gathered = call(
        gather_up,
        (
            VMEM((2, 256, TILE), BF16),
            VMEM((2, 256, TILE), BF16),
            VMEM((256, TILE), BF16),
            VMEM((4, 128, 128), BF16),
            VMEM((256, TILE), BF16),
            VMEM((TILE, TILE), BF16),
        ),
        (blocks,),
        (VMEM,),
        name="gather_up",
    )
    (out,) = call(
        finish,
        (sds((2, TILE, TILE), BF16),),
        (twin, *(in_vmem(x) for x in gathered)),
        (VMEM,) * 7,
        (
            VMEM((2, TILE, TILE), BF16),
            pltpu.SemaphoreType.DMA((4,)),
        ),
        name="finish",
        into=pl.ANY,
    )
    return out[None, :, None]


def solution(mesh):
    front = ("pair", "side")
    split = Mesh(mesh.devices.reshape(4, 2, N, N), ("pair", "side", "row", "col"))
    placed = (
        P(front, ("row", "col"), None),
        P(front, "row", None, "col"),
        P(front, "row", None, "col"),
        P(front, "row"),
        P(front, "col", None, "row"),
        P(front, "col", None, "row"),
        P(front, "col"),
        P(front, "row", "col", None, None),
        P(front, "row", "col", None, None),
        P(front, "row", "col"),
        P(front, None),
    )

    return jax.shard_map(
        shards,
        mesh=split,
        in_specs=placed,
        out_specs=P(front, "row", "col", None, None),
        check_vma=False,
    )
```

```python
import jax
import jax.numpy as jnp
from jax import lax
from jax.experimental import pallas as pl
from jax.experimental.pallas import tpu as pltpu
from jax.sharding import Mesh, PartitionSpec as P

F32 = jnp.float32
BF16 = jnp.bfloat16
RANK = 96
TILE = 512
N = 8
SMEM = pltpu.SMEM
VMEM = pltpu.VMEM


def iota(shape, dim):
    return lax.broadcasted_iota(jnp.int32, shape, dim)


def dot(a, b, contract):
    return lax.dot_general(
        a, b, ((contract[:1], contract[1:]), ((), ())), preferred_element_type=F32
    )


def call(body, outs, args, specs, scratch=(), name=None, into=VMEM, limit=24 * 2**20):
    kernel = pl.pallas_call(
        body,
        out_shape=outs,
        in_specs=[pl.BlockSpec(memory_space=s) for s in specs],
        out_specs=[pl.BlockSpec(memory_space=into) for _ in outs],
        scratch_shapes=scratch,
        compiler_params=pltpu.CompilerParams(vmem_limit_bytes=limit),
        name=name,
    )
    with jax.named_scope("do_" + name):
        return kernel(*args)


def fill_inverse(mapping, inverse):
    lane = iota((1, N), 1)
    x = mapping[...].astype(F32)
    scale = jnp.where(lane % 4 == 0, 1.0, jnp.where(lane % 4 == 1, 16.0, jnp.where(lane % 4 == 2, 256.0, 4096.0)))
    digits = [
        jnp.sum(jnp.where(lane // 4 == k, x * scale, 0.0)).astype(jnp.int32) for k in range(2)
    ]
    for k in range(2 * N):
        inverse[k] = N
    for k in range(N):
        inverse[(digits[k // 4] >> (4 * (k % 4))) & 15] = k


def onehot(offset):
    row = iota((64, RANK), 0)
    level = iota((64, RANK), 1)
    t = row % 8
    return ((t < 6) & (level == 12 * (row // 8) + offset + t)).astype(BF16)


def pack(piv, cu, cv, ru, rv, cbu, cbv, rank_c, rank_r, rank_b, send):
    level = iota((64, RANK), 1)
    even = onehot(0)
    odd = onehot(6)

    def panel(ref, rank):
        x = jnp.where(level < rank, ref[...].astype(F32), 0.0).astype(BF16)
        return jnp.concatenate([dot(even, x, (1, 1)), dot(odd, x, (1, 1))], axis=1)

    col_u = panel(cu, rank_c[0, 0]).astype(BF16)
    col_v = panel(cv, rank_c[0, 0])
    row_u = panel(ru, rank_r[0, 0])
    row_v = panel(rv, rank_r[0, 0]).astype(BF16)
    first_half = iota((64, 128), 1) < 64
    col_v = (
        jnp.where(first_half, col_v, 0.0),
        jnp.where(first_half, pltpu.roll(col_v, 64, 1), 0.0),
    )
    q = lax.axis_index("row") * N + lax.axis_index("col")
    full = piv[...]
    on_diag = iota((8, TILE), 1) == 8 * q + iota((8, TILE), 0)
    diag = jnp.sum(jnp.where(on_diag, full, 0.0), axis=1, keepdims=True)
    off = jnp.where(on_diag, 0.0, full)
    high = diag.astype(BF16).astype(F32)
    rest = diag - high
    mid = rest.astype(BF16).astype(F32)
    lane = iota((8, 128), 1)
    sub = iota((8, 128), 0)
    parts = jnp.zeros((8, 128), F32)
    for k, x in enumerate((high, mid, rest - mid)):
        parts = jnp.where(lane == 96 + 8 * k + sub, x, parts)
    parts = jnp.where(sub == 0, jnp.sum(parts, axis=0, keepdims=True), 0.0)
    pivot = [off[:, 128 * m : 128 * m + 128] for m in range(4)]
    wide = iota((RANK, TILE), 0)
    row = iota((64, RANK), 0)
    lev = iota((64, RANK), 1)
    t = row % 8
    extra = [
        ((t >= 6) & (lev == 64 + 4 * (row // 8) + 2 * e + t - 6)).astype(BF16) for e in range(2)
    ]
    from_lane = iota((128, 128), 0)
    place = iota((128, 128), 1) - 8 * (from_lane // 64) - from_lane % 64
    inside = from_lane % 64 // 8
    thin = []
    for g in range(N):
        thin.append(
            [
                dot(x, ((inside == g) & (place == at - 8 * g)).astype(BF16), (1, 0))
                for x, at in ((row_v, 64), (col_u, 80))
            ]
        )
    for side, ref in enumerate((cbu, cbv)):
        x = jnp.where(wide < rank_b[0, 0, 0], ref[...].astype(F32), 0.0)
        narrow = x.astype(BF16)
        x1 = dot(extra[0], narrow, (1, 0))
        x2 = dot(extra[1], narrow, (1, 0))
        for g in range(N):
            rows = slice(8 * g, 8 * g + 8)
            for m in range(4):
                lanes = slice(128 * m, 128 * m + 128)
                c = 2 * m + side
                cols = slice(8 * c, 8 * c + 8)
                send[g * N + c] = jnp.concatenate(
                    [
                        x[rows, lanes],
                        row_u[cols] + x1[rows, lanes],
                        col_v[side][rows] + thin[g][0][cols] + thin[c][1][rows] + parts + x2[rows, lanes],
                        pivot[2 * side],
                        pivot[2 * side + 1],
                    ],
                    axis=0,
                ).astype(BF16)


def spread(tiles):
    lane = iota(tiles[0].shape, 1)
    halves = ([], [])
    for m in range(N // 2):
        x, y = tiles[2 * m], tiles[2 * m + 1]
        halves[0].append(jnp.where(lane < 64, x, pltpu.roll(y, 64, 1)))
        halves[1].append(jnp.where(lane < 64, pltpu.roll(x, 64, 1), y))
    return [jnp.concatenate(h, axis=1) for h in halves]


def move(x, start, to):
    return pltpu.roll(x, (to - start) % 128, 1) if (to - start) % 128 else x


def panel_half(ref, i, at):
    sub = iota((8, 128), 0)
    lane = iota((8, 128), 1)
    x = [jnp.where(sub < 6, ref[i * N + j, at : at + 8, :].astype(F32), 0.0) for j in range(N)]
    return jnp.concatenate(
        [jnp.where(lane < 64, x[2 * m], pltpu.roll(x[2 * m + 1], 64, 1)) for m in range(4)], axis=1
    )


def pivot_half(ref, at):
    return jnp.concatenate(
        [
            ref[:, at + 8 * m : at + 8 * m + 8, :].astype(F32).reshape(TILE, 128).astype(BF16)
            for m in range(2)
        ],
        axis=1,
    )


def sort(
    got, t0, g0, g1, left, right_ref, row_ref, col_ref, off, inv
):
    sub = iota((8, 128), 0)
    lane = iota((8, 128), 1)
    valid = sub < 6
    zero = jnp.zeros((8, 128), F32)
    t0[64] = zero
    g0[64] = zero
    g1[64] = zero
    right = [[] for _ in range(N)]
    thin = [zero] * N
    diag = [zero] * 4
    group = lane // 8
    for i in range(N):
        thick = zero
        for j in range(N):
            k = i * N + j
            x = got[k, 0:24, :].astype(F32)
            a, b = x[8:16], x[16:24]
            t0[k] = x[0:8]
            g0[k] = jnp.where(sub >= 6, a, jnp.where(sub >= 4, pltpu.roll(b, 6, 0), 0.0))
            g1[k] = jnp.where(
                sub >= 4, 0.0, jnp.where(sub >= 2, pltpu.roll(a, 4, 0), pltpu.roll(b, 2, 0))
            )
            right[j].append(jnp.where(valid, a, 0.0))
            for half in range(2):
                thin[j] = jnp.where(group == 8 * half + i, move(b, 64 + 8 * half, 64 * half + 8 * i), thin[j])
                thick = jnp.where(group == 8 * half + j, move(b, 80 + 8 * half, 64 * half + 8 * j), thick)
            total = b + pltpu.roll(b, 120, 1) + pltpu.roll(b, 112, 1)
            to = 64 * (i % 2) + 8 * j
            diag[i // 2] = jnp.where(group == to // 8, move(total, 96, to), diag[i // 2])
        col_ref[i] = jnp.where(valid, thick, 0.0)
        left[8 * i : 8 * i + 8, :] = panel_half(got, i, 16)
    col_ref[N] = zero
    off[...] = pivot_half(got, 24)
    full = 1.0 / jnp.concatenate([x[0:1] for x in diag], axis=1)
    inv[...] = jnp.broadcast_to(full, (8, TILE))
    right_ref[2 * N] = jnp.zeros((8, TILE), F32)
    row_ref[N] = zero
    for j in range(N):
        parts = spread(right[j])
        right_ref[2 * j] = parts[0]
        right_ref[2 * j + 1] = parts[1]
        row_ref[j] = jnp.where(valid, thin[j], 0.0)


def route(
    other, t0, g0, g1, left, right_ref, row_ref, col_ref, off, inv, mapping, send, inverse, lower_ref, off_ref,
    pair_ref
):
    fill_inverse(mapping, inverse)
    core_id = lax.axis_index("col") % 2
    sub = iota((8, 128), 0)
    valid = sub < 6
    off_ref[core_id] = off[...]
    off_ref[1 - core_id] = pivot_half(other, 8)
    whole = jnp.concatenate([off_ref[0], off_ref[1]], axis=1)
    scale = inv[0:1, :]

    def times(x):
        high = x.astype(BF16)
        low = (x - high.astype(F32)).astype(BF16)
        both = dot(jnp.concatenate([high, low], axis=0), whole, (1, 0))
        return (both[:128] + both[128:]) * scale

    v = jnp.concatenate([left[...]] + [panel_half(other, i, 0) for i in range(N)], axis=0) * scale
    y = v - times(v)
    z = y + times(y)
    lower = 2.0 * y - z + times(z)
    for k in range(2 * N):
        lower_ref[k] = lower[8 * k : 8 * k + 8]
    lower_ref[2 * N] = jnp.zeros((8, TILE), F32)
    rows = []
    for half in range(2):
        for s in range(2):
            for r in range(N):
                i = inverse[2 * r + s]
                at = jnp.bitwise_xor(half, core_id) * N + i
                rows.append(lower_ref[jnp.where(i < N, at, 2 * N)])
    cols = []
    for k in range(2 * N):
        j = inverse[k]
        for half in range(2):
            cols.append(right_ref[jnp.where(j < N, 2 * j + half, 2 * N)])
    core = dot(
        jnp.concatenate(rows, axis=0).astype(BF16), jnp.concatenate(cols, axis=0).astype(BF16), (1, 1)
    )
    core = core.astype(BF16).astype(F32)
    place = iota((64, 128), 1) // 16
    lane = iota((8, 128), 1)
    low_lanes = lane < 64
    for r in range(N):
        x = col_ref[inverse[2 * r]]
        y = col_ref[inverse[2 * r + 1]]
        pair_ref[2 * r] = jnp.where(lane < 64, x, pltpu.roll(y, 64, 1))
        pair_ref[2 * r + 1] = jnp.where(lane < 64, pltpu.roll(x, 64, 1), y)
    for k in range(2 * N):
        c, h = k // 2, k % 2
        total = jnp.zeros((64, 128), F32)
        for combo in range(4):
            x = core[64 * combo : 64 * combo + 64, 128 * (k // 8) : 128 * (k // 8) + 128]
            total = jnp.where(place == combo, move(x, 16 * (k % 8), 16 * combo), total)
        beside = pltpu.roll(total, 64, 1)
        j = inverse[k]
        tail = row_ref[j]
        for r in range(N):
            part = total[8 * r : 8 * r + 8]
            shifted = beside[8 * r : 8 * r + 8]
            i0 = inverse[2 * r]
            i1 = inverse[2 * r + 1]
            at0 = jnp.where((i0 < N) & (j < N), i0 * N + j, 64)
            at1 = jnp.where((i1 < N) & (j < N), i1 * N + j, 64)
            spare = jnp.where(low_lanes, pltpu.roll(part, 6, 0), pltpu.roll(shifted, 4, 0))
            send[(h * N + r) * N + c] = jnp.concatenate(
                [
                    t0[at0],
                    t0[at1],
                    g0[at0] + g1[at1],
                    jnp.where(valid, tail, spare),
                    jnp.where(valid, pair_ref[2 * r + c % 2], pltpu.roll(part, 2, 0)),
                ],
                axis=0,
            ).astype(BF16)


def gather_up(blocks, lefts, rights, row_v, cores, own_u, order_out):
    def tile(f, g, c, at):
        return blocks[f * 64 + g * N + c, 8 * at : 8 * at + 8, :].astype(F32)

    k = iota((TILE, TILE), 0)
    target = 64 * ((k // 8) % 8) + 8 * (k // 64) + k % 8
    order = (target == iota((TILE, TILE), 1)).astype(BF16)
    order_out[...] = order
    sub = iota((8, 128), 0)
    group = iota((64, 128), 1) // 16
    core_id = lax.axis_index("col") % 2
    of_slot = (sub >= 4, sub < 4)
    mixed = []
    own = []
    for f in range(2):
        for side, into in ((0, lefts), (1, rights)):
            lanes = ([], [])
            for m in range(4):
                x = [
                    blocks[f * 64 + g * N + 2 * m + side, 0:24, :].astype(F32) for g in range(N)
                ]
                for s in range(2):
                    rows = []
                    for y in x:
                        rest = y[16:24]
                        if side == 0:
                            rest = jnp.where(of_slot[s], rest, 0.0)
                        rows += [y[8 * s : 8 * s + 8], rest]
                    lanes[s].append(jnp.concatenate(rows, axis=0))
            for s in range(2):
                into[s, 128 * f : 128 * f + 128, :] = jnp.concatenate(lanes[s], axis=1).astype(BF16)
        parts = []
        for c in range(N):
            rows = []
            for g in range(N):
                x = tile(f, g, c, 3)
                y = tile(f, g, c, 4)
                y = jnp.where(sub < 4, pltpu.roll(pltpu.roll(x, 64, 1), 4, 0), pltpu.roll(y, 6, 0))
                y = jnp.where(sub < 2, pltpu.roll(x, 2, 0), y)
                rows.append(jnp.where(sub < 6, y, 0.0))
            parts.append(jnp.concatenate(rows, axis=0))
        for s in range(2):
            halves = []
            for half in range(2):
                total = jnp.zeros((64, 128), F32)
                combo = 2 * half + s
                for c in range(N):
                    total = jnp.where(group == c, move(parts[c], 16 * combo, 16 * c), total)
                halves.append(total)
            first = jnp.where(core_id == 0, halves[0], halves[1])
            second = jnp.where(core_id == 0, halves[1], halves[0])
            cores[2 * f + s] = jnp.concatenate([first, second], axis=0).astype(BF16)
        for c in range(N):
            mixed += spread([tile(f, g, c, 3) for g in range(N)])
        own += half_panels([[tile(f, g, c, 4) for c in range(N)] for g in range(N)])
    panels = jnp.concatenate(mixed + own, axis=0).astype(BF16)
    panels = dot(panels, order, (1, 0)).astype(BF16)
    row_v[...] = panels[:256]
    own_u[...] = panels[256:]


def half_panels(tiles):
    both = [spread(x) for x in tiles]
    return [jnp.concatenate([x[s] for x in both], axis=0) for s in range(2)]


def finish(twin, lefts, rights, row_v, cores, own_u, order, out, made, sems):
    other = []
    for f in range(2):
        other += half_panels(
            [[twin[f * 64 + g * N + c].astype(F32) for c in range(N)] for g in range(N)]
        )
    other = dot(jnp.concatenate(other, axis=0).astype(BF16), order[...], (1, 0)).astype(BF16)
    updates = [[], []]
    for f in range(2):
        for s in range(2):
            at = slice(64 * (2 * f + s), 64 * (2 * f + s) + 64)
            col_u = jnp.concatenate([own_u[at, :], other[at]], axis=0)
            updates[s].append((-dot(cores[2 * f + s], col_u, (0, 0))).astype(BF16))
    stores = []
    for s in range(2):
        both = jnp.concatenate([lefts[s]] + updates[s], axis=0)
        right = jnp.concatenate([rights[s], row_v[...]], axis=0)
        for part in range(4):
            rows = slice(128 * part, 128 * part + 128)
            made[s, rows, :] = dot(both[:, rows], right, (0, 0)).astype(BF16)
            copy = pltpu.make_async_copy(made.at[s, rows], out.at[s, rows], sems.at[4 * s + part])
            copy.start()
            stores.append(copy)
    for copy in stores:
        copy.wait()


def exchange(x, axes, name):
    with jax.named_scope(name):
        return lax.all_to_all(x, axes, split_axis=0, concat_axis=0, tiled=True)


def swap(x):
    return lax.ppermute(x, "col", [(k, k ^ 1) for k in range(N)])


def in_vmem(x):
    return pltpu.with_memory_space_constraint(x, VMEM)


def shards(
    pivot, col_ut, col_vt, col_rank, row_ut, row_vt, row_rank, cb_ut, cb_vt, cb_rank, parent_map
):
    sds = jax.ShapeDtypeStruct
    (send,) = call(
        pack,
        (VMEM((64, 40, 128), BF16),),
        (
            pivot[0],
            col_ut[0, 0].T,
            col_vt[0, 0].T,
            row_ut[0, 0].T,
            row_vt[0, 0].T,
            cb_ut[0, 0, 0],
            cb_vt[0, 0, 0],
            col_rank,
            row_rank,
            cb_rank,
        ),
        (VMEM,) * 7 + (SMEM,) * 3,
        name="pack",
        limit=None,
    )
    got = exchange(send, ("row", "col"), "scatter")
    other = in_vmem(swap(got[:, 16:40]))
    got = in_vmem(got)
    sorted_out = call(
        sort,
        (VMEM((65, 8, 128), F32),) * 3
        + (
            VMEM((64, TILE), F32),
            VMEM((2 * N + 1, 8, TILE), F32),
            VMEM((N + 1, 8, 128), F32),
            VMEM((N + 1, 8, 128), F32),
            VMEM((TILE, TILE // 2), BF16),
            VMEM((8, TILE), F32),
        ),
        (got,),
        (VMEM,),
        name="sort",
    )
    (send,) = call(
        route,
        (VMEM((128, 40, 128), BF16),),
        (other, *(in_vmem(x) for x in sorted_out), parent_map),
        (VMEM,) * 11,
        (
            SMEM((2 * N,), jnp.int32),
            VMEM((2 * N + 1, 8, TILE), F32),
            VMEM((2, TILE, TILE // 2), BF16),
            VMEM((2 * N, 8, 128), F32),
        ),
        name="route",
    )
    blocks = exchange(send, ("side", "row", "col"), "gather")
    twin = in_vmem(swap(blocks[:, 32:40]))
    blocks = in_vmem(blocks)
    gathered = call(
        gather_up,
        (
            VMEM((2, 256, TILE), BF16),
            VMEM((2, 256, TILE), BF16),
            VMEM((256, TILE), BF16),
            VMEM((4, 128, 128), BF16),
            VMEM((256, TILE), BF16),
            VMEM((TILE, TILE), BF16),
        ),
        (blocks,),
        (VMEM,),
        name="gather_up",
    )
    (out,) = call(
        finish,
        (sds((2, TILE, TILE), BF16),),
        (twin, *(in_vmem(x) for x in gathered)),
        (VMEM,) * 7,
        (
            VMEM((2, TILE, TILE), BF16),
            pltpu.SemaphoreType.DMA((8,)),
        ),
        name="finish",
        into=pl.ANY,
    )
    return out[None, :, None]


def solution(mesh):
    front = ("pair", "side")
    split = Mesh(mesh.devices.reshape(4, 2, N, N), ("pair", "side", "row", "col"))
    placed = (
        P(front, ("row", "col"), None),
        P(front, "row", None, "col"),
        P(front, "row", None, "col"),
        P(front, "row"),
        P(front, "col", None, "row"),
        P(front, "col", None, "row"),
        P(front, "col"),
        P(front, "row", "col", None, None),
        P(front, "row", "col", None, None),
        P(front, "row", "col"),
        P(front, None),
    )

    return jax.shard_map(
        shards,
        mesh=split,
        in_specs=placed,
        out_specs=P(front, "row", "col", None, None),
        check_vma=False,
    )
```

```python
import jax
import jax.numpy as jnp
from jax import lax
from jax.experimental import pallas as pl
from jax.experimental.pallas import tpu as pltpu
from jax.sharding import Mesh, PartitionSpec as P

F32 = jnp.float32
BF16 = jnp.bfloat16
RANK = 96
TILE = 512
N = 8
SMEM = pltpu.SMEM
VMEM = pltpu.VMEM


def iota(shape, dim):
    return lax.broadcasted_iota(jnp.int32, shape, dim)


def dot(a, b, contract):
    return lax.dot_general(
        a, b, ((contract[:1], contract[1:]), ((), ())), preferred_element_type=F32
    )


def call(body, outs, args, specs, scratch=(), name=None, into=VMEM, limit=24 * 2**20):
    kernel = pl.pallas_call(
        body,
        out_shape=outs,
        in_specs=[pl.BlockSpec(memory_space=s) for s in specs],
        out_specs=[pl.BlockSpec(memory_space=into) for _ in outs],
        scratch_shapes=scratch,
        compiler_params=pltpu.CompilerParams(vmem_limit_bytes=limit),
        name=name,
    )
    with jax.named_scope("do_" + name):
        return kernel(*args)


def fill_inverse(mapping, inverse):
    lane = iota((1, N), 1)
    x = mapping[...].astype(F32)
    scale = jnp.where(lane % 4 == 0, 1.0, jnp.where(lane % 4 == 1, 16.0, jnp.where(lane % 4 == 2, 256.0, 4096.0)))
    digits = [
        jnp.sum(jnp.where(lane // 4 == k, x * scale, 0.0)).astype(jnp.int32) for k in range(2)
    ]
    for k in range(2 * N):
        inverse[k] = N
    for k in range(N):
        inverse[(digits[k // 4] >> (4 * (k % 4))) & 15] = k


def onehot(offset):
    row = iota((64, RANK), 0)
    level = iota((64, RANK), 1)
    t = row % 8
    return ((t < 6) & (level == 12 * (row // 8) + offset + t)).astype(BF16)


def pack(piv, cu, cv, ru, rv, cbu, cbv, rank_c, rank_r, rank_b, send):
    level = iota((64, RANK), 1)
    even = onehot(0)
    odd = onehot(6)

    def panel(ref, rank):
        x = jnp.where(level < rank, ref[...].astype(F32), 0.0).astype(BF16)
        return jnp.concatenate([dot(even, x, (1, 1)), dot(odd, x, (1, 1))], axis=1)

    col_u = panel(cu, rank_c[0, 0]).astype(BF16)
    col_v = panel(cv, rank_c[0, 0])
    row_u = panel(ru, rank_r[0, 0])
    row_v = panel(rv, rank_r[0, 0]).astype(BF16)
    first_half = iota((64, 128), 1) < 64
    col_v = (
        jnp.where(first_half, col_v, 0.0),
        jnp.where(first_half, pltpu.roll(col_v, 64, 1), 0.0),
    )
    q = lax.axis_index("row") * N + lax.axis_index("col")
    full = piv[...]
    on_diag = iota((8, TILE), 1) == 8 * q + iota((8, TILE), 0)
    diag = jnp.sum(jnp.where(on_diag, full, 0.0), axis=1, keepdims=True)
    off = jnp.where(on_diag, 0.0, full)
    high = diag.astype(BF16).astype(F32)
    rest = diag - high
    mid = rest.astype(BF16).astype(F32)
    lane = iota((8, 128), 1)
    sub = iota((8, 128), 0)
    parts = jnp.zeros((8, 128), F32)
    for k, x in enumerate((high, mid, rest - mid)):
        parts = jnp.where(lane == 96 + 8 * k + sub, x, parts)
    parts = jnp.where(sub == 0, jnp.sum(parts, axis=0, keepdims=True), 0.0)
    pivot = [off[:, 128 * m : 128 * m + 128] for m in range(4)]
    wide = iota((RANK, TILE), 0)
    row = iota((64, RANK), 0)
    lev = iota((64, RANK), 1)
    t = row % 8
    extra = [
        ((t >= 6) & (lev == 64 + 4 * (row // 8) + 2 * e + t - 6)).astype(BF16) for e in range(2)
    ]
    from_lane = iota((128, 128), 0)
    place = iota((128, 128), 1) - 8 * (from_lane // 64) - from_lane % 64
    inside = from_lane % 64 // 8
    thin = []
    for g in range(N):
        thin.append(
            [
                dot(x, ((inside == g) & (place == at - 8 * g)).astype(BF16), (1, 0))
                for x, at in ((row_v, 64), (col_u, 80))
            ]
        )
    for side, ref in enumerate((cbu, cbv)):
        x = jnp.where(wide < rank_b[0, 0, 0], ref[...].astype(F32), 0.0)
        narrow = x.astype(BF16)
        x1 = dot(extra[0], narrow, (1, 0))
        x2 = dot(extra[1], narrow, (1, 0))
        for g in range(N):
            rows = slice(8 * g, 8 * g + 8)
            for m in range(4):
                lanes = slice(128 * m, 128 * m + 128)
                c = 2 * m + side
                cols = slice(8 * c, 8 * c + 8)
                send[g * N + c] = jnp.concatenate(
                    [
                        x[rows, lanes],
                        row_u[cols] + x1[rows, lanes],
                        col_v[side][rows] + thin[g][0][cols] + thin[c][1][rows] + parts + x2[rows, lanes],
                        pivot[2 * side],
                        pivot[2 * side + 1],
                    ],
                    axis=0,
                ).astype(BF16)


def spread(tiles):
    lane = iota(tiles[0].shape, 1)
    halves = ([], [])
    for m in range(N // 2):
        x, y = tiles[2 * m], tiles[2 * m + 1]
        halves[0].append(jnp.where(lane < 64, x, pltpu.roll(y, 64, 1)))
        halves[1].append(jnp.where(lane < 64, pltpu.roll(x, 64, 1), y))
    return [jnp.concatenate(h, axis=1) for h in halves]


def move(x, start, to):
    return pltpu.roll(x, (to - start) % 128, 1) if (to - start) % 128 else x


def panel_half(ref, i, at):
    sub = iota((8, 128), 0)
    lane = iota((8, 128), 1)
    x = [jnp.where(sub < 6, ref[i * N + j, at : at + 8, :].astype(F32), 0.0) for j in range(N)]
    return jnp.concatenate(
        [jnp.where(lane < 64, x[2 * m], pltpu.roll(x[2 * m + 1], 64, 1)) for m in range(4)], axis=1
    )


def pivot_half(ref, at):
    return jnp.concatenate(
        [
            ref[:, at + 8 * m : at + 8 * m + 8, :].astype(F32).reshape(TILE, 128).astype(BF16)
            for m in range(2)
        ],
        axis=1,
    )


def sort(
    got, t0, g0, g1, left, right_ref, row_ref, col_ref, off, inv
):
    sub = iota((8, 128), 0)
    lane = iota((8, 128), 1)
    valid = sub < 6
    zero = jnp.zeros((8, 128), F32)
    for k in range(N + 1):
        for at in sorted({N * (N + 1) + k, k * (N + 1) + N}):
            t0[at] = zero
            g0[at] = zero
            g1[at] = zero
    right = [[] for _ in range(N)]
    thin = [zero] * N
    diag = [zero] * 4
    group = lane // 8
    for i in range(N):
        thick = zero
        for j in range(N):
            k = i * N + j
            x = got[k, 0:24, :].astype(F32)
            a, b = x[8:16], x[16:24]
            at = i * (N + 1) + j
            t0[at] = x[0:8]
            g0[at] = jnp.where(sub >= 6, a, jnp.where(sub >= 4, pltpu.roll(b, 6, 0), 0.0))
            g1[at] = jnp.where(
                sub >= 4, 0.0, jnp.where(sub >= 2, pltpu.roll(a, 4, 0), pltpu.roll(b, 2, 0))
            )
            right[j].append(jnp.where(valid, a, 0.0))
            for half in range(2):
                thin[j] = jnp.where(group == 8 * half + i, move(b, 64 + 8 * half, 64 * half + 8 * i), thin[j])
                thick = jnp.where(group == 8 * half + j, move(b, 80 + 8 * half, 64 * half + 8 * j), thick)
            total = b + pltpu.roll(b, 120, 1) + pltpu.roll(b, 112, 1)
            to = 64 * (i % 2) + 8 * j
            diag[i // 2] = jnp.where(group == to // 8, move(total, 96, to), diag[i // 2])
        col_ref[i] = jnp.where(valid, thick, 0.0)
        left[8 * i : 8 * i + 8, :] = panel_half(got, i, 16)
    col_ref[N] = zero
    off[...] = pivot_half(got, 24)
    full = 1.0 / jnp.concatenate([x[0:1] for x in diag], axis=1)
    inv[...] = jnp.broadcast_to(full, (8, TILE))
    right_ref[2 * N] = jnp.zeros((8, TILE), F32)
    right_ref[2 * N + 1] = jnp.zeros((8, TILE), F32)
    row_ref[N] = zero
    for j in range(N):
        parts = spread(right[j])
        right_ref[2 * j] = parts[0]
        right_ref[2 * j + 1] = parts[1]
        row_ref[j] = jnp.where(valid, thin[j], 0.0)


def route(
    other, t0, g0, g1, left, right_ref, row_ref, col_ref, off, inv, mapping, send, inverse, lower_ref, off_ref,
    pair_ref
):
    fill_inverse(mapping, inverse)
    core_id = lax.axis_index("col") % 2
    sub = iota((8, 128), 0)
    valid = sub < 6
    off_ref[core_id] = off[...]
    off_ref[1 - core_id] = pivot_half(other, 8)
    whole = jnp.concatenate([off_ref[0], off_ref[1]], axis=1)
    scale = inv[0:1, :]

    def times(x):
        high = x.astype(BF16)
        low = (x - high.astype(F32)).astype(BF16)
        both = dot(jnp.concatenate([high, low], axis=0), whole, (1, 0))
        return (both[:128] + both[128:]) * scale

    v = jnp.concatenate([left[...]] + [panel_half(other, i, 0) for i in range(N)], axis=0) * scale
    y = v - times(v)
    z = y + times(y)
    lower = 2.0 * y - z + times(z)
    for half in range(2):
        for i in range(N):
            at = 8 * (half * N + i)
            lower_ref[half * (N + 1) + i] = lower[at : at + 8]
        lower_ref[half * (N + 1) + N] = jnp.zeros((8, TILE), F32)
    index = [inverse[k] for k in range(2 * N)]
    rows = []
    for half in range(2):
        for s in range(2):
            for r in range(N):
                rows.append(lower_ref[jnp.bitwise_xor(half, core_id) * (N + 1) + index[2 * r + s]])
    cols = []
    for k in range(2 * N):
        for half in range(2):
            cols.append(right_ref[2 * index[k] + half])
    core = dot(
        jnp.concatenate(rows, axis=0).astype(BF16), jnp.concatenate(cols, axis=0).astype(BF16), (1, 1)
    )
    core = core.astype(BF16).astype(F32)
    first = [(N + 1) * x for x in index]
    place = iota((64, 128), 1) // 16
    lane = iota((8, 128), 1)
    low_lanes = lane < 64
    for r in range(N):
        x = col_ref[index[2 * r]]
        y = col_ref[index[2 * r + 1]]
        pair_ref[2 * r] = jnp.where(lane < 64, x, pltpu.roll(y, 64, 1))
        pair_ref[2 * r + 1] = jnp.where(lane < 64, pltpu.roll(x, 64, 1), y)
    for k in range(2 * N):
        c, h = k // 2, k % 2
        total = jnp.zeros((64, 128), F32)
        for combo in range(4):
            x = core[64 * combo : 64 * combo + 64, 128 * (k // 8) : 128 * (k // 8) + 128]
            total = jnp.where(place == combo, move(x, 16 * (k % 8), 16 * combo), total)
        beside = pltpu.roll(total, 64, 1)
        j = index[k]
        tail = row_ref[j]
        for r in range(N):
            part = total[8 * r : 8 * r + 8]
            shifted = beside[8 * r : 8 * r + 8]
            at0 = first[2 * r] + j
            at1 = first[2 * r + 1] + j
            spare = jnp.where(low_lanes, pltpu.roll(part, 6, 0), pltpu.roll(shifted, 4, 0))
            send[(h * N + r) * N + c] = jnp.concatenate(
                [
                    t0[at0],
                    t0[at1],
                    g0[at0] + g1[at1],
                    jnp.where(valid, tail, spare),
                    jnp.where(valid, pair_ref[2 * r + c % 2], pltpu.roll(part, 2, 0)),
                ],
                axis=0,
            ).astype(BF16)


def gather_up(blocks, lefts, rights, row_v, cores, own_u, order_out):
    def tile(f, g, c, at):
        return blocks[f * 64 + g * N + c, 8 * at : 8 * at + 8, :].astype(F32)

    k = iota((TILE, TILE), 0)
    target = 64 * ((k // 8) % 8) + 8 * (k // 64) + k % 8
    order = (target == iota((TILE, TILE), 1)).astype(BF16)
    order_out[...] = order
    sub = iota((8, 128), 0)
    group = iota((64, 128), 1) // 16
    core_id = lax.axis_index("col") % 2
    of_slot = (sub >= 4, sub < 4)
    mixed = []
    own = []
    for f in range(2):
        for side, into in ((0, lefts), (1, rights)):
            lanes = ([], [])
            for m in range(4):
                x = [
                    blocks[f * 64 + g * N + 2 * m + side, 0:24, :].astype(F32) for g in range(N)
                ]
                for s in range(2):
                    rows = []
                    for y in x:
                        rest = y[16:24]
                        if side == 0:
                            rest = jnp.where(of_slot[s], rest, 0.0)
                        rows += [y[8 * s : 8 * s + 8], rest]
                    lanes[s].append(jnp.concatenate(rows, axis=0))
            for s in range(2):
                into[s, 128 * f : 128 * f + 128, :] = jnp.concatenate(lanes[s], axis=1).astype(BF16)
        parts = []
        for c in range(N):
            rows = []
            for g in range(N):
                x = tile(f, g, c, 3)
                y = tile(f, g, c, 4)
                y = jnp.where(sub < 4, pltpu.roll(pltpu.roll(x, 64, 1), 4, 0), pltpu.roll(y, 6, 0))
                y = jnp.where(sub < 2, pltpu.roll(x, 2, 0), y)
                rows.append(jnp.where(sub < 6, y, 0.0))
            parts.append(jnp.concatenate(rows, axis=0))
        for s in range(2):
            halves = []
            for half in range(2):
                total = jnp.zeros((64, 128), F32)
                combo = 2 * half + s
                for c in range(N):
                    total = jnp.where(group == c, move(parts[c], 16 * combo, 16 * c), total)
                halves.append(total)
            first = jnp.where(core_id == 0, halves[0], halves[1])
            second = jnp.where(core_id == 0, halves[1], halves[0])
            cores[2 * f + s] = jnp.concatenate([first, second], axis=0).astype(BF16)
        for c in range(N):
            mixed += spread([tile(f, g, c, 3) for g in range(N)])
        own += half_panels([[tile(f, g, c, 4) for c in range(N)] for g in range(N)])
    panels = jnp.concatenate(mixed + own, axis=0).astype(BF16)
    panels = dot(panels, order, (1, 0)).astype(BF16)
    row_v[...] = panels[:256]
    own_u[...] = panels[256:]


def half_panels(tiles):
    both = [spread(x) for x in tiles]
    return [jnp.concatenate([x[s] for x in both], axis=0) for s in range(2)]


def finish(twin, lefts, rights, row_v, cores, own_u, order, out, made, sems):
    other = []
    for f in range(2):
        other += half_panels(
            [[twin[f * 64 + g * N + c].astype(F32) for c in range(N)] for g in range(N)]
        )
    other = dot(jnp.concatenate(other, axis=0).astype(BF16), order[...], (1, 0)).astype(BF16)
    updates = [[], []]
    for f in range(2):
        for s in range(2):
            at = slice(64 * (2 * f + s), 64 * (2 * f + s) + 64)
            col_u = jnp.concatenate([own_u[at, :], other[at]], axis=0)
            updates[s].append((-dot(cores[2 * f + s], col_u, (0, 0))).astype(BF16))
    stores = []
    for s in range(2):
        both = jnp.concatenate([lefts[s]] + updates[s], axis=0)
        right = jnp.concatenate([rights[s], row_v[...]], axis=0)
        for part in range(4):
            rows = slice(128 * part, 128 * part + 128)
            made[s, rows, :] = dot(both[:, rows], right, (0, 0)).astype(BF16)
            copy = pltpu.make_async_copy(made.at[s, rows], out.at[s, rows], sems.at[4 * s + part])
            copy.start()
            stores.append(copy)
    for copy in stores:
        copy.wait()


def exchange(x, axes, name):
    with jax.named_scope(name):
        return lax.all_to_all(x, axes, split_axis=0, concat_axis=0, tiled=True)


def swap(x):
    return lax.ppermute(x, "col", [(k, k ^ 1) for k in range(N)])


def in_vmem(x):
    return pltpu.with_memory_space_constraint(x, VMEM)


def shards(
    pivot, col_ut, col_vt, col_rank, row_ut, row_vt, row_rank, cb_ut, cb_vt, cb_rank, parent_map
):
    sds = jax.ShapeDtypeStruct
    (send,) = call(
        pack,
        (VMEM((64, 40, 128), BF16),),
        (
            pivot[0],
            col_ut[0, 0].T,
            col_vt[0, 0].T,
            row_ut[0, 0].T,
            row_vt[0, 0].T,
            cb_ut[0, 0, 0],
            cb_vt[0, 0, 0],
            col_rank,
            row_rank,
            cb_rank,
        ),
        (VMEM,) * 7 + (SMEM,) * 3,
        name="pack",
        limit=None,
    )
    got = exchange(send, ("row", "col"), "scatter")
    other = in_vmem(swap(got[:, 16:40]))
    got = in_vmem(got)
    sorted_out = call(
        sort,
        (VMEM(((N + 1) ** 2, 8, 128), F32),) * 3
        + (
            VMEM((64, TILE), F32),
            VMEM((2 * N + 2, 8, TILE), F32),
            VMEM((N + 1, 8, 128), F32),
            VMEM((N + 1, 8, 128), F32),
            VMEM((TILE, TILE // 2), BF16),
            VMEM((8, TILE), F32),
        ),
        (got,),
        (VMEM,),
        name="sort",
    )
    (send,) = call(
        route,
        (VMEM((128, 40, 128), BF16),),
        (other, *(in_vmem(x) for x in sorted_out), parent_map),
        (VMEM,) * 11,
        (
            SMEM((2 * N,), jnp.int32),
            VMEM((2 * N + 2, 8, TILE), F32),
            VMEM((2, TILE, TILE // 2), BF16),
            VMEM((2 * N, 8, 128), F32),
        ),
        name="route",
    )
    blocks = exchange(send, ("side", "row", "col"), "gather")
    twin = in_vmem(swap(blocks[:, 32:40]))
    blocks = in_vmem(blocks)
    gathered = call(
        gather_up,
        (
            VMEM((2, 256, TILE), BF16),
            VMEM((2, 256, TILE), BF16),
            VMEM((256, TILE), BF16),
            VMEM((4, 128, 128), BF16),
            VMEM((256, TILE), BF16),
            VMEM((TILE, TILE), BF16),
        ),
        (blocks,),
        (VMEM,),
        name="gather_up",
    )
    (out,) = call(
        finish,
        (sds((2, TILE, TILE), BF16),),
        (twin, *(in_vmem(x) for x in gathered)),
        (VMEM,) * 7,
        (
            VMEM((2, TILE, TILE), BF16),
            pltpu.SemaphoreType.DMA((8,)),
        ),
        name="finish",
        into=pl.ANY,
    )
    return out[None, :, None]


def solution(mesh):
    front = ("pair", "side")
    split = Mesh(mesh.devices.reshape(4, 2, N, N), ("pair", "side", "row", "col"))
    placed = (
        P(front, ("row", "col"), None),
        P(front, "row", None, "col"),
        P(front, "row", None, "col"),
        P(front, "row"),
        P(front, "col", None, "row"),
        P(front, "col", None, "row"),
        P(front, "col"),
        P(front, "row", "col", None, None),
        P(front, "row", "col", None, None),
        P(front, "row", "col"),
        P(front, None),
    )

    return jax.shard_map(
        shards,
        mesh=split,
        in_specs=placed,
        out_specs=P(front, "row", "col", None, None),
        check_vma=False,
    )
```

```python
import jax
import jax.numpy as jnp
from jax import lax
from jax.experimental import pallas as pl
from jax.experimental.pallas import tpu as pltpu
from jax.sharding import Mesh, PartitionSpec as P

F32 = jnp.float32
BF16 = jnp.bfloat16
RANK = 96
TILE = 512
N = 8
SMEM = pltpu.SMEM
VMEM = pltpu.VMEM


def iota(shape, dim):
    return lax.broadcasted_iota(jnp.int32, shape, dim)


def dot(a, b, contract):
    return lax.dot_general(
        a, b, ((contract[:1], contract[1:]), ((), ())), preferred_element_type=F32
    )


def call(body, outs, args, specs, scratch=(), name=None, into=VMEM, limit=24 * 2**20):
    kernel = pl.pallas_call(
        body,
        out_shape=outs,
        in_specs=[pl.BlockSpec(memory_space=s) for s in specs],
        out_specs=[pl.BlockSpec(memory_space=into) for _ in outs],
        scratch_shapes=scratch,
        compiler_params=pltpu.CompilerParams(vmem_limit_bytes=limit),
        name=name,
    )
    with jax.named_scope("do_" + name):
        return kernel(*args)


def fill_inverse(mapping, inverse):
    lane = iota((1, N), 1)
    x = mapping[...].astype(F32)
    scale = jnp.where(lane % 4 == 0, 1.0, jnp.where(lane % 4 == 1, 16.0, jnp.where(lane % 4 == 2, 256.0, 4096.0)))
    digits = [
        jnp.sum(jnp.where(lane // 4 == k, x * scale, 0.0)).astype(jnp.int32) for k in range(2)
    ]
    for k in range(2 * N):
        inverse[k] = N
    for k in range(N):
        inverse[(digits[k // 4] >> (4 * (k % 4))) & 15] = k


def onehot(offset):
    row = iota((64, RANK), 0)
    level = iota((64, RANK), 1)
    t = row % 8
    return ((t < 6) & (level == 12 * (row // 8) + offset + t)).astype(BF16)


def pack(piv, cu, cv, ru, rv, cbu, cbv, rank_c, rank_r, rank_b, send):
    level = iota((64, RANK), 1)
    even = onehot(0)
    odd = onehot(6)

    def panel(ref, rank):
        x = jnp.where(level < rank, ref[...].astype(F32), 0.0).astype(BF16)
        return jnp.concatenate([dot(even, x, (1, 1)), dot(odd, x, (1, 1))], axis=1)

    col_u = panel(cu, rank_c[0, 0]).astype(BF16)
    col_v = panel(cv, rank_c[0, 0])
    row_u = panel(ru, rank_r[0, 0])
    row_v = panel(rv, rank_r[0, 0]).astype(BF16)
    first_half = iota((64, 128), 1) < 64
    col_v = (
        jnp.where(first_half, col_v, 0.0),
        jnp.where(first_half, pltpu.roll(col_v, 64, 1), 0.0),
    )
    q = lax.axis_index("row") * N + lax.axis_index("col")
    full = piv[...]
    on_diag = iota((8, TILE), 1) == 8 * q + iota((8, TILE), 0)
    diag = jnp.sum(jnp.where(on_diag, full, 0.0), axis=1, keepdims=True)
    off = jnp.where(on_diag, 0.0, full)
    high = diag.astype(BF16).astype(F32)
    rest = diag - high
    mid = rest.astype(BF16).astype(F32)
    lane = iota((8, 128), 1)
    sub = iota((8, 128), 0)
    parts = jnp.zeros((8, 128), F32)
    for k, x in enumerate((high, mid, rest - mid)):
        parts = jnp.where(lane == 96 + 8 * k + sub, x, parts)
    parts = jnp.where(sub == 0, jnp.sum(parts, axis=0, keepdims=True), 0.0)
    pivot = [off[:, 128 * m : 128 * m + 128] for m in range(4)]
    wide = iota((RANK, TILE), 0)
    row = iota((64, RANK), 0)
    lev = iota((64, RANK), 1)
    t = row % 8
    extra = [
        ((t >= 6) & (lev == 64 + 4 * (row // 8) + 2 * e + t - 6)).astype(BF16) for e in range(2)
    ]
    from_lane = iota((128, 128), 0)
    place = iota((128, 128), 1) - 8 * (from_lane // 64) - from_lane % 64
    inside = from_lane % 64 // 8
    thin = []
    for g in range(N):
        thin.append(
            [
                dot(x, ((inside == g) & (place == at - 8 * g)).astype(BF16), (1, 0))
                for x, at in ((row_v, 64), (col_u, 80))
            ]
        )
    for side, ref in enumerate((cbu, cbv)):
        x = jnp.where(wide < rank_b[0, 0, 0], ref[...].astype(F32), 0.0)
        narrow = x.astype(BF16)
        x1 = dot(extra[0], narrow, (1, 0))
        x2 = dot(extra[1], narrow, (1, 0))
        for g in range(N):
            rows = slice(8 * g, 8 * g + 8)
            for m in range(4):
                lanes = slice(128 * m, 128 * m + 128)
                c = 2 * m + side
                cols = slice(8 * c, 8 * c + 8)
                send[g * N + c] = jnp.concatenate(
                    [
                        x[rows, lanes],
                        row_u[cols] + x1[rows, lanes],
                        col_v[side][rows] + thin[g][0][cols] + thin[c][1][rows] + parts + x2[rows, lanes],
                        pivot[2 * side],
                        pivot[2 * side + 1],
                    ],
                    axis=0,
                ).astype(BF16)


def spread(tiles):
    lane = iota(tiles[0].shape, 1)
    halves = ([], [])
    for m in range(N // 2):
        x, y = tiles[2 * m], tiles[2 * m + 1]
        halves[0].append(jnp.where(lane < 64, x, pltpu.roll(y, 64, 1)))
        halves[1].append(jnp.where(lane < 64, pltpu.roll(x, 64, 1), y))
    return [jnp.concatenate(h, axis=1) for h in halves]


def move(x, start, to):
    return pltpu.roll(x, (to - start) % 128, 1) if (to - start) % 128 else x


def panel_half(ref, i, at):
    sub = iota((8, 128), 0)
    lane = iota((8, 128), 1)
    x = [jnp.where(sub < 6, ref[i * N + j, at : at + 8, :].astype(F32), 0.0) for j in range(N)]
    return jnp.concatenate(
        [jnp.where(lane < 64, x[2 * m], pltpu.roll(x[2 * m + 1], 64, 1)) for m in range(4)], axis=1
    )


def pivot_half(ref, at):
    return jnp.concatenate(
        [
            ref[:, at + 8 * m : at + 8 * m + 8, :].astype(F32).reshape(TILE, 128).astype(BF16)
            for m in range(2)
        ],
        axis=1,
    )


def sort(
    got, t0, g0, g1, left, right_ref, row_ref, col_ref, off, inv
):
    sub = iota((8, 128), 0)
    lane = iota((8, 128), 1)
    valid = sub < 6
    zero = jnp.zeros((8, 128), F32)
    for k in range(N + 1):
        for at in sorted({N * (N + 1) + k, k * (N + 1) + N}):
            t0[at] = zero
            g0[at] = zero
            g1[at] = zero
    right = [[] for _ in range(N)]
    thin = [zero] * N
    diag = [zero] * 4
    group = lane // 8
    for i in range(N):
        thick = zero
        for j in range(N):
            k = i * N + j
            x = got[k, 0:24, :].astype(F32)
            a, b = x[8:16], x[16:24]
            at = i * (N + 1) + j
            t0[at] = x[0:8]
            g0[at] = jnp.where(sub >= 6, a, jnp.where(sub >= 4, pltpu.roll(b, 6, 0), 0.0))
            g1[at] = jnp.where(
                sub >= 4, 0.0, jnp.where(sub >= 2, pltpu.roll(a, 4, 0), pltpu.roll(b, 2, 0))
            )
            right[j].append(jnp.where(valid, a, 0.0))
            for half in range(2):
                thin[j] = jnp.where(group == 8 * half + i, move(b, 64 + 8 * half, 64 * half + 8 * i), thin[j])
                thick = jnp.where(group == 8 * half + j, move(b, 80 + 8 * half, 64 * half + 8 * j), thick)
            total = b + pltpu.roll(b, 120, 1) + pltpu.roll(b, 112, 1)
            to = 64 * (i % 2) + 8 * j
            diag[i // 2] = jnp.where(group == to // 8, move(total, 96, to), diag[i // 2])
        col_ref[i] = jnp.where(valid, thick, 0.0)
        left[8 * i : 8 * i + 8, :] = panel_half(got, i, 16)
    col_ref[N] = zero
    off[...] = pivot_half(got, 24)
    full = 1.0 / jnp.concatenate([x[0:1] for x in diag], axis=1)
    inv[...] = jnp.broadcast_to(full, (8, TILE))
    right_ref[2 * N] = jnp.zeros((8, TILE), F32)
    right_ref[2 * N + 1] = jnp.zeros((8, TILE), F32)
    row_ref[N] = zero
    for j in range(N):
        parts = spread(right[j])
        right_ref[2 * j] = parts[0]
        right_ref[2 * j + 1] = parts[1]
        row_ref[j] = jnp.where(valid, thin[j], 0.0)


def route(
    other, t0, g0, g1, left, right_ref, row_ref, col_ref, off, inv, mapping, send, inverse, lower_ref, off_ref,
    pair_ref
):
    fill_inverse(mapping, inverse)
    core_id = lax.axis_index("col") % 2
    sub = iota((8, 128), 0)
    valid = sub < 6
    off_ref[core_id] = off[...]
    off_ref[1 - core_id] = pivot_half(other, 8)
    whole = jnp.concatenate([off_ref[0], off_ref[1]], axis=1)
    scale = inv[0:1, :]

    def times(x):
        high = x.astype(BF16)
        low = (x - high.astype(F32)).astype(BF16)
        both = dot(jnp.concatenate([high, low], axis=0), whole, (1, 0))
        return (both[:128] + both[128:]) * scale

    v = jnp.concatenate([left[...]] + [panel_half(other, i, 0) for i in range(N)], axis=0) * scale
    y = v - times(v)
    z = y + times(y)
    lower = 2.0 * y - z + times(z)
    for half in range(2):
        for i in range(N):
            at = 8 * (half * N + i)
            lower_ref[half * (N + 1) + i] = lower[at : at + 8]
        lower_ref[half * (N + 1) + N] = jnp.zeros((8, TILE), F32)
    index = [inverse[k] for k in range(2 * N)]
    rows = []
    for half in range(2):
        for s in range(2):
            for r in range(N):
                rows.append(lower_ref[jnp.bitwise_xor(half, core_id) * (N + 1) + index[2 * r + s]])
    cols = []
    for k in range(2 * N):
        for half in range(2):
            cols.append(right_ref[2 * index[k] + half])
    core = dot(
        jnp.concatenate(rows, axis=0).astype(BF16), jnp.concatenate(cols, axis=0).astype(BF16), (1, 1)
    )
    core = core.astype(BF16).astype(F32)
    first = [(N + 1) * x for x in index]
    place = iota((64, 128), 1) // 16
    lane = iota((8, 128), 1)
    low_lanes = lane < 64
    for r in range(N):
        x = col_ref[index[2 * r]]
        y = col_ref[index[2 * r + 1]]
        pair_ref[2 * r] = jnp.where(lane < 64, x, pltpu.roll(y, 64, 1))
        pair_ref[2 * r + 1] = jnp.where(lane < 64, pltpu.roll(x, 64, 1), y)
    for k in range(2 * N):
        c, h = k // 2, k % 2
        total = jnp.zeros((64, 128), F32)
        for combo in range(4):
            x = core[64 * combo : 64 * combo + 64, 128 * (k // 8) : 128 * (k // 8) + 128]
            total = jnp.where(place == combo, move(x, 16 * (k % 8), 16 * combo), total)
        beside = pltpu.roll(total, 64, 1)
        j = index[k]
        tail = row_ref[j]
        for r in range(N):
            part = total[8 * r : 8 * r + 8]
            shifted = beside[8 * r : 8 * r + 8]
            at0 = first[2 * r] + j
            at1 = first[2 * r + 1] + j
            spare = jnp.where(low_lanes, pltpu.roll(part, 6, 0), pltpu.roll(shifted, 4, 0))
            send[(h * N + r) * N + c] = jnp.concatenate(
                [
                    t0[at0],
                    t0[at1],
                    g0[at0] + g1[at1],
                    jnp.where(valid, tail, spare),
                    jnp.where(valid, pair_ref[2 * r + c % 2], pltpu.roll(part, 2, 0)),
                ],
                axis=0,
            ).astype(BF16)


def gather_up(blocks, lefts, rights, row_v, cores, own_u, order_out):
    def tile(f, g, c, at):
        return blocks[f * 64 + g * N + c, 8 * at : 8 * at + 8, :].astype(F32)

    k = iota((TILE, TILE), 0)
    target = 64 * ((k // 8) % 8) + 8 * (k // 64) + k % 8
    order = (target == iota((TILE, TILE), 1)).astype(BF16)
    order_out[...] = order
    sub = iota((8, 128), 0)
    group = iota((64, 128), 1) // 16
    core_id = lax.axis_index("col") % 2
    of_slot = (sub >= 4, sub < 4)
    mixed = []
    own = []
    for f in range(2):
        for side, into in ((0, lefts), (1, rights)):
            lanes = ([], [])
            for m in range(4):
                x = [
                    blocks[f * 64 + g * N + 2 * m + side, 0:24, :].astype(F32) for g in range(N)
                ]
                for s in range(2):
                    rows = []
                    for y in x:
                        rest = y[16:24]
                        if side == 0:
                            rest = jnp.where(of_slot[s], rest, 0.0)
                        rows += [y[8 * s : 8 * s + 8], rest]
                    lanes[s].append(jnp.concatenate(rows, axis=0))
            for s in range(2):
                into[s, 128 * f : 128 * f + 128, :] = jnp.concatenate(lanes[s], axis=1).astype(BF16)
        parts = []
        for c in range(N):
            rows = []
            for g in range(N):
                x = tile(f, g, c, 3)
                y = tile(f, g, c, 4)
                y = jnp.where(sub < 4, pltpu.roll(pltpu.roll(x, 64, 1), 4, 0), pltpu.roll(y, 6, 0))
                y = jnp.where(sub < 2, pltpu.roll(x, 2, 0), y)
                rows.append(jnp.where(sub < 6, y, 0.0))
            parts.append(jnp.concatenate(rows, axis=0))
        for s in range(2):
            halves = []
            for half in range(2):
                total = jnp.zeros((64, 128), F32)
                combo = 2 * half + s
                for c in range(N):
                    total = jnp.where(group == c, move(parts[c], 16 * combo, 16 * c), total)
                halves.append(total)
            first = jnp.where(core_id == 0, halves[0], halves[1])
            second = jnp.where(core_id == 0, halves[1], halves[0])
            cores[2 * f + s] = jnp.concatenate([first, second], axis=0).astype(BF16)
        for c in range(N):
            mixed += spread([tile(f, g, c, 3) for g in range(N)])
        own += half_panels([[tile(f, g, c, 4) for c in range(N)] for g in range(N)])
    panels = jnp.concatenate(mixed + own, axis=0).astype(BF16)
    panels = dot(panels, order, (1, 0)).astype(BF16)
    row_v[...] = panels[:256]
    own_u[...] = panels[256:]


def half_panels(tiles):
    both = [spread(x) for x in tiles]
    return [jnp.concatenate([x[s] for x in both], axis=0) for s in range(2)]


def finish(twin, lefts, rights, row_v, cores, own_u, order, out, made, sems):
    other = []
    for f in range(2):
        other += half_panels(
            [[twin[f * 64 + g * N + c].astype(F32) for c in range(N)] for g in range(N)]
        )
    stores = []
    for s in range(2):
        half = jnp.concatenate([other[s], other[2 + s]], axis=0).astype(BF16)
        half = dot(half, order[...], (1, 0)).astype(BF16)
        updates = []
        for f in range(2):
            at = slice(64 * (2 * f + s), 64 * (2 * f + s) + 64)
            col_u = jnp.concatenate([own_u[at, :], half[64 * f : 64 * f + 64]], axis=0)
            updates.append((-dot(cores[2 * f + s], col_u, (0, 0))).astype(BF16))
        both = jnp.concatenate([lefts[s]] + updates, axis=0)
        right = jnp.concatenate([rights[s], row_v[...]], axis=0)
        for part in range(4):
            rows = slice(128 * part, 128 * part + 128)
            made[s, rows, :] = dot(both[:, rows], right, (0, 0)).astype(BF16)
            copy = pltpu.make_async_copy(made.at[s, rows], out.at[s, rows], sems.at[4 * s + part])
            copy.start()
            stores.append(copy)
    for copy in stores:
        copy.wait()


def exchange(x, axes, name):
    with jax.named_scope(name):
        return lax.all_to_all(x, axes, split_axis=0, concat_axis=0, tiled=True)


def swap(x):
    return lax.ppermute(x, "col", [(k, k ^ 1) for k in range(N)])


def in_vmem(x):
    return pltpu.with_memory_space_constraint(x, VMEM)


def shards(
    pivot, col_ut, col_vt, col_rank, row_ut, row_vt, row_rank, cb_ut, cb_vt, cb_rank, parent_map
):
    sds = jax.ShapeDtypeStruct
    (send,) = call(
        pack,
        (VMEM((64, 40, 128), BF16),),
        (
            pivot[0],
            col_ut[0, 0].T,
            col_vt[0, 0].T,
            row_ut[0, 0].T,
            row_vt[0, 0].T,
            cb_ut[0, 0, 0],
            cb_vt[0, 0, 0],
            col_rank,
            row_rank,
            cb_rank,
        ),
        (VMEM,) * 7 + (SMEM,) * 3,
        name="pack",
        limit=None,
    )
    got = exchange(send, ("row", "col"), "scatter")
    other = in_vmem(swap(got[:, 16:40]))
    got = in_vmem(got)
    sorted_out = call(
        sort,
        (VMEM(((N + 1) ** 2, 8, 128), F32),) * 3
        + (
            VMEM((64, TILE), F32),
            VMEM((2 * N + 2, 8, TILE), F32),
            VMEM((N + 1, 8, 128), F32),
            VMEM((N + 1, 8, 128), F32),
            VMEM((TILE, TILE // 2), BF16),
            VMEM((8, TILE), F32),
        ),
        (got,),
        (VMEM,),
        name="sort",
    )
    (send,) = call(
        route,
        (VMEM((128, 40, 128), BF16),),
        (other, *(in_vmem(x) for x in sorted_out), parent_map),
        (VMEM,) * 11,
        (
            SMEM((2 * N,), jnp.int32),
            VMEM((2 * N + 2, 8, TILE), F32),
            VMEM((2, TILE, TILE // 2), BF16),
            VMEM((2 * N, 8, 128), F32),
        ),
        name="route",
    )
    blocks = exchange(send, ("side", "row", "col"), "gather")
    twin = in_vmem(swap(blocks[:, 32:40]))
    blocks = in_vmem(blocks)
    gathered = call(
        gather_up,
        (
            VMEM((2, 256, TILE), BF16),
            VMEM((2, 256, TILE), BF16),
            VMEM((256, TILE), BF16),
            VMEM((4, 128, 128), BF16),
            VMEM((256, TILE), BF16),
            VMEM((TILE, TILE), BF16),
        ),
        (blocks,),
        (VMEM,),
        name="gather_up",
    )
    (out,) = call(
        finish,
        (sds((2, TILE, TILE), BF16),),
        (twin, *(in_vmem(x) for x in gathered)),
        (VMEM,) * 7,
        (
            VMEM((2, TILE, TILE), BF16),
            pltpu.SemaphoreType.DMA((8,)),
        ),
        name="finish",
        into=pl.ANY,
    )
    return out[None, :, None]


def solution(mesh):
    front = ("pair", "side")
    split = Mesh(mesh.devices.reshape(4, 2, N, N), ("pair", "side", "row", "col"))
    placed = (
        P(front, ("row", "col"), None),
        P(front, "row", None, "col"),
        P(front, "row", None, "col"),
        P(front, "row"),
        P(front, "col", None, "row"),
        P(front, "col", None, "row"),
        P(front, "col"),
        P(front, "row", "col", None, None),
        P(front, "row", "col", None, None),
        P(front, "row", "col"),
        P(front, None),
    )

    return jax.shard_map(
        shards,
        mesh=split,
        in_specs=placed,
        out_specs=P(front, "row", "col", None, None),
        check_vma=False,
    )
```
